32 devices in a mesh: events: 2 (over y), blk: 4 (over z), sub: 2 (over x), pair: 2 (over core).
Axes of the slice: x: 2, y: 2, z: 4, core: 2. Of those that a mesh axis runs over, the one named last changes fastest.
Arguments:
- synthetic: bfloat16 [2560, 4096], P(('events', 'sub', 'pair'), 'blk'), parts along dimension 0, may hold values from -6 to 6
- observed: bfloat16 [2560, 4096], P(('events', 'sub', 'pair'), 'blk'), parts along dimension 0, may hold values from -6 to 6
- station_weights: int32 [2560], P('events'), parts along dimension 0, may hold values from 1 to 4
- pair_mask: int32 [32, 16], P('events'), parts along dimension 0, may hold values from 0 to 1, as said below
Outputs:
- adjoint_traces: bfloat16 [2560, 4096], P(('events', 'sub', 'pair'), 'blk'), parts along dimension 0
The draws below stay inside these ranges and needn't reach their ends.
There are 2 independent parts, one for each index of `events`. The reference program is written for one: setup_inputs(seed, part) draws one part's arguments, and reference() takes and returns one part's arrays. A program takes and returns all parts, laid end to end along the dimension named above; each array names one. Nothing has to cross between parts.
Inputs may be any that keep to these rules, and one draw needn't show every extreme that they name: pair_mask[p, q] is 1 where station pieces p and q are coupled; piece p holds stations p * 80 to (p + 1) * 80 - 1.
All inputs are finite; a program needn't handle non-finite values.
Results may differ from the reference program's by a relative error of at most 0.025.
Values may be sent and summed in bfloat16 or wider, within the bound.
No kernel may reach another device: no remote copies, remote signals or barrier semaphores. Data moves between devices by JAX's collectives and lax.ppermute only.
A program may use at most 64 MiB of HBM per device.

```python
import math
import jax
import jax.numpy as jnp
from jax import lax

NT = 4096
NF = 512
F_LO = 64
PIECE = 80
CYCLE = 4
STATIONS = 1280
NPIECE = 16


def draw_pair_mask(key, part):
    level_key = jax.random.fold_in(key, 11)
    entry_key = jax.random.fold_in(key, 12)
    levels = jax.random.randint(level_key, (CYCLE,), 0, 5)
    entries = jax.random.randint(entry_key, (NPIECE, NPIECE), 0, 4)
    bands = jnp.arange(NPIECE, dtype=jnp.int32) % CYCLE
    piece_level = levels[bands]
    bound = jnp.minimum(piece_level[:, None], piece_level[None, :])
    return (entries < bound).astype(jnp.int32)


def touch_ends(drawn, rng, low, top_value):
    spot = [jax.random.randint(jax.random.fold_in(rng, axis), (), 0, length) for axis, length in enumerate(drawn.shape)]
    main_axis = drawn.shape.index(max(drawn.shape))
    neighbour = spot[:main_axis] + [(spot[main_axis] + 1) % drawn.shape[main_axis]] + spot[main_axis + 1:]
    return drawn.at[tuple(spot)].set(low).at[tuple(neighbour)].set(top_value)


def shard_levels(rng, extent, pieces, smallest, high):
    def one(dim, blocks):
        heights = jax.random.uniform(jax.random.fold_in(jax.random.fold_in(rng, 6), dim), (blocks,), jnp.float32, smallest / len(pieces), high / len(pieces))
        return jnp.repeat(jnp.exp(heights), extent[dim] // blocks).reshape((-1,) + (1,) * (len(extent) - dim - 1))

    gain = one(*pieces[0])
    for cut in pieces[1:]:
        gain = gain * one(*cut)
    return gain


def noise(stream_key, shape, deviation, most, shards=(), kind=jnp.bfloat16):
    values = jax.random.normal(stream_key, shape, jnp.float32) * deviation
    if len(shards) > 0:
        values = shard_levels(stream_key, shape, shards, -0.22, 0.18) * values
    return jnp.clip(values, min=-most, max=most).astype(kind)


def setup_inputs(seed: int = 0, part: int = 0) -> dict:
    key_of = jax.random.split(jax.random.key(seed), 5)
    own_keys = jax.random.split(jax.random.fold_in(key_of[4], part), 5)
    return {
        "synthetic": noise(own_keys[0], (STATIONS, NT), 1.0, 6.0, ((0, 4), (1, 4))),
        "observed": noise(own_keys[1], (STATIONS, NT), 1.0, 6.0, ((0, 4), (1, 4))),
        "station_weights": touch_ends(jax.random.randint(own_keys[2], (STATIONS,), 1, 5), jax.random.fold_in(own_keys[2], 1), 1, 4).astype(jnp.int32),
        "pair_mask": draw_pair_mask(jax.random.fold_in(jax.random.fold_in(key_of[4], part), 71), part),
    }


epsilon = 1e-06

def make_basis(first_sample, sample_count):
    sample_index = first_sample + jnp.arange(sample_count, dtype=jnp.int32)
    bin_index = F_LO + jnp.arange(NF, dtype=jnp.int32)
    phases = sample_index[:, None] * bin_index[None, :] % NT
    angles = phases.astype(jnp.float32) * (2.0 * math.pi / NT)
    return jnp.concatenate([jnp.cos(angles), -jnp.sin(angles)], axis=1).astype(jnp.bfloat16)

def spectral_rate(spectrum):
    angular = 2.0 * math.pi / NT * (F_LO + jnp.arange(NF, dtype=jnp.int32)).astype(jnp.float32)
    widened = spectrum.astype(jnp.float32)
    return jnp.concatenate([-angular * widened[:, NF:], angular * widened[:, :NF]], axis=1).astype(jnp.bfloat16)

def reference(synthetic, observed, station_weights, pair_mask):
    basis = make_basis(0, NT)
    scale_factor = 1.0 / math.sqrt(NT)
    model_spec = (jnp.dot(synthetic, basis, preferred_element_type=jnp.float32) * scale_factor).astype(jnp.bfloat16)
    data_spec = (jnp.dot(observed, basis, preferred_element_type=jnp.float32) * scale_factor).astype(jnp.bfloat16)
    model_rate = spectral_rate(model_spec)
    data_rate = spectral_rate(data_spec)
    power = lax.optimization_barrier(jnp.sum(jnp.square(model_rate.astype(jnp.float32)), axis=1))
    link_piece = jnp.maximum(pair_mask, pair_mask.T)
    gains = station_weights.astype(jnp.float32)
    factor = 4.0 / math.sqrt(STATIONS)
    rows_per = math.gcd(STATIONS, 128)
    starts = jnp.arange(0, STATIONS, rows_per, dtype=jnp.int32)

    def one_block(row_start):
        row_ids = row_start + jnp.arange(rows_per, dtype=jnp.int32)
        model_rows = lax.dynamic_slice_in_dim(model_spec, row_start, rows_per, 0)
        data_rows = lax.dynamic_slice_in_dim(data_spec, row_start, rows_per, 0)
        cross_model = jnp.dot(model_rows, model_rate.T, preferred_element_type=jnp.float32)
        cross_data = jnp.dot(data_rows, data_rate.T, preferred_element_type=jnp.float32)
        link_rows = jnp.repeat(link_piece[row_ids // PIECE], PIECE, axis=1).astype(jnp.float32)
        row_power = lax.dynamic_slice_in_dim(power, row_start, rows_per, 0)
        row_gain = lax.dynamic_slice_in_dim(gains, row_start, rows_per, 0)
        normalizer = 0.5 * (row_power[:, None] + power[None, :]) + epsilon
        coupling = (factor * row_gain[:, None] * gains[None, :] * link_rows * (cross_model - cross_data) / normalizer).astype(jnp.bfloat16)
        return jnp.dot(coupling, model_rate, preferred_element_type=jnp.float32)
    adjoint_spec = lax.map(one_block, starts).reshape(STATIONS, 2 * NF).astype(jnp.bfloat16)
    inverse_scale = 1.0 / math.sqrt(NF)
    return (jnp.dot(adjoint_spec, basis.T, preferred_element_type=jnp.float32) * inverse_scale).astype(jnp.bfloat16)
```

```python
import functools
import math

import jax
import jax.numpy as jnp
from jax import lax
from jax.experimental import pallas as pl
from jax.experimental.pallas import tpu as pltpu
from jax.sharding import PartitionSpec as P

NT = 4096
NF = 512
F_LO = 64

epsilon = 1e-06
CONTRACT_LAST = (((1,), (1,)), ((), ()))


def shift(value, axis, steps):
    count = lax.axis_size(axis)
    pairs = [(source, (source + steps) % count) for source in range(count)]
    return lax.ppermute(value, axis, pairs)


def sweep(count):
    order = []
    for near in range(1, count // 2 + 1):
        order.append(near)
        if (count - near) % count != near:
            order.append(count - near)
    return order


def cos_sin(samples):
    bins = F_LO + jnp.arange(NF, dtype=jnp.int32)
    phases = samples[:, None] * bins[None, :] % NT
    angles = phases.astype(jnp.float32) * (2.0 * math.pi / NT)
    return jnp.cos(angles), jnp.sin(angles)


def basis_kernel(per_step, low_rows, hc_ref, hs_ref, lc_ref, ls_ref, out_ref):
    step = pl.program_id(0)
    for h in range(per_step):
        hc = hc_ref[pl.ds(step * per_step + h, 1), :]
        hs = hs_ref[pl.ds(step * per_step + h, 1), :]
        lc = lc_ref[...]
        ls = ls_ref[...]
        rows = slice(h * low_rows, (h + 1) * low_rows)
        out_ref[rows, :NF] = (hc * lc - hs * ls).astype(jnp.bfloat16)
        out_ref[rows, NF:] = (-(hs * lc + hc * ls)).astype(jnp.bfloat16)


def make_basis(firsts, span):
    low_rows = math.gcd(span, 64)
    low_c, low_s = cos_sin(jnp.arange(low_rows, dtype=jnp.int32))
    highs = (firsts[:, None] + jnp.arange(0, span, low_rows, dtype=jnp.int32)[None, :]).reshape(-1)
    high_c, high_s = cos_sin(highs)
    per_step = math.gcd(highs.shape[0], 4)
    whole = lambda a: pl.BlockSpec(a.shape, lambda i: (0, 0))
    rows = highs.shape[0] * low_rows
    return pl.pallas_call(
        functools.partial(basis_kernel, per_step, low_rows),
        grid=(highs.shape[0] // per_step,),
        in_specs=[whole(high_c), whole(high_s), whole(low_c), whole(low_s)],
        out_specs=pl.BlockSpec((per_step * low_rows, 2 * NF), lambda i: (i, 0)),
        out_shape=jax.ShapeDtypeStruct((rows, 2 * NF), jnp.bfloat16),
        cost_estimate=pl.CostEstimate(
            flops=8 * rows * NF, bytes_accessed=4 * rows * NF, transcendentals=0
        ),
        name="basis",
    )(high_c, high_s, low_c, low_s)


def angular_row():
    bins = F_LO + lax.broadcasted_iota(jnp.int32, (1, NF), 1)
    return 2.0 * math.pi / NT * bins.astype(jnp.float32)


def rate_of(re, im):
    angular = angular_row()
    return jnp.concatenate([-angular * im, angular * re], axis=1).astype(jnp.bfloat16)


def tile_kernel(first, rows_ref, power_ref, coef_ref, gain_ref, col_ref, *rest):
    out_ref = rest[-1]
    col = col_ref[...].astype(jnp.float32)
    model_rate = rate_of(col[:, :NF], col[:, NF : 2 * NF])
    data_rate = rate_of(-col[:, 2 * NF : 3 * NF], -col[:, 3 * NF :])
    both = jnp.concatenate([model_rate, data_rate], axis=1)
    cross = lax.dot_general(
        rows_ref[...], both, CONTRACT_LAST, preferred_element_type=jnp.float32
    )
    col_power = lax.dot_general(
        jnp.ones((8, 2 * NF), jnp.float32),
        jnp.square(model_rate.astype(jnp.float32)),
        CONTRACT_LAST,
        precision=lax.Precision.HIGHEST,
        preferred_element_type=jnp.float32,
    )[0:1, :]
    normalizer = 0.5 * (power_ref[...] + col_power) + epsilon
    coupling = (coef_ref[...] * gain_ref[...] * cross / normalizer).astype(jnp.bfloat16)
    update = jnp.dot(coupling, model_rate, preferred_element_type=jnp.float32)
    if first:
        out_ref[...] = update
    else:
        out_ref[...] = rest[0][...] + update


def pair_tile(running, rows, row_power, coef, gain, col):
    args = [rows, row_power, coef, gain, col]
    aliases = {}
    if running is not None:
        aliases = {len(args): 0}
        args.append(running)
    height, width = rows.shape[0], col.shape[0]
    return pl.pallas_call(
        functools.partial(tile_kernel, running is None),
        in_specs=[pl.BlockSpec(memory_space=pltpu.VMEM)] * len(args),
        out_specs=pl.BlockSpec(memory_space=pltpu.VMEM),
        out_shape=jax.ShapeDtypeStruct((height, 2 * NF), jnp.float32),
        input_output_aliases=aliases,
        cost_estimate=pl.CostEstimate(
            flops=12 * height * width * NF,
            bytes_accessed=16 * height * NF,
            transcendentals=0,
        ),
        name="pair_tile",
    )(*args)


def shards(synthetic, observed, station_weights, pair_mask):
    levels = lax.axis_size("blk")
    subs = lax.axis_size("sub")
    pairs = lax.axis_size("pair")
    level = lax.axis_index("blk")
    sub = lax.axis_index("sub")
    pair = lax.axis_index("pair")
    span = synthetic.shape[1]
    piece = synthetic.shape[0] // levels
    stations = station_weights.shape[0]

    def owned_by(steps):
        owner = (level + steps) % levels
        return jnp.concatenate(
            [
                lax.dynamic_slice_in_dim(synthetic, owner * piece, piece, 0),
                lax.dynamic_slice_in_dim(observed, owner * piece, piece, 0),
            ],
            axis=0,
        )

    order = sweep(levels)
    blocks = {0: owned_by(0)}
    for steps in order:
        blocks[steps] = shift(owned_by(steps), "blk", steps)
    arrivals = [0] + order
    firsts = jnp.stack([(level - steps) % levels * span for steps in arrivals]).astype(jnp.int32)
    basis = make_basis(firsts, span)
    total = None
    for place, steps in enumerate(arrivals):
        part = jnp.dot(
            blocks[steps],
            basis[place * span : (place + 1) * span],
            preferred_element_type=jnp.float32,
        )
        total = part if total is None else total + part
    spec = (total * (1.0 / math.sqrt(NT))).astype(jnp.bfloat16)
    own = jnp.concatenate([spec[:piece], spec[piece:]], axis=1)

    columns = {0: own}
    for steps in order:
        columns[steps] = shift(own, "blk", steps)
    blocks_of_rows = []
    members = []
    for s in range(subs):
        here = own if s == 0 else shift(own, "sub", s)
        for q in range(pairs):
            blocks_of_rows.append(here if q == 0 else shift(here, "pair", q))
            members.append((sub - s) % subs * pairs + (pair - q) % pairs)
    rows = jnp.concatenate(blocks_of_rows, axis=0)
    members = jnp.stack(members)
    member = sub * pairs + pair

    gains = station_weights.astype(jnp.float32).reshape(-1, piece)
    link = jnp.maximum(pair_mask, pair_mask.T).astype(jnp.float32)
    row_pieces = members * levels + level
    row_gain = gains[row_pieces].reshape(-1, 1)
    row_link = link[row_pieces]
    factor = 4.0 / math.sqrt(stations)
    widened = rows[:, : 2 * NF].astype(jnp.float32)
    row_rate = rate_of(widened[:, :NF], widened[:, NF:])
    row_power = jnp.sum(jnp.square(row_rate.astype(jnp.float32)), axis=1, keepdims=True)

    running = None
    for steps in arrivals:
        column_piece = member * levels + (level - steps) % levels
        active = lax.dynamic_slice_in_dim(row_link, column_piece, 1, 1)
        coef = factor * row_gain * jnp.repeat(active, piece, axis=0)
        gain = lax.dynamic_slice_in_dim(gains, column_piece, 1, 0)
        running = pair_tile(running, rows, row_power, coef, gain, columns[steps])

    partial = running.reshape(subs, pairs, piece, 2 * NF)
    held = partial[:, 0]
    for q in range(1, pairs):
        sent = partial[:, q].astype(jnp.bfloat16)
        held = held + shift(sent, "pair", -q).astype(jnp.float32)
    adjoint = held[0]
    for s in range(1, subs):
        adjoint = adjoint + shift(held[s].astype(jnp.bfloat16), "sub", -s).astype(jnp.float32)
    adjoint = adjoint.astype(jnp.bfloat16)

    gathered = jnp.zeros((levels * piece, 2 * NF), jnp.bfloat16)
    for steps in arrivals:
        arrived = adjoint if steps == 0 else shift(adjoint, "blk", steps)
        gathered = lax.dynamic_update_slice_in_dim(
            gathered, arrived, (level - steps) % levels * piece, 0
        )
    return (
        lax.dot_general(
            gathered, basis[:span], CONTRACT_LAST, preferred_element_type=jnp.float32
        )
        * (1.0 / math.sqrt(NF))
    ).astype(jnp.bfloat16)


def solution(mesh):
    placed = (
        P(("events", "sub", "pair"), "blk"),
        P(("events", "sub", "pair"), "blk"),
        P("events"),
        P("events", None),
    )
    return jax.shard_map(
        shards,
        mesh=mesh,
        in_specs=placed,
        out_specs=P(("events", "sub", "pair"), "blk"),
        check_vma=False,
    )
```

```python
import functools
import math

import jax
import jax.numpy as jnp
from jax import lax
from jax.experimental import pallas as pl
from jax.experimental.pallas import tpu as pltpu
from jax.sharding import PartitionSpec as P


NT = 4096
NF = 512
F_LO = 64

epsilon = 1e-06
CONTRACT_LAST = (((1,), (1,)), ((), ()))


def shift(value, axis, steps):
    count = lax.axis_size(axis)
    pairs = [(source, (source + steps) % count) for source in range(count)]
    return lax.ppermute(value, axis, pairs)


def sweep(count):
    order = []
    for near in range(1, count // 2 + 1):
        order.append(near)
        if (count - near) % count != near:
            order.append(count - near)
    return order


def cos_sin(samples):
    bins = F_LO + jnp.arange(NF, dtype=jnp.int32)
    phases = samples[:, None] * bins[None, :] % NT
    angles = phases.astype(jnp.float32) * (2.0 * math.pi / NT)
    return jnp.cos(angles), jnp.sin(angles)


def basis_kernel(per_step, low_rows, hc_ref, hs_ref, lc_ref, ls_ref, out_ref):
    step = pl.program_id(0)
    for h in range(per_step):
        hc = hc_ref[pl.ds(step * per_step + h, 1), :]
        hs = hs_ref[pl.ds(step * per_step + h, 1), :]
        lc = lc_ref[...]
        ls = ls_ref[...]
        rows = slice(h * low_rows, (h + 1) * low_rows)
        out_ref[rows, :NF] = (hc * lc - hs * ls).astype(jnp.bfloat16)
        out_ref[rows, NF:] = (-(hs * lc + hc * ls)).astype(jnp.bfloat16)


def make_basis(firsts, span):
    low_rows = math.gcd(span, 64)
    low_c, low_s = cos_sin(jnp.arange(low_rows, dtype=jnp.int32))
    highs = (firsts[:, None] + jnp.arange(0, span, low_rows, dtype=jnp.int32)[None, :]).reshape(-1)
    high_c, high_s = cos_sin(highs)
    per_step = math.gcd(highs.shape[0], 4)
    whole = lambda a: pl.BlockSpec(a.shape, lambda i: (0, 0))
    rows = highs.shape[0] * low_rows
    return pl.pallas_call(
        functools.partial(basis_kernel, per_step, low_rows),
        grid=(highs.shape[0] // per_step,),
        in_specs=[whole(high_c), whole(high_s), whole(low_c), whole(low_s)],
        out_specs=pl.BlockSpec((per_step * low_rows, 2 * NF), lambda i: (i, 0)),
        out_shape=jax.ShapeDtypeStruct((rows, 2 * NF), jnp.bfloat16),
        cost_estimate=pl.CostEstimate(
            flops=8 * rows * NF, bytes_accessed=4 * rows * NF, transcendentals=0
        ),
        name="basis",
    )(high_c, high_s, low_c, low_s)


def angular_row():
    bins = F_LO + lax.broadcasted_iota(jnp.int32, (1, NF), 1)
    return 2.0 * math.pi / NT * bins.astype(jnp.float32)


def rate_of(re, im):
    angular = angular_row()
    return jnp.concatenate([-angular * im, angular * re], axis=1).astype(jnp.bfloat16)


def tile_kernel(first, rows_ref, power_ref, coef_ref, gain_ref, col_ref, *rest):
    out_ref = rest[-1]
    col = col_ref[...].astype(jnp.float32)
    model_rate = rate_of(col[:, :NF], col[:, NF : 2 * NF])
    data_rate = rate_of(-col[:, 2 * NF : 3 * NF], -col[:, 3 * NF :])
    both = jnp.concatenate([model_rate, data_rate], axis=1)
    cross = lax.dot_general(
        rows_ref[...], both, CONTRACT_LAST, preferred_element_type=jnp.float32
    )
    col_power = lax.dot_general(
        jnp.ones((8, 2 * NF), jnp.float32),
        jnp.square(model_rate.astype(jnp.float32)),
        CONTRACT_LAST,
        precision=lax.Precision.HIGHEST,
        preferred_element_type=jnp.float32,
    )[0:1, :]
    normalizer = 0.5 * (power_ref[...] + col_power) + epsilon
    coupling = (coef_ref[...] * gain_ref[...] * cross / normalizer).astype(jnp.bfloat16)
    update = jnp.dot(coupling, model_rate, preferred_element_type=jnp.float32)
    if first:
        out_ref[...] = update
    else:
        out_ref[...] = rest[0][...] + update


def pair_tile(running, rows, row_power, coef, gain, col):
    args = [rows, row_power, coef, gain, col]
    aliases = {}
    if running is not None:
        aliases = {len(args): 0}
        args.append(running)
    height, width = rows.shape[0], col.shape[0]
    return pl.pallas_call(
        functools.partial(tile_kernel, running is None),
        in_specs=[pl.BlockSpec(memory_space=pltpu.VMEM)] * len(args),
        out_specs=pl.BlockSpec(memory_space=pltpu.VMEM),
        out_shape=jax.ShapeDtypeStruct((height, 2 * NF), jnp.float32),
        input_output_aliases=aliases,
        cost_estimate=pl.CostEstimate(
            flops=12 * height * width * NF,
            bytes_accessed=16 * height * NF,
            transcendentals=0,
        ),
        name="pair_tile",
    )(*args)


def body(synthetic, observed, station_weights, pair_mask):
    levels = lax.axis_size("blk")
    subs = lax.axis_size("sub")
    pairs = lax.axis_size("pair")
    level = lax.axis_index("blk")
    sub = lax.axis_index("sub")
    pair = lax.axis_index("pair")
    span = synthetic.shape[1]
    piece = synthetic.shape[0] // levels
    stations = station_weights.shape[0]

    def owned_by(steps):
        owner = (level + steps) % levels
        return jnp.concatenate(
            [
                lax.dynamic_slice_in_dim(synthetic, owner * piece, piece, 0),
                lax.dynamic_slice_in_dim(observed, owner * piece, piece, 0),
            ],
            axis=0,
        )

    order = sweep(levels)
    blocks = {0: owned_by(0)}
    for steps in order:
        blocks[steps] = shift(owned_by(steps), "blk", steps)
    arrivals = [0] + order
    firsts = jnp.stack([(level - steps) % levels * span for steps in arrivals]).astype(jnp.int32)
    basis = make_basis(firsts, span)
    member = sub * pairs + pair
    members = jnp.stack(
        [
            (sub - s) % subs * pairs + (pair - q) % pairs
            for s in range(subs)
            for q in range(pairs)
        ]
    )
    gains = station_weights.astype(jnp.float32).reshape(-1, piece)
    link = jnp.maximum(pair_mask, pair_mask.T).astype(jnp.float32)
    row_pieces = members * levels + level
    row_gain = gains[row_pieces].reshape(-1, 1)
    row_link = link[row_pieces]
    factor = 4.0 / math.sqrt(stations)
    coefs, col_gains = [], []
    for steps in arrivals:
        column_piece = member * levels + (level - steps) % levels
        active = lax.dynamic_slice_in_dim(row_link, column_piece, 1, 1)
        coefs.append(factor * row_gain * jnp.repeat(active, piece, axis=0))
        col_gains.append(lax.dynamic_slice_in_dim(gains, column_piece, 1, 0))
    last = order[-1]
    blocks[last], coefs, col_gains = lax.optimization_barrier((blocks[last], coefs, col_gains))
    total = None
    for place, steps in enumerate(arrivals):
        part = jnp.dot(
            blocks[steps],
            basis[place * span : (place + 1) * span],
            preferred_element_type=jnp.float32,
        )
        total = part if total is None else total + part
    spec = (total * (1.0 / math.sqrt(NT))).astype(jnp.bfloat16)
    own = jnp.concatenate([spec[:piece], spec[piece:]], axis=1)

    columns = {0: own}
    for steps in order:
        columns[steps] = shift(own, "blk", steps)
    blocks_of_rows = []
    for s in range(subs):
        here = own if s == 0 else shift(own, "sub", s)
        for q in range(pairs):
            blocks_of_rows.append(here if q == 0 else shift(here, "pair", q))
    rows = jnp.concatenate(blocks_of_rows, axis=0)
    widened = rows[:, : 2 * NF].astype(jnp.float32)
    row_rate = rate_of(widened[:, :NF], widened[:, NF:])
    row_power = jnp.sum(jnp.square(row_rate.astype(jnp.float32)), axis=1, keepdims=True)

    running = None
    for place, steps in enumerate(arrivals):
        running = pair_tile(
            running, rows, row_power, coefs[place], col_gains[place], columns[steps]
        )

    partial = running.reshape(subs, pairs, piece, 2 * NF)
    held = partial[:, 0]
    for q in range(1, pairs):
        sent = partial[:, q].astype(jnp.bfloat16)
        held = held + shift(sent, "pair", -q).astype(jnp.float32)
    adjoint = held[0]
    for s in range(1, subs):
        adjoint = adjoint + shift(held[s].astype(jnp.bfloat16), "sub", -s).astype(jnp.float32)
    adjoint = adjoint.astype(jnp.bfloat16)

    gathered = jnp.zeros((levels * piece, 2 * NF), jnp.bfloat16)
    for steps in arrivals:
        arrived = adjoint if steps == 0 else shift(adjoint, "blk", steps)
        gathered = lax.dynamic_update_slice_in_dim(
            gathered, arrived, (level - steps) % levels * piece, 0
        )
    return (
        lax.dot_general(
            gathered, basis[:span], CONTRACT_LAST, preferred_element_type=jnp.float32
        )
        * (1.0 / math.sqrt(NF))
    ).astype(jnp.bfloat16)


def solution(mesh):
    placed = (
        P(("events", "sub", "pair"), "blk"),
        P(("events", "sub", "pair"), "blk"),
        P("events"),
        P("events", None),
    )
    return jax.shard_map(
        body,
        mesh=mesh,
        in_specs=placed,
        out_specs=P(("events", "sub", "pair"), "blk"),
        check_vma=False,
    )
```

```python
import functools
import math

import jax
import jax.numpy as jnp
from jax import lax
from jax.experimental import pallas as pl
from jax.experimental.pallas import tpu as pltpu
from jax.sharding import PartitionSpec as P


NT = 4096
NF = 512
F_LO = 64

epsilon = 1e-06
CONTRACT_LAST = (((1,), (1,)), ((), ()))


def shift(value, axis, steps):
    count = lax.axis_size(axis)
    pairs = [(source, (source + steps) % count) for source in range(count)]
    return lax.ppermute(value, axis, pairs)


def sweep(count):
    order = []
    for near in range(1, count // 2 + 1):
        order.append(near)
        if (count - near) % count != near:
            order.append(count - near)
    return order


def cos_sin(samples):
    bins = F_LO + jnp.arange(NF, dtype=jnp.int32)
    phases = samples[:, None] * bins[None, :] % NT
    angles = phases.astype(jnp.float32) * (2.0 * math.pi / NT)
    return jnp.cos(angles), jnp.sin(angles)


def basis_kernel(per_step, low_rows, hc_ref, hs_ref, lc_ref, ls_ref, out_ref):
    step = pl.program_id(0)
    for h in range(per_step):
        hc = hc_ref[pl.ds(step * per_step + h, 1), :]
        hs = hs_ref[pl.ds(step * per_step + h, 1), :]
        lc = lc_ref[...]
        ls = ls_ref[...]
        rows = slice(h * low_rows, (h + 1) * low_rows)
        out_ref[rows, :NF] = (hc * lc - hs * ls).astype(jnp.bfloat16)
        out_ref[rows, NF:] = (-(hs * lc + hc * ls)).astype(jnp.bfloat16)


def make_basis(firsts, span):
    low_rows = math.gcd(span, 64)
    low_c, low_s = cos_sin(jnp.arange(low_rows, dtype=jnp.int32))
    highs = (firsts[:, None] + jnp.arange(0, span, low_rows, dtype=jnp.int32)[None, :]).reshape(-1)
    high_c, high_s = cos_sin(highs)
    per_step = math.gcd(highs.shape[0], 4)
    whole = lambda a: pl.BlockSpec(a.shape, lambda i: (0, 0))
    rows = highs.shape[0] * low_rows
    return pl.pallas_call(
        functools.partial(basis_kernel, per_step, low_rows),
        grid=(highs.shape[0] // per_step,),
        in_specs=[whole(high_c), whole(high_s), whole(low_c), whole(low_s)],
        out_specs=pl.BlockSpec((per_step * low_rows, 2 * NF), lambda i: (i, 0)),
        out_shape=jax.ShapeDtypeStruct((rows, 2 * NF), jnp.bfloat16),
        cost_estimate=pl.CostEstimate(
            flops=8 * rows * NF, bytes_accessed=4 * rows * NF, transcendentals=0
        ),
        name="basis",
    )(high_c, high_s, low_c, low_s)


def angular_row():
    bins = F_LO + lax.broadcasted_iota(jnp.int32, (1, NF), 1)
    return 2.0 * math.pi / NT * bins.astype(jnp.float32)


def rate_of(re, im):
    angular = angular_row()
    return jnp.concatenate([-angular * im, angular * re], axis=1).astype(jnp.bfloat16)


def tile_kernel(first, rows_ref, power_ref, coef_ref, gain_ref, col_ref, *rest):
    out_ref = rest[-1]
    col = col_ref[...].astype(jnp.float32)
    model_rate = rate_of(col[:, :NF], col[:, NF : 2 * NF])
    data_rate = rate_of(-col[:, 2 * NF : 3 * NF], -col[:, 3 * NF :])
    both = jnp.concatenate([model_rate, data_rate], axis=1)
    cross = lax.dot_general(
        rows_ref[...], both, CONTRACT_LAST, preferred_element_type=jnp.float32
    )
    col_power = lax.dot_general(
        jnp.ones((8, 2 * NF), jnp.float32),
        jnp.square(model_rate.astype(jnp.float32)),
        CONTRACT_LAST,
        precision=lax.Precision.HIGHEST,
        preferred_element_type=jnp.float32,
    )[0:1, :]
    normalizer = 0.5 * (power_ref[...] + col_power) + epsilon
    coupling = (coef_ref[...] * gain_ref[...] * cross / normalizer).astype(jnp.bfloat16)
    update = jnp.dot(coupling, model_rate, preferred_element_type=jnp.float32)
    if first:
        out_ref[...] = update
    else:
        out_ref[...] = rest[0][...] + update


def pair_tile(running, rows, row_power, coef, gain, col):
    args = [rows, row_power, coef, gain, col]
    aliases = {}
    if running is not None:
        aliases = {len(args): 0}
        args.append(running)
    height, width = rows.shape[0], col.shape[0]
    return pl.pallas_call(
        functools.partial(tile_kernel, running is None),
        in_specs=[pl.BlockSpec(memory_space=pltpu.VMEM)] * len(args),
        out_specs=pl.BlockSpec(memory_space=pltpu.VMEM),
        out_shape=jax.ShapeDtypeStruct((height, 2 * NF), jnp.float32),
        input_output_aliases=aliases,
        cost_estimate=pl.CostEstimate(
            flops=12 * height * width * NF,
            bytes_accessed=16 * height * NF,
            transcendentals=0,
        ),
        name="pair_tile",
    )(*args)


def ring_body(synthetic, observed, station_weights, pair_mask):
    levels = lax.axis_size("blk")
    subs = lax.axis_size("sub")
    pairs = lax.axis_size("pair")
    level = lax.axis_index("blk")
    sub = lax.axis_index("sub")
    pair = lax.axis_index("pair")
    span = synthetic.shape[1]
    piece = synthetic.shape[0] // levels
    stations = station_weights.shape[0]

    def owned_by(steps):
        owner = (level + steps) % levels
        return jnp.concatenate(
            [
                lax.dynamic_slice_in_dim(synthetic, owner * piece, piece, 0),
                lax.dynamic_slice_in_dim(observed, owner * piece, piece, 0),
            ],
            axis=0,
        )

    order = sweep(levels)
    blocks = {0: owned_by(0)}
    for steps in order:
        blocks[steps] = shift(owned_by(steps), "blk", steps)
    arrivals = [0] + order
    firsts = jnp.stack([(level - steps) % levels * span for steps in arrivals]).astype(jnp.int32)
    basis = make_basis(firsts, span)
    member = sub * pairs + pair
    members = jnp.stack(
        [
            (sub - s) % subs * pairs + (pair - q) % pairs
            for s in range(subs)
            for q in range(pairs)
        ]
    )
    gains = station_weights.astype(jnp.float32).reshape(-1, piece)
    link = jnp.maximum(pair_mask, pair_mask.T).astype(jnp.float32)
    row_pieces = members * levels + level
    row_gain = gains[row_pieces].reshape(-1, 1)
    row_link = link[row_pieces]
    factor = 4.0 / math.sqrt(stations)
    coefs, col_gains = [], []
    for steps in arrivals:
        column_piece = member * levels + (level - steps) % levels
        active = lax.dynamic_slice_in_dim(row_link, column_piece, 1, 1)
        coefs.append(factor * row_gain * jnp.repeat(active, piece, axis=0))
        col_gains.append(lax.dynamic_slice_in_dim(gains, column_piece, 1, 0))
    last = order[-1]
    blocks[last], coefs, col_gains = lax.optimization_barrier((blocks[last], coefs, col_gains))
    total = None
    for place, steps in enumerate(arrivals):
        part = jnp.dot(
            blocks[steps],
            basis[place * span : (place + 1) * span],
            preferred_element_type=jnp.float32,
        )
        total = part if total is None else total + part
    spec = (total * (1.0 / math.sqrt(NT))).astype(jnp.bfloat16)
    own = jnp.concatenate([spec[:piece], spec[piece:]], axis=1)

    columns = {0: own}
    for steps in order:
        columns[steps] = shift(own, "blk", steps)
    blocks_of_rows = []
    for s in range(subs):
        here = own if s == 0 else shift(own, "sub", s)
        for q in range(pairs):
            blocks_of_rows.append(here if q == 0 else shift(here, "pair", q))
    rows = jnp.concatenate(blocks_of_rows, axis=0)
    widened = rows[:, : 2 * NF].astype(jnp.float32)
    row_rate = rate_of(widened[:, :NF], widened[:, NF:])
    row_power = jnp.sum(jnp.square(row_rate.astype(jnp.float32)), axis=1, keepdims=True)

    running = None
    for place, steps in enumerate(arrivals):
        running = pair_tile(
            running, rows, row_power, coefs[place], col_gains[place], columns[steps]
        )

    partial = running.reshape(subs, pairs, piece, 2 * NF)
    held = partial[:, 0]
    for q in range(1, pairs):
        sent = partial[:, q].astype(jnp.bfloat16)
        held = held + shift(sent, "pair", -q).astype(jnp.float32)
    adjoint = held[0]
    for s in range(1, subs):
        adjoint = adjoint + shift(held[s].astype(jnp.bfloat16), "sub", -s).astype(jnp.float32)
    adjoint = adjoint.astype(jnp.bfloat16)

    gathered = jnp.zeros((levels * piece, 2 * NF), jnp.bfloat16)
    for steps in arrivals:
        arrived = adjoint if steps == 0 else shift(adjoint, "blk", steps)
        gathered = lax.dynamic_update_slice_in_dim(
            gathered, arrived, (level - steps) % levels * piece, 0
        )
    return (
        lax.dot_general(
            gathered, basis[:span], CONTRACT_LAST, preferred_element_type=jnp.float32
        )
        * (1.0 / math.sqrt(NF))
    ).astype(jnp.bfloat16)


def power_of(spec):
    wide = spec.astype(jnp.float32)
    rate = rate_of(wide[:, :NF], wide[:, NF:])
    return rate, jnp.sum(jnp.square(rate.astype(jnp.float32)), axis=1, keepdims=True)


def couple_kernel(row_count, col_count, *refs):
    row_refs = refs[:row_count]
    col_refs = refs[row_count : row_count + col_count]
    weight_ref, out_ref = refs[-2:]
    half = row_refs[0].shape[0] // 2
    row_model = jnp.concatenate([ref[:half] for ref in row_refs], axis=0)
    row_data = jnp.concatenate([ref[half:] for ref in row_refs], axis=0)
    row_power = jnp.concatenate([power_of(ref[:half])[1] for ref in row_refs], axis=0)
    models, datas, powers = [], [], []
    for ref in col_refs:
        rate, power = power_of(ref[:half])
        models.append(rate)
        powers.append(power)
        wide = ref[half:].astype(jnp.float32)
        datas.append(rate_of(wide[:, :NF], wide[:, NF:]))
    col_model = jnp.concatenate(models, axis=0)
    col_data = jnp.concatenate(datas, axis=0)
    powers = jnp.concatenate(powers, axis=0)
    width = powers.shape[0]
    diagonal = lax.broadcasted_iota(jnp.int32, (width, width), 0) == lax.broadcasted_iota(
        jnp.int32, (width, width), 1
    )
    col_power = jnp.sum(jnp.where(diagonal, powers, 0.0), axis=0, keepdims=True)
    cross = lax.dot_general(
        row_model, col_model, CONTRACT_LAST, preferred_element_type=jnp.float32
    ) - lax.dot_general(row_data, col_data, CONTRACT_LAST, preferred_element_type=jnp.float32)
    normalizer = 0.5 * (row_power + col_power) + epsilon
    coupling = (weight_ref[...] * cross / normalizer).astype(jnp.bfloat16)
    out_ref[...] = jnp.dot(coupling, col_model, preferred_element_type=jnp.float32)


def couple(rows, cols, weights):
    args = [*rows, *cols, weights]
    height, width = weights.shape
    return pl.pallas_call(
        functools.partial(couple_kernel, len(rows), len(cols)),
        in_specs=[pl.BlockSpec(memory_space=pltpu.VMEM)] * len(args),
        out_specs=pl.BlockSpec(memory_space=pltpu.VMEM),
        out_shape=jax.ShapeDtypeStruct((height, 2 * NF), jnp.float32),
        cost_estimate=pl.CostEstimate(
            flops=12 * height * width * NF,
            bytes_accessed=8 * (height + width) * NF,
            transcendentals=0,
        ),
        name="couple",
    )(*args)


def inner_body(synthetic, observed, station_weights, pair_mask):
    levels = lax.axis_size("blk")
    subs = lax.axis_size("sub")
    pairs = lax.axis_size("pair")
    level = lax.axis_index("blk")
    sub = lax.axis_index("sub")
    pair = lax.axis_index("pair")
    span = synthetic.shape[1]
    half = synthetic.shape[0] // 2
    per_half = levels // 2
    stations = station_weights.shape[0]
    piece = half // per_half
    side = level // 2
    inward, across, swapped = [(0, 1), (3, 2)], [(0, 2), (3, 1)], [(1, 2), (2, 1)]
    outward, beyond = [(1, 0), (2, 3)], [(1, 3), (2, 0)]

    def stations_of(which):
        return jnp.concatenate(
            [
                lax.dynamic_slice_in_dim(synthetic, which * half, half, 0),
                lax.dynamic_slice_in_dim(observed, which * half, half, 0),
            ],
            axis=0,
        )

    kept, sent = stations_of(side), stations_of(1 - side)
    near = lax.ppermute(kept, "blk", inward)
    middle = lax.ppermute(sent, "blk", swapped)
    far = lax.ppermute(sent, "blk", across)

    member = sub * pairs + pair
    hops = [(s, q) for s in range(subs) for q in range(pairs)]
    members = jnp.stack([(sub - s) % subs * pairs + (pair - q) % pairs for s, q in hops])
    within = jnp.arange(per_half, dtype=jnp.int32)
    row_pieces = member * levels + jnp.concatenate(
        [side * per_half + within, (1 - side) * per_half + within]
    )
    col_pieces = (members[:, None] * levels + side * per_half + within[None, :]).reshape(-1)
    gains = station_weights.astype(jnp.float32).reshape(-1, piece)
    link = jnp.maximum(pair_mask, pair_mask.T).astype(jnp.float32)
    active = link[row_pieces][:, col_pieces]
    weights = (
        4.0
        / math.sqrt(stations)
        * gains[row_pieces].reshape(-1, 1)
        * gains[col_pieces].reshape(1, -1)
        * jnp.repeat(jnp.repeat(active, piece, axis=0), piece, axis=1)
    )

    sources = [level, level ^ 1, levels - 1 - level, (level + 2) % levels]
    basis = make_basis(jnp.stack(sources).astype(jnp.int32) * span, span)
    total = None
    far, weights = lax.optimization_barrier((far, weights))
    for place, block in enumerate([kept, near, middle, far]):
        part = jnp.dot(
            block,
            basis[place * span : (place + 1) * span],
            preferred_element_type=jnp.float32,
        )
        total = part if total is None else total + part
    own = (total * (1.0 / math.sqrt(NT))).astype(jnp.bfloat16)

    other = lax.ppermute(own, "blk", swapped)
    cols = []
    for s, q in hops:
        if q == 0:
            here = own if s == 0 else shift(own, "sub", s)
        cols.append(here if q == 0 else shift(here, "pair", q))
    running = couple([own, other], cols, weights)

    received = lax.ppermute(running[half:].astype(jnp.bfloat16), "blk", swapped)
    adjoint = (running[:half] + received.astype(jnp.float32)).astype(jnp.bfloat16)
    first = lax.ppermute(adjoint, "blk", outward)
    second = lax.ppermute(adjoint, "blk", swapped)
    third = lax.ppermute(adjoint, "blk", beyond)
    is_inner = (level == 1) | (level == 2)
    mine = jnp.where(is_inner, adjoint, first)
    theirs = jnp.where(is_inner, second, third)
    gathered = jnp.concatenate(
        [jnp.where(side == 0, mine, theirs), jnp.where(side == 0, theirs, mine)], axis=0
    )
    return (
        lax.dot_general(
            gathered, basis[:span], CONTRACT_LAST, preferred_element_type=jnp.float32
        )
        * (1.0 / math.sqrt(NF))
    ).astype(jnp.bfloat16)


def shards(*args):
    body = inner_body if lax.axis_size("blk") == 4 else ring_body
    return body(*args)


def solution(mesh):
    placed = (
        P(("events", "sub", "pair"), "blk"),
        P(("events", "sub", "pair"), "blk"),
        P("events"),
        P("events", None),
    )
    return jax.shard_map(
        shards,
        mesh=mesh,
        in_specs=placed,
        out_specs=P(("events", "sub", "pair"), "blk"),
        check_vma=False,
    )
```

```python
import functools
import math

import jax
import jax.numpy as jnp
from jax import lax
from jax.experimental import pallas as pl
from jax.experimental.pallas import tpu as pltpu
from jax.sharding import PartitionSpec as P


NT = 4096
NF = 512
F_LO = 64

epsilon = 1e-06
CONTRACT_LAST = (((1,), (1,)), ((), ()))


def shift(value, axis, steps):
    count = lax.axis_size(axis)
    pairs = [(source, (source + steps) % count) for source in range(count)]
    return lax.ppermute(value, axis, pairs)


def sweep(count):
    order = []
    for near in range(1, count // 2 + 1):
        order.append(near)
        if (count - near) % count != near:
            order.append(count - near)
    return order


def cos_sin(samples):
    bins = F_LO + jnp.arange(NF, dtype=jnp.int32)
    phases = samples[:, None] * bins[None, :] % NT
    angles = phases.astype(jnp.float32) * (2.0 * math.pi / NT)
    return jnp.cos(angles), jnp.sin(angles)


def basis_kernel(per_step, low_rows, hc_ref, hs_ref, lc_ref, ls_ref, out_ref):
    step = pl.program_id(0)
    for h in range(per_step):
        hc = hc_ref[pl.ds(step * per_step + h, 1), :]
        hs = hs_ref[pl.ds(step * per_step + h, 1), :]
        lc = lc_ref[...]
        ls = ls_ref[...]
        rows = slice(h * low_rows, (h + 1) * low_rows)
        out_ref[rows, :NF] = (hc * lc - hs * ls).astype(jnp.bfloat16)
        out_ref[rows, NF:] = (-(hs * lc + hc * ls)).astype(jnp.bfloat16)


def make_basis(firsts, span):
    low_rows = math.gcd(span, 64)
    low_c, low_s = cos_sin(jnp.arange(low_rows, dtype=jnp.int32))
    highs = (firsts[:, None] + jnp.arange(0, span, low_rows, dtype=jnp.int32)[None, :]).reshape(-1)
    high_c, high_s = cos_sin(highs)
    per_step = math.gcd(highs.shape[0], 4)
    whole = lambda a: pl.BlockSpec(a.shape, lambda i: (0, 0))
    rows = highs.shape[0] * low_rows
    return pl.pallas_call(
        functools.partial(basis_kernel, per_step, low_rows),
        grid=(highs.shape[0] // per_step,),
        in_specs=[whole(high_c), whole(high_s), whole(low_c), whole(low_s)],
        out_specs=pl.BlockSpec((per_step * low_rows, 2 * NF), lambda i: (i, 0)),
        out_shape=jax.ShapeDtypeStruct((rows, 2 * NF), jnp.bfloat16),
        cost_estimate=pl.CostEstimate(
            flops=8 * rows * NF, bytes_accessed=4 * rows * NF, transcendentals=0
        ),
        name="basis",
    )(high_c, high_s, low_c, low_s)


def angular_row():
    bins = F_LO + lax.broadcasted_iota(jnp.int32, (1, NF), 1)
    return 2.0 * math.pi / NT * bins.astype(jnp.float32)


def rate_of(re, im):
    angular = angular_row()
    return jnp.concatenate([-angular * im, angular * re], axis=1).astype(jnp.bfloat16)


def tile_kernel(first, rows_ref, power_ref, coef_ref, gain_ref, col_ref, *rest):
    out_ref = rest[-1]
    col = col_ref[...].astype(jnp.float32)
    model_rate = rate_of(col[:, :NF], col[:, NF : 2 * NF])
    data_rate = rate_of(-col[:, 2 * NF : 3 * NF], -col[:, 3 * NF :])
    both = jnp.concatenate([model_rate, data_rate], axis=1)
    cross = lax.dot_general(
        rows_ref[...], both, CONTRACT_LAST, preferred_element_type=jnp.float32
    )
    col_power = lax.dot_general(
        jnp.ones((8, 2 * NF), jnp.float32),
        jnp.square(model_rate.astype(jnp.float32)),
        CONTRACT_LAST,
        precision=lax.Precision.HIGHEST,
        preferred_element_type=jnp.float32,
    )[0:1, :]
    normalizer = 0.5 * (power_ref[...] + col_power) + epsilon
    coupling = (coef_ref[...] * gain_ref[...] * cross / normalizer).astype(jnp.bfloat16)
    update = jnp.dot(coupling, model_rate, preferred_element_type=jnp.float32)
    if first:
        out_ref[...] = update
    else:
        out_ref[...] = rest[0][...] + update


def pair_tile(running, rows, row_power, coef, gain, col):
    args = [rows, row_power, coef, gain, col]
    aliases = {}
    if running is not None:
        aliases = {len(args): 0}
        args.append(running)
    height, width = rows.shape[0], col.shape[0]
    return pl.pallas_call(
        functools.partial(tile_kernel, running is None),
        in_specs=[pl.BlockSpec(memory_space=pltpu.VMEM)] * len(args),
        out_specs=pl.BlockSpec(memory_space=pltpu.VMEM),
        out_shape=jax.ShapeDtypeStruct((height, 2 * NF), jnp.float32),
        input_output_aliases=aliases,
        cost_estimate=pl.CostEstimate(
            flops=12 * height * width * NF,
            bytes_accessed=16 * height * NF,
            transcendentals=0,
        ),
        name="pair_tile",
    )(*args)


def ring_body(synthetic, observed, station_weights, pair_mask):
    levels = lax.axis_size("blk")
    subs = lax.axis_size("sub")
    pairs = lax.axis_size("pair")
    level = lax.axis_index("blk")
    sub = lax.axis_index("sub")
    pair = lax.axis_index("pair")
    span = synthetic.shape[1]
    piece = synthetic.shape[0] // levels
    stations = station_weights.shape[0]

    def owned_by(steps):
        owner = (level + steps) % levels
        return jnp.concatenate(
            [
                lax.dynamic_slice_in_dim(synthetic, owner * piece, piece, 0),
                lax.dynamic_slice_in_dim(observed, owner * piece, piece, 0),
            ],
            axis=0,
        )

    order = sweep(levels)
    blocks = {0: owned_by(0)}
    for steps in order:
        blocks[steps] = shift(owned_by(steps), "blk", steps)
    arrivals = [0] + order
    firsts = jnp.stack([(level - steps) % levels * span for steps in arrivals]).astype(jnp.int32)
    basis = make_basis(firsts, span)
    member = sub * pairs + pair
    members = jnp.stack(
        [
            (sub - s) % subs * pairs + (pair - q) % pairs
            for s in range(subs)
            for q in range(pairs)
        ]
    )
    gains = station_weights.astype(jnp.float32).reshape(-1, piece)
    link = jnp.maximum(pair_mask, pair_mask.T).astype(jnp.float32)
    row_pieces = members * levels + level
    row_gain = gains[row_pieces].reshape(-1, 1)
    row_link = link[row_pieces]
    factor = 4.0 / math.sqrt(stations)
    coefs, col_gains = [], []
    for steps in arrivals:
        column_piece = member * levels + (level - steps) % levels
        active = lax.dynamic_slice_in_dim(row_link, column_piece, 1, 1)
        coefs.append(factor * row_gain * jnp.repeat(active, piece, axis=0))
        col_gains.append(lax.dynamic_slice_in_dim(gains, column_piece, 1, 0))
    last = order[-1]
    blocks[last], coefs, col_gains = lax.optimization_barrier((blocks[last], coefs, col_gains))
    total = None
    for place, steps in enumerate(arrivals):
        part = jnp.dot(
            blocks[steps],
            basis[place * span : (place + 1) * span],
            preferred_element_type=jnp.float32,
        )
        total = part if total is None else total + part
    spec = (total * (1.0 / math.sqrt(NT))).astype(jnp.bfloat16)
    own = jnp.concatenate([spec[:piece], spec[piece:]], axis=1)

    columns = {0: own}
    for steps in order:
        columns[steps] = shift(own, "blk", steps)
    blocks_of_rows = []
    for s in range(subs):
        here = own if s == 0 else shift(own, "sub", s)
        for q in range(pairs):
            blocks_of_rows.append(here if q == 0 else shift(here, "pair", q))
    rows = jnp.concatenate(blocks_of_rows, axis=0)
    widened = rows[:, : 2 * NF].astype(jnp.float32)
    row_rate = rate_of(widened[:, :NF], widened[:, NF:])
    row_power = jnp.sum(jnp.square(row_rate.astype(jnp.float32)), axis=1, keepdims=True)

    running = None
    for place, steps in enumerate(arrivals):
        running = pair_tile(
            running, rows, row_power, coefs[place], col_gains[place], columns[steps]
        )

    partial = running.reshape(subs, pairs, piece, 2 * NF)
    held = partial[:, 0]
    for q in range(1, pairs):
        sent = partial[:, q].astype(jnp.bfloat16)
        held = held + shift(sent, "pair", -q).astype(jnp.float32)
    adjoint = held[0]
    for s in range(1, subs):
        adjoint = adjoint + shift(held[s].astype(jnp.bfloat16), "sub", -s).astype(jnp.float32)
    adjoint = adjoint.astype(jnp.bfloat16)

    gathered = jnp.zeros((levels * piece, 2 * NF), jnp.bfloat16)
    for steps in arrivals:
        arrived = adjoint if steps == 0 else shift(adjoint, "blk", steps)
        gathered = lax.dynamic_update_slice_in_dim(
            gathered, arrived, (level - steps) % levels * piece, 0
        )
    return (
        lax.dot_general(
            gathered, basis[:span], CONTRACT_LAST, preferred_element_type=jnp.float32
        )
        * (1.0 / math.sqrt(NF))
    ).astype(jnp.bfloat16)


def power_of(spec):
    wide = spec.astype(jnp.float32)
    rate = rate_of(wide[:, :NF], wide[:, NF:])
    return rate, jnp.sum(jnp.square(rate.astype(jnp.float32)), axis=1, keepdims=True)


def couple_kernel(row_count, col_count, *refs):
    row_refs = refs[:row_count]
    col_refs = refs[row_count : row_count + col_count]
    weight_ref, out_ref = refs[-2:]
    half = row_refs[0].shape[0] // 2
    row_model = jnp.concatenate([ref[:half] for ref in row_refs], axis=0)
    row_data = jnp.concatenate([ref[half:] for ref in row_refs], axis=0)
    row_power = jnp.concatenate([power_of(ref[:half])[1] for ref in row_refs], axis=0)
    models, datas, powers = [], [], []
    for ref in col_refs:
        rate, power = power_of(ref[:half])
        models.append(rate)
        powers.append(power)
        wide = ref[half:].astype(jnp.float32)
        datas.append(rate_of(wide[:, :NF], wide[:, NF:]))
    col_model = jnp.concatenate(models, axis=0)
    col_data = jnp.concatenate(datas, axis=0)
    powers = jnp.concatenate(powers, axis=0)
    width = powers.shape[0]
    diagonal = lax.broadcasted_iota(jnp.int32, (width, width), 0) == lax.broadcasted_iota(
        jnp.int32, (width, width), 1
    )
    col_power = jnp.sum(jnp.where(diagonal, powers, 0.0), axis=0, keepdims=True)
    cross = lax.dot_general(
        row_model, col_model, CONTRACT_LAST, preferred_element_type=jnp.float32
    ) - lax.dot_general(row_data, col_data, CONTRACT_LAST, preferred_element_type=jnp.float32)
    normalizer = 0.5 * (row_power + col_power) + epsilon
    coupling = (weight_ref[...] * cross / normalizer).astype(jnp.bfloat16)
    out_ref[...] = jnp.dot(
        coupling, col_model, preferred_element_type=jnp.float32
    ).astype(out_ref.dtype)


def couple(rows, cols, weights, kind):
    args = [*rows, *cols, weights]
    height, width = weights.shape
    return pl.pallas_call(
        functools.partial(couple_kernel, len(rows), len(cols)),
        in_specs=[pl.BlockSpec(memory_space=pltpu.VMEM)] * len(args),
        out_specs=pl.BlockSpec(memory_space=pltpu.VMEM),
        out_shape=jax.ShapeDtypeStruct((height, 2 * NF), kind),
        cost_estimate=pl.CostEstimate(
            flops=12 * height * width * NF,
            bytes_accessed=8 * (height + width) * NF,
            transcendentals=0,
        ),
        name="couple",
    )(*args)


def to_time_kernel(flag_ref, here_ref, there_ref, basis_ref, *rest):
    out_ref = rest[-1]
    adjoint = jnp.where(flag_ref[1] == 1, here_ref[...], there_ref[...])
    traces = lax.dot_general(
        adjoint, basis_ref[...], CONTRACT_LAST, preferred_element_type=jnp.float32
    )
    out_ref[...] = (traces * (1.0 / math.sqrt(NF))).astype(jnp.bfloat16)


def to_time(place, is_inner, here, there, basis, span, rows, before):
    half = here.shape[0]
    wide = math.gcd(span, 256)
    whole = pl.BlockSpec(here.shape, lambda j, flags: (0, 0))
    specs = [whole, whole, pl.BlockSpec((wide, 2 * NF), lambda j, flags: (j, 0))]
    args = [here, there, basis]
    aliases = {}
    if before is not None:
        specs.append(pl.BlockSpec(memory_space=pl.ANY))
        args.append(before)
        aliases = {4: 0}
    return pl.pallas_call(
        to_time_kernel,
        grid_spec=pltpu.PrefetchScalarGridSpec(
            num_scalar_prefetch=1,
            grid=(span // wide,),
            in_specs=specs,
            out_specs=pl.BlockSpec((half, wide), lambda j, flags: (flags[0], j)),
        ),
        out_shape=jax.ShapeDtypeStruct((rows, span), jnp.bfloat16),
        input_output_aliases=aliases,
        cost_estimate=pl.CostEstimate(
            flops=4 * half * span * NF, bytes_accessed=4 * span * NF, transcendentals=0
        ),
        name="to_time",
    )(jnp.stack([place, is_inner.astype(jnp.int32)]).astype(jnp.int32), *args)


def inner_body(synthetic, observed, station_weights, pair_mask):
    levels = lax.axis_size("blk")
    subs = lax.axis_size("sub")
    pairs = lax.axis_size("pair")
    level = lax.axis_index("blk")
    sub = lax.axis_index("sub")
    pair = lax.axis_index("pair")
    span = synthetic.shape[1]
    half = synthetic.shape[0] // 2
    per_half = levels // 2
    stations = station_weights.shape[0]
    piece = half // per_half
    side = level // 2
    inward, swapped, outward = [(0, 1), (3, 2)], [(1, 2), (2, 1)], [(1, 0), (2, 3)]

    def stations_of(which):
        return jnp.concatenate(
            [
                lax.dynamic_slice_in_dim(synthetic, which * half, half, 0),
                lax.dynamic_slice_in_dim(observed, which * half, half, 0),
            ],
            axis=0,
        )

    passed, kept = stations_of(1 - side), stations_of(side)
    near_passed = lax.ppermute(passed, "blk", inward)
    near_kept = lax.ppermute(kept, "blk", inward)

    member = sub * pairs + pair
    hops = [(s, q) for s in range(subs) for q in range(pairs)]
    members = jnp.stack([(sub - s) % subs * pairs + (pair - q) % pairs for s, q in hops])
    within = jnp.arange(per_half, dtype=jnp.int32)
    row_pieces = member * levels + jnp.concatenate(
        [side * per_half + within, (1 - side) * per_half + within]
    )
    col_pieces = (members[:, None] * levels + side * per_half + within[None, :]).reshape(-1)
    gains = station_weights.astype(jnp.float32).reshape(-1, piece)
    link = jnp.maximum(pair_mask, pair_mask.T).astype(jnp.float32)
    active = link[row_pieces][:, col_pieces]
    weights = (
        4.0
        / math.sqrt(stations)
        * gains[row_pieces].reshape(-1, 1)
        * gains[col_pieces].reshape(1, -1)
        * jnp.repeat(jnp.repeat(active, piece, axis=0), piece, axis=1)
    )
    own_weights, other_weights = weights[:half], weights[half:]

    basis = make_basis(jnp.stack([level, level ^ 1]).astype(jnp.int32) * span, span)
    scale = 1.0 / math.sqrt(NT)

    def transform(here, near):
        return (
            jnp.dot(here, basis[:span], preferred_element_type=jnp.float32)
            + jnp.dot(near, basis[span:], preferred_element_type=jnp.float32)
        ) * scale

    to_pass = transform(passed, near_passed).astype(jnp.bfloat16)
    kept_rest = lax.ppermute(to_pass, "blk", swapped)
    near_kept, own_weights, other_weights = lax.optimization_barrier(
        (near_kept, own_weights, other_weights)
    )
    kept_sum = transform(kept, near_kept)
    passed_rest = lax.ppermute(kept_sum.astype(jnp.bfloat16), "blk", swapped)
    own = (kept_sum + kept_rest.astype(jnp.float32)).astype(jnp.bfloat16)
    cols = []
    for s, q in hops:
        if q == 0:
            here = own if s == 0 else shift(own, "sub", s)
        cols.append(here if q == 0 else shift(here, "pair", q))
    other = (to_pass.astype(jnp.float32) + passed_rest.astype(jnp.float32)).astype(jnp.bfloat16)

    other_part = couple([other], cols, other_weights, jnp.bfloat16)
    own_rest = lax.ppermute(other_part, "blk", swapped)
    own_part = couple([own], cols, own_weights, jnp.bfloat16)
    other_rest = lax.ppermute(own_part, "blk", swapped)
    widen = lambda a: a.astype(jnp.float32)
    own_adjoint = (widen(own_part) + widen(own_rest)).astype(jnp.bfloat16)
    near_own = lax.ppermute(own_adjoint, "blk", outward)
    other_adjoint = (widen(other_part) + widen(other_rest)).astype(jnp.bfloat16)
    near_other = lax.ppermute(other_adjoint, "blk", outward)
    is_inner = (level == 1) | (level == 2)
    rows = synthetic.shape[0]
    traces = to_time(side, is_inner, own_adjoint, near_own, basis, span, rows, None)
    return to_time(1 - side, is_inner, other_adjoint, near_other, basis, span, rows, traces)


def shards(*args):
    body = inner_body if lax.axis_size("blk") == 4 else ring_body
    return body(*args)


def solution(mesh):
    placed = (
        P(("events", "sub", "pair"), "blk"),
        P(("events", "sub", "pair"), "blk"),
        P("events"),
        P("events", None),
    )
    return jax.shard_map(
        shards,
        mesh=mesh,
        in_specs=placed,
        out_specs=P(("events", "sub", "pair"), "blk"),
        check_vma=False,
    )
```

```python
import functools
import math

import jax
import jax.numpy as jnp
from jax import lax
from jax.experimental import pallas as pl
from jax.experimental.pallas import tpu as pltpu
from jax.sharding import PartitionSpec as P


NT = 4096
NF = 512
F_LO = 64

epsilon = 1e-06
CONTRACT_LAST = (((1,), (1,)), ((), ()))


def shift(value, axis, steps):
    count = lax.axis_size(axis)
    pairs = [(source, (source + steps) % count) for source in range(count)]
    return lax.ppermute(value, axis, pairs)


def sweep(count):
    order = []
    for near in range(1, count // 2 + 1):
        order.append(near)
        if (count - near) % count != near:
            order.append(count - near)
    return order


def cos_sin(samples):
    bins = F_LO + jnp.arange(NF, dtype=jnp.int32)
    phases = samples[:, None] * bins[None, :] % NT
    angles = phases.astype(jnp.float32) * (2.0 * math.pi / NT)
    return jnp.cos(angles), jnp.sin(angles)


def basis_kernel(per_step, low_rows, hc_ref, hs_ref, lc_ref, ls_ref, out_ref):
    step = pl.program_id(0)
    for h in range(per_step):
        hc = hc_ref[pl.ds(step * per_step + h, 1), :]
        hs = hs_ref[pl.ds(step * per_step + h, 1), :]
        lc = lc_ref[...]
        ls = ls_ref[...]
        rows = slice(h * low_rows, (h + 1) * low_rows)
        out_ref[rows, :NF] = (hc * lc - hs * ls).astype(jnp.bfloat16)
        out_ref[rows, NF:] = (-(hs * lc + hc * ls)).astype(jnp.bfloat16)


def make_basis(firsts, span):
    low_rows = math.gcd(span, 64)
    low_c, low_s = cos_sin(jnp.arange(low_rows, dtype=jnp.int32))
    highs = (firsts[:, None] + jnp.arange(0, span, low_rows, dtype=jnp.int32)[None, :]).reshape(-1)
    high_c, high_s = cos_sin(highs)
    per_step = math.gcd(highs.shape[0], 4)
    whole = lambda a: pl.BlockSpec(a.shape, lambda i: (0, 0))
    rows = highs.shape[0] * low_rows
    return pl.pallas_call(
        functools.partial(basis_kernel, per_step, low_rows),
        grid=(highs.shape[0] // per_step,),
        in_specs=[whole(high_c), whole(high_s), whole(low_c), whole(low_s)],
        out_specs=pl.BlockSpec((per_step * low_rows, 2 * NF), lambda i: (i, 0)),
        out_shape=jax.ShapeDtypeStruct((rows, 2 * NF), jnp.bfloat16),
        cost_estimate=pl.CostEstimate(
            flops=8 * rows * NF, bytes_accessed=4 * rows * NF, transcendentals=0
        ),
        compiler_params=pltpu.CompilerParams(vmem_limit_bytes=16 << 20),
        name="basis",
    )(high_c, high_s, low_c, low_s)


def angular_row():
    bins = F_LO + lax.broadcasted_iota(jnp.int32, (1, NF), 1)
    return 2.0 * math.pi / NT * bins.astype(jnp.float32)


def rate_of(re, im):
    angular = angular_row()
    return jnp.concatenate([-angular * im, angular * re], axis=1).astype(jnp.bfloat16)


def tile_kernel(first, rows_ref, power_ref, coef_ref, gain_ref, col_ref, *rest):
    out_ref = rest[-1]
    col = col_ref[...].astype(jnp.float32)
    model_rate = rate_of(col[:, :NF], col[:, NF : 2 * NF])
    data_rate = rate_of(-col[:, 2 * NF : 3 * NF], -col[:, 3 * NF :])
    both = jnp.concatenate([model_rate, data_rate], axis=1)
    cross = lax.dot_general(
        rows_ref[...], both, CONTRACT_LAST, preferred_element_type=jnp.float32
    )
    col_power = lax.dot_general(
        jnp.ones((8, 2 * NF), jnp.float32),
        jnp.square(model_rate.astype(jnp.float32)),
        CONTRACT_LAST,
        precision=lax.Precision.HIGHEST,
        preferred_element_type=jnp.float32,
    )[0:1, :]
    normalizer = 0.5 * (power_ref[...] + col_power) + epsilon
    coupling = (coef_ref[...] * gain_ref[...] * cross / normalizer).astype(jnp.bfloat16)
    update = jnp.dot(coupling, model_rate, preferred_element_type=jnp.float32)
    if first:
        out_ref[...] = update
    else:
        out_ref[...] = rest[0][...] + update


def pair_tile(running, rows, row_power, coef, gain, col):
    args = [rows, row_power, coef, gain, col]
    aliases = {}
    if running is not None:
        aliases = {len(args): 0}
        args.append(running)
    height, width = rows.shape[0], col.shape[0]
    return pl.pallas_call(
        functools.partial(tile_kernel, running is None),
        in_specs=[pl.BlockSpec(memory_space=pltpu.VMEM)] * len(args),
        out_specs=pl.BlockSpec(memory_space=pltpu.VMEM),
        out_shape=jax.ShapeDtypeStruct((height, 2 * NF), jnp.float32),
        input_output_aliases=aliases,
        cost_estimate=pl.CostEstimate(
            flops=12 * height * width * NF,
            bytes_accessed=16 * height * NF,
            transcendentals=0,
        ),
        name="pair_tile",
    )(*args)


def ring_body(synthetic, observed, station_weights, pair_mask):
    levels = lax.axis_size("blk")
    subs = lax.axis_size("sub")
    pairs = lax.axis_size("pair")
    level = lax.axis_index("blk")
    sub = lax.axis_index("sub")
    pair = lax.axis_index("pair")
    span = synthetic.shape[1]
    piece = synthetic.shape[0] // levels
    stations = station_weights.shape[0]

    def owned_by(steps):
        owner = (level + steps) % levels
        return jnp.concatenate(
            [
                lax.dynamic_slice_in_dim(synthetic, owner * piece, piece, 0),
                lax.dynamic_slice_in_dim(observed, owner * piece, piece, 0),
            ],
            axis=0,
        )

    order = sweep(levels)
    blocks = {0: owned_by(0)}
    for steps in order:
        blocks[steps] = shift(owned_by(steps), "blk", steps)
    arrivals = [0] + order
    firsts = jnp.stack([(level - steps) % levels * span for steps in arrivals]).astype(jnp.int32)
    basis = make_basis(firsts, span)
    member = sub * pairs + pair
    members = jnp.stack(
        [
            (sub - s) % subs * pairs + (pair - q) % pairs
            for s in range(subs)
            for q in range(pairs)
        ]
    )
    gains = station_weights.astype(jnp.float32).reshape(-1, piece)
    link = jnp.maximum(pair_mask, pair_mask.T).astype(jnp.float32)
    row_pieces = members * levels + level
    row_gain = gains[row_pieces].reshape(-1, 1)
    row_link = link[row_pieces]
    factor = 4.0 / math.sqrt(stations)
    coefs, col_gains = [], []
    for steps in arrivals:
        column_piece = member * levels + (level - steps) % levels
        active = lax.dynamic_slice_in_dim(row_link, column_piece, 1, 1)
        coefs.append(factor * row_gain * jnp.repeat(active, piece, axis=0))
        col_gains.append(lax.dynamic_slice_in_dim(gains, column_piece, 1, 0))
    last = order[-1]
    blocks[last], coefs, col_gains = lax.optimization_barrier((blocks[last], coefs, col_gains))
    total = None
    for place, steps in enumerate(arrivals):
        part = jnp.dot(
            blocks[steps],
            basis[place * span : (place + 1) * span],
            preferred_element_type=jnp.float32,
        )
        total = part if total is None else total + part
    spec = (total * (1.0 / math.sqrt(NT))).astype(jnp.bfloat16)
    own = jnp.concatenate([spec[:piece], spec[piece:]], axis=1)

    columns = {0: own}
    for steps in order:
        columns[steps] = shift(own, "blk", steps)
    blocks_of_rows = []
    for s in range(subs):
        here = own if s == 0 else shift(own, "sub", s)
        for q in range(pairs):
            blocks_of_rows.append(here if q == 0 else shift(here, "pair", q))
    rows = jnp.concatenate(blocks_of_rows, axis=0)
    widened = rows[:, : 2 * NF].astype(jnp.float32)
    row_rate = rate_of(widened[:, :NF], widened[:, NF:])
    row_power = jnp.sum(jnp.square(row_rate.astype(jnp.float32)), axis=1, keepdims=True)

    running = None
    for place, steps in enumerate(arrivals):
        running = pair_tile(
            running, rows, row_power, coefs[place], col_gains[place], columns[steps]
        )

    partial = running.reshape(subs, pairs, piece, 2 * NF)
    held = partial[:, 0]
    for q in range(1, pairs):
        sent = partial[:, q].astype(jnp.bfloat16)
        held = held + shift(sent, "pair", -q).astype(jnp.float32)
    adjoint = held[0]
    for s in range(1, subs):
        adjoint = adjoint + shift(held[s].astype(jnp.bfloat16), "sub", -s).astype(jnp.float32)
    adjoint = adjoint.astype(jnp.bfloat16)

    gathered = jnp.zeros((levels * piece, 2 * NF), jnp.bfloat16)
    for steps in arrivals:
        arrived = adjoint if steps == 0 else shift(adjoint, "blk", steps)
        gathered = lax.dynamic_update_slice_in_dim(
            gathered, arrived, (level - steps) % levels * piece, 0
        )
    return (
        lax.dot_general(
            gathered, basis[:span], CONTRACT_LAST, preferred_element_type=jnp.float32
        )
        * (1.0 / math.sqrt(NF))
    ).astype(jnp.bfloat16)


def power_of(spec):
    wide = spec.astype(jnp.float32)
    rate = rate_of(wide[:, :NF], wide[:, NF:])
    return rate, jnp.sum(jnp.square(rate.astype(jnp.float32)), axis=1, keepdims=True)


def planes(ref, piece):
    starts = range(0, ref.shape[0], 2 * piece)
    return tuple(
        jnp.concatenate([ref[at + off : at + off + piece] for at in starts], axis=0)
        for off in (0, piece)
    )


def couple_kernel(piece, row_count, col_count, *refs):
    row_refs = refs[:row_count]
    col_refs = refs[row_count : row_count + col_count]
    weight_ref, out_ref = refs[-2:]
    row_planes = [planes(ref, piece) for ref in row_refs]
    row_model = jnp.concatenate([model for model, _ in row_planes], axis=0)
    row_data = jnp.concatenate([data for _, data in row_planes], axis=0)
    row_power = power_of(row_model)[1]
    models, datas, powers = [], [], []
    for ref in col_refs:
        model, data = planes(ref, piece)
        rate, power = power_of(model)
        models.append(rate)
        powers.append(power)
        wide = data.astype(jnp.float32)
        datas.append(rate_of(wide[:, :NF], wide[:, NF:]))
    col_model = jnp.concatenate(models, axis=0)
    col_data = jnp.concatenate(datas, axis=0)
    powers = jnp.concatenate(powers, axis=0)
    width = powers.shape[0]
    diagonal = lax.broadcasted_iota(jnp.int32, (width, width), 0) == lax.broadcasted_iota(
        jnp.int32, (width, width), 1
    )
    col_power = jnp.sum(jnp.where(diagonal, powers, 0.0), axis=0, keepdims=True)
    cross = lax.dot_general(
        row_model, col_model, CONTRACT_LAST, preferred_element_type=jnp.float32
    ) - lax.dot_general(row_data, col_data, CONTRACT_LAST, preferred_element_type=jnp.float32)
    normalizer = 0.5 * (row_power + col_power) + epsilon
    coupling = (weight_ref[...] * cross / normalizer).astype(jnp.bfloat16)
    out_ref[...] = jnp.dot(
        coupling, col_model, preferred_element_type=jnp.float32
    ).astype(out_ref.dtype)


def couple(rows, cols, weights, piece):
    args = [*rows, *cols, weights]
    height, width = weights.shape
    return pl.pallas_call(
        functools.partial(couple_kernel, piece, len(rows), len(cols)),
        in_specs=[pl.BlockSpec(memory_space=pltpu.VMEM)] * len(args),
        out_specs=pl.BlockSpec(memory_space=pltpu.VMEM),
        out_shape=jax.ShapeDtypeStruct((height, 2 * NF), jnp.bfloat16),
        cost_estimate=pl.CostEstimate(
            flops=12 * height * width * NF,
            bytes_accessed=8 * (height + width) * NF,
            transcendentals=0,
        ),
        compiler_params=pltpu.CompilerParams(vmem_limit_bytes=16 << 20),
        name="couple",
    )(*args)


def to_time_kernel(flag_ref, here_ref, there_ref, basis_ref, *rest):
    out_ref = rest[-1]
    adjoint = jnp.where(flag_ref[1] == 1, here_ref[...], there_ref[...])
    traces = lax.dot_general(
        adjoint, basis_ref[...], CONTRACT_LAST, preferred_element_type=jnp.float32
    )
    out_ref[...] = (traces * (1.0 / math.sqrt(NF))).astype(jnp.bfloat16)


def to_time(place, is_inner, here, there, basis, span, rows, before):
    half = here.shape[0]
    wide = math.gcd(span, 256)
    whole = pl.BlockSpec(here.shape, lambda j, flags: (0, 0))
    specs = [whole, whole, pl.BlockSpec((wide, 2 * NF), lambda j, flags: (j, 0))]
    args = [here, there, basis]
    aliases = {}
    if before is not None:
        specs.append(pl.BlockSpec(memory_space=pl.ANY))
        args.append(before)
        aliases = {4: 0}
    return pl.pallas_call(
        to_time_kernel,
        grid_spec=pltpu.PrefetchScalarGridSpec(
            num_scalar_prefetch=1,
            grid=(span // wide,),
            in_specs=specs,
            out_specs=pl.BlockSpec((half, wide), lambda j, flags: (flags[0], j)),
        ),
        out_shape=jax.ShapeDtypeStruct((rows, span), jnp.bfloat16),
        input_output_aliases=aliases,
        cost_estimate=pl.CostEstimate(
            flops=4 * half * span * NF, bytes_accessed=4 * span * NF, transcendentals=0
        ),
        compiler_params=pltpu.CompilerParams(vmem_limit_bytes=12 << 20),
        name="to_time",
    )(jnp.stack([place, is_inner.astype(jnp.int32)]).astype(jnp.int32), *args)


def inner_body(synthetic, observed, station_weights, pair_mask):
    levels = lax.axis_size("blk")
    subs = lax.axis_size("sub")
    pairs = lax.axis_size("pair")
    level = lax.axis_index("blk")
    sub = lax.axis_index("sub")
    pair = lax.axis_index("pair")
    span = synthetic.shape[1]
    half = synthetic.shape[0] // 2
    per_half = levels // 2
    stations = station_weights.shape[0]
    piece = half // per_half
    side = level // 2
    inward, swapped, outward = [(0, 1), (3, 2)], [(1, 2), (2, 1)], [(1, 0), (2, 3)]

    def pieces_of(which):
        halves = [
            lax.dynamic_slice_in_dim(source, which * half, half, 0)
            for source in (synthetic, observed)
        ]
        return [
            jnp.concatenate([rows[at : at + piece] for rows in halves], axis=0)
            for at in range(0, half, piece)
        ]

    passed, kept = pieces_of(1 - side), jnp.concatenate(pieces_of(side), axis=0)
    near_passed = []
    for block in passed:
        near_passed.append(lax.ppermute(block, "blk", inward))
    near_kept = lax.ppermute(kept, "blk", inward)

    basis = make_basis(jnp.stack([level, level ^ 1]).astype(jnp.int32) * span, span)
    scale = 1.0 / math.sqrt(NT)

    def transform(here, near):
        return (
            jnp.dot(here, basis[:span], preferred_element_type=jnp.float32)
            + jnp.dot(near, basis[span:], preferred_element_type=jnp.float32)
        ) * scale

    to_pass, kept_rest = [], []
    for here, near in zip(passed, near_passed):
        to_pass.append(transform(here, near).astype(jnp.bfloat16))
        kept_rest.append(lax.ppermute(to_pass[-1], "blk", swapped))
    station_weights, pair_mask, kept_rest[0] = lax.optimization_barrier(
        (station_weights, pair_mask, kept_rest[0])
    )
    member = sub * pairs + pair
    hops = [(s, q) for s in range(subs) for q in range(pairs)]
    members = jnp.stack([(sub - s) % subs * pairs + (pair - q) % pairs for s, q in hops])
    within = jnp.arange(per_half, dtype=jnp.int32)
    row_pieces = member * levels + jnp.concatenate(
        [side * per_half + within, (1 - side) * per_half + within]
    )
    col_pieces = (members[:, None] * levels + side * per_half + within[None, :]).reshape(-1)
    gains = station_weights.astype(jnp.float32).reshape(-1, piece)
    link = jnp.maximum(pair_mask, pair_mask.T).astype(jnp.float32)
    active = link[row_pieces][:, col_pieces]
    weights = (
        4.0
        / math.sqrt(stations)
        * gains[row_pieces].reshape(-1, 1)
        * gains[col_pieces].reshape(1, -1)
        * jnp.repeat(jnp.repeat(active, piece, axis=0), piece, axis=1)
    )
    own_weights, other_weights = weights[:half], weights[half:]

    near_kept, own_weights, other_weights = lax.optimization_barrier(
        (near_kept, own_weights, other_weights)
    )
    kept_sum = transform(kept, near_kept)
    passed_rest = lax.ppermute(kept_sum.astype(jnp.bfloat16), "blk", swapped)
    kept_rest = jnp.concatenate(kept_rest, axis=0)
    own = (kept_sum + kept_rest.astype(jnp.float32)).astype(jnp.bfloat16)
    cols = []
    for s, q in hops:
        if q == 0:
            here = own if s == 0 else shift(own, "sub", s)
        cols.append(here if q == 0 else shift(here, "pair", q))
    to_pass = jnp.concatenate(to_pass, axis=0)
    other = (to_pass.astype(jnp.float32) + passed_rest.astype(jnp.float32)).astype(jnp.bfloat16)

    other_part = couple([other], cols, other_weights, piece)
    own_rest = lax.ppermute(other_part, "blk", swapped)
    own_part = couple([own], cols, own_weights, piece)
    other_rest = lax.ppermute(own_part, "blk", swapped)
    widen = lambda a: a.astype(jnp.float32)
    own_adjoint = (widen(own_part) + widen(own_rest)).astype(jnp.bfloat16)
    near_own = lax.ppermute(own_adjoint, "blk", outward)
    other_adjoint = (widen(other_part) + widen(other_rest)).astype(jnp.bfloat16)
    near_other = lax.ppermute(other_adjoint, "blk", outward)
    is_inner = (level == 1) | (level == 2)
    rows = synthetic.shape[0]
    traces = to_time(side, is_inner, own_adjoint, near_own, basis, span, rows, None)
    return to_time(1 - side, is_inner, other_adjoint, near_other, basis, span, rows, traces)


def shards(*args):
    body = inner_body if lax.axis_size("blk") == 4 else ring_body
    return body(*args)


def solution(mesh):
    placed = (
        P(("events", "sub", "pair"), "blk"),
        P(("events", "sub", "pair"), "blk"),
        P("events"),
        P("events", None),
    )
    return jax.shard_map(
        shards,
        mesh=mesh,
        in_specs=placed,
        out_specs=P(("events", "sub", "pair"), "blk"),
        check_vma=False,
    )
```

```python
import functools
import math

import jax
import jax.numpy as jnp
from jax import lax
from jax.experimental import pallas as pl
from jax.experimental.pallas import tpu as pltpu
from jax.sharding import PartitionSpec as P


NT = 4096
NF = 512
F_LO = 64

epsilon = 1e-06
CONTRACT_LAST = (((1,), (1,)), ((), ()))


def shift(value, axis, steps):
    count = lax.axis_size(axis)
    pairs = [(source, (source + steps) % count) for source in range(count)]
    return lax.ppermute(value, axis, pairs)


def sweep(count):
    order = []
    for near in range(1, count // 2 + 1):
        order.append(near)
        if (count - near) % count != near:
            order.append(count - near)
    return order


def cos_sin(samples):
    bins = F_LO + jnp.arange(NF, dtype=jnp.int32)
    phases = samples[:, None] * bins[None, :] % NT
    angles = phases.astype(jnp.float32) * (2.0 * math.pi / NT)
    return jnp.cos(angles), jnp.sin(angles)


def basis_kernel(per_step, low_rows, hc_ref, hs_ref, lc_ref, ls_ref, out_ref):
    step = pl.program_id(0)
    for h in range(per_step):
        hc = hc_ref[pl.ds(step * per_step + h, 1), :]
        hs = hs_ref[pl.ds(step * per_step + h, 1), :]
        lc = lc_ref[...]
        ls = ls_ref[...]
        rows = slice(h * low_rows, (h + 1) * low_rows)
        out_ref[rows, :NF] = (hc * lc - hs * ls).astype(jnp.bfloat16)
        out_ref[rows, NF:] = (-(hs * lc + hc * ls)).astype(jnp.bfloat16)


def make_basis(firsts, span):
    low_rows = math.gcd(span, 64)
    low_c, low_s = cos_sin(jnp.arange(low_rows, dtype=jnp.int32))
    highs = (firsts[:, None] + jnp.arange(0, span, low_rows, dtype=jnp.int32)[None, :]).reshape(-1)
    high_c, high_s = cos_sin(highs)
    per_step = math.gcd(highs.shape[0], 4)
    whole = lambda a: pl.BlockSpec(a.shape, lambda i: (0, 0))
    rows = highs.shape[0] * low_rows
    return pl.pallas_call(
        functools.partial(basis_kernel, per_step, low_rows),
        grid=(highs.shape[0] // per_step,),
        in_specs=[whole(high_c), whole(high_s), whole(low_c), whole(low_s)],
        out_specs=pl.BlockSpec((per_step * low_rows, 2 * NF), lambda i: (i, 0)),
        out_shape=jax.ShapeDtypeStruct((rows, 2 * NF), jnp.bfloat16),
        cost_estimate=pl.CostEstimate(
            flops=8 * rows * NF, bytes_accessed=4 * rows * NF, transcendentals=0
        ),
        compiler_params=pltpu.CompilerParams(vmem_limit_bytes=16 << 20),
        name="basis",
    )(high_c, high_s, low_c, low_s)


def angular_row():
    bins = F_LO + lax.broadcasted_iota(jnp.int32, (1, NF), 1)
    return 2.0 * math.pi / NT * bins.astype(jnp.float32)


def rate_of(re, im):
    angular = angular_row()
    return jnp.concatenate([-angular * im, angular * re], axis=1).astype(jnp.bfloat16)


def tile_kernel(first, rows_ref, power_ref, coef_ref, gain_ref, col_ref, *rest):
    out_ref = rest[-1]
    col = col_ref[...].astype(jnp.float32)
    model_rate = rate_of(col[:, :NF], col[:, NF : 2 * NF])
    data_rate = rate_of(-col[:, 2 * NF : 3 * NF], -col[:, 3 * NF :])
    both = jnp.concatenate([model_rate, data_rate], axis=1)
    cross = lax.dot_general(
        rows_ref[...], both, CONTRACT_LAST, preferred_element_type=jnp.float32
    )
    col_power = lax.dot_general(
        jnp.ones((8, 2 * NF), jnp.float32),
        jnp.square(model_rate.astype(jnp.float32)),
        CONTRACT_LAST,
        precision=lax.Precision.HIGHEST,
        preferred_element_type=jnp.float32,
    )[0:1, :]
    normalizer = 0.5 * (power_ref[...] + col_power) + epsilon
    coupling = (coef_ref[...] * gain_ref[...] * cross / normalizer).astype(jnp.bfloat16)
    update = jnp.dot(coupling, model_rate, preferred_element_type=jnp.float32)
    if first:
        out_ref[...] = update
    else:
        out_ref[...] = rest[0][...] + update


def pair_tile(running, rows, row_power, coef, gain, col):
    args = [rows, row_power, coef, gain, col]
    aliases = {}
    if running is not None:
        aliases = {len(args): 0}
        args.append(running)
    height, width = rows.shape[0], col.shape[0]
    return pl.pallas_call(
        functools.partial(tile_kernel, running is None),
        in_specs=[pl.BlockSpec(memory_space=pltpu.VMEM)] * len(args),
        out_specs=pl.BlockSpec(memory_space=pltpu.VMEM),
        out_shape=jax.ShapeDtypeStruct((height, 2 * NF), jnp.float32),
        input_output_aliases=aliases,
        cost_estimate=pl.CostEstimate(
            flops=12 * height * width * NF,
            bytes_accessed=16 * height * NF,
            transcendentals=0,
        ),
        name="pair_tile",
    )(*args)


def ring_body(synthetic, observed, station_weights, pair_mask):
    levels = lax.axis_size("blk")
    subs = lax.axis_size("sub")
    pairs = lax.axis_size("pair")
    level = lax.axis_index("blk")
    sub = lax.axis_index("sub")
    pair = lax.axis_index("pair")
    span = synthetic.shape[1]
    piece = synthetic.shape[0] // levels
    stations = station_weights.shape[0]

    def owned_by(steps):
        owner = (level + steps) % levels
        return jnp.concatenate(
            [
                lax.dynamic_slice_in_dim(synthetic, owner * piece, piece, 0),
                lax.dynamic_slice_in_dim(observed, owner * piece, piece, 0),
            ],
            axis=0,
        )

    order = sweep(levels)
    blocks = {0: owned_by(0)}
    for steps in order:
        blocks[steps] = shift(owned_by(steps), "blk", steps)
    arrivals = [0] + order
    firsts = jnp.stack([(level - steps) % levels * span for steps in arrivals]).astype(jnp.int32)
    basis = make_basis(firsts, span)
    member = sub * pairs + pair
    members = jnp.stack(
        [
            (sub - s) % subs * pairs + (pair - q) % pairs
            for s in range(subs)
            for q in range(pairs)
        ]
    )
    gains = station_weights.astype(jnp.float32).reshape(-1, piece)
    link = jnp.maximum(pair_mask, pair_mask.T).astype(jnp.float32)
    row_pieces = members * levels + level
    row_gain = gains[row_pieces].reshape(-1, 1)
    row_link = link[row_pieces]
    factor = 4.0 / math.sqrt(stations)
    coefs, col_gains = [], []
    for steps in arrivals:
        column_piece = member * levels + (level - steps) % levels
        active = lax.dynamic_slice_in_dim(row_link, column_piece, 1, 1)
        coefs.append(factor * row_gain * jnp.repeat(active, piece, axis=0))
        col_gains.append(lax.dynamic_slice_in_dim(gains, column_piece, 1, 0))
    last = order[-1]
    blocks[last], coefs, col_gains = lax.optimization_barrier((blocks[last], coefs, col_gains))
    total = None
    for place, steps in enumerate(arrivals):
        part = jnp.dot(
            blocks[steps],
            basis[place * span : (place + 1) * span],
            preferred_element_type=jnp.float32,
        )
        total = part if total is None else total + part
    spec = (total * (1.0 / math.sqrt(NT))).astype(jnp.bfloat16)
    own = jnp.concatenate([spec[:piece], spec[piece:]], axis=1)

    columns = {0: own}
    for steps in order:
        columns[steps] = shift(own, "blk", steps)
    blocks_of_rows = []
    for s in range(subs):
        here = own if s == 0 else shift(own, "sub", s)
        for q in range(pairs):
            blocks_of_rows.append(here if q == 0 else shift(here, "pair", q))
    rows = jnp.concatenate(blocks_of_rows, axis=0)
    widened = rows[:, : 2 * NF].astype(jnp.float32)
    row_rate = rate_of(widened[:, :NF], widened[:, NF:])
    row_power = jnp.sum(jnp.square(row_rate.astype(jnp.float32)), axis=1, keepdims=True)

    running = None
    for place, steps in enumerate(arrivals):
        running = pair_tile(
            running, rows, row_power, coefs[place], col_gains[place], columns[steps]
        )

    partial = running.reshape(subs, pairs, piece, 2 * NF)
    held = partial[:, 0]
    for q in range(1, pairs):
        sent = partial[:, q].astype(jnp.bfloat16)
        held = held + shift(sent, "pair", -q).astype(jnp.float32)
    adjoint = held[0]
    for s in range(1, subs):
        adjoint = adjoint + shift(held[s].astype(jnp.bfloat16), "sub", -s).astype(jnp.float32)
    adjoint = adjoint.astype(jnp.bfloat16)

    gathered = jnp.zeros((levels * piece, 2 * NF), jnp.bfloat16)
    for steps in arrivals:
        arrived = adjoint if steps == 0 else shift(adjoint, "blk", steps)
        gathered = lax.dynamic_update_slice_in_dim(
            gathered, arrived, (level - steps) % levels * piece, 0
        )
    return (
        lax.dot_general(
            gathered, basis[:span], CONTRACT_LAST, preferred_element_type=jnp.float32
        )
        * (1.0 / math.sqrt(NF))
    ).astype(jnp.bfloat16)


def power_of(spec):
    wide = spec.astype(jnp.float32)
    rate = rate_of(wide[:, :NF], wide[:, NF:])
    return rate, jnp.sum(jnp.square(rate.astype(jnp.float32)), axis=1, keepdims=True)


def planes(ref, piece):
    starts = range(0, ref.shape[0], 2 * piece)
    return tuple(
        jnp.concatenate([ref[at + off : at + off + piece] for at in starts], axis=0)
        for off in (0, piece)
    )


def couple_kernel(piece, row_count, col_count, *refs):
    row_refs = refs[:row_count]
    col_refs = refs[row_count : row_count + col_count]
    weight_ref, out_ref = refs[-2:]
    row_planes = [planes(ref, piece) for ref in row_refs]
    row_model = jnp.concatenate([model for model, _ in row_planes], axis=0)
    row_data = jnp.concatenate([data for _, data in row_planes], axis=0)
    row_power = power_of(row_model)[1]
    models, datas, powers = [], [], []
    for ref in col_refs:
        model, data = planes(ref, piece)
        rate, power = power_of(model)
        models.append(rate)
        powers.append(power)
        wide = data.astype(jnp.float32)
        datas.append(rate_of(wide[:, :NF], wide[:, NF:]))
    col_model = jnp.concatenate(models, axis=0)
    col_data = jnp.concatenate(datas, axis=0)
    powers = jnp.concatenate(powers, axis=0)
    width = powers.shape[0]
    diagonal = lax.broadcasted_iota(jnp.int32, (width, width), 0) == lax.broadcasted_iota(
        jnp.int32, (width, width), 1
    )
    col_power = jnp.sum(jnp.where(diagonal, powers, 0.0), axis=0, keepdims=True)
    cross = lax.dot_general(
        row_model, col_model, CONTRACT_LAST, preferred_element_type=jnp.float32
    ) - lax.dot_general(row_data, col_data, CONTRACT_LAST, preferred_element_type=jnp.float32)
    normalizer = 0.5 * (row_power + col_power) + epsilon
    coupling = (weight_ref[...] * cross / normalizer).astype(jnp.bfloat16)
    out_ref[...] = jnp.dot(
        coupling, col_model, preferred_element_type=jnp.float32
    ).astype(out_ref.dtype)


def couple(rows, cols, weights, piece):
    args = [*rows, *cols, weights]
    height, width = weights.shape
    return pl.pallas_call(
        functools.partial(couple_kernel, piece, len(rows), len(cols)),
        in_specs=[pl.BlockSpec(memory_space=pltpu.VMEM)] * len(args),
        out_specs=pl.BlockSpec(memory_space=pltpu.VMEM),
        out_shape=jax.ShapeDtypeStruct((height, 2 * NF), jnp.bfloat16),
        cost_estimate=pl.CostEstimate(
            flops=12 * height * width * NF,
            bytes_accessed=8 * (height + width) * NF,
            transcendentals=0,
        ),
        compiler_params=pltpu.CompilerParams(vmem_limit_bytes=16 << 20),
        name="couple",
    )(*args)


def to_time_kernel(flag_ref, here_ref, there_ref, basis_ref, *rest):
    out_ref = rest[-1]
    adjoint = jnp.where(flag_ref[1] == 1, here_ref[...], there_ref[...])
    traces = lax.dot_general(
        adjoint, basis_ref[...], CONTRACT_LAST, preferred_element_type=jnp.float32
    )
    out_ref[...] = (traces * (1.0 / math.sqrt(NF))).astype(jnp.bfloat16)


def to_time(place, is_inner, here, there, basis, span, rows, before):
    half = here.shape[0]
    wide = math.gcd(span, 256)
    whole = pl.BlockSpec(here.shape, lambda j, flags: (0, 0))
    specs = [whole, whole, pl.BlockSpec((wide, 2 * NF), lambda j, flags: (j, 0))]
    args = [here, there, basis]
    aliases = {}
    if before is not None:
        specs.append(pl.BlockSpec(memory_space=pl.ANY))
        args.append(before)
        aliases = {4: 0}
    return pl.pallas_call(
        to_time_kernel,
        grid_spec=pltpu.PrefetchScalarGridSpec(
            num_scalar_prefetch=1,
            grid=(span // wide,),
            in_specs=specs,
            out_specs=pl.BlockSpec((half, wide), lambda j, flags: (flags[0], j)),
        ),
        out_shape=jax.ShapeDtypeStruct((rows, span), jnp.bfloat16),
        input_output_aliases=aliases,
        cost_estimate=pl.CostEstimate(
            flops=4 * half * span * NF, bytes_accessed=4 * span * NF, transcendentals=0
        ),
        compiler_params=pltpu.CompilerParams(vmem_limit_bytes=12 << 20),
        name="to_time",
    )(jnp.stack([place, is_inner.astype(jnp.int32)]).astype(jnp.int32), *args)


VMEM = pl.BlockSpec(memory_space=pltpu.VMEM)


def two_bases_kernel(per_step, low_rows, *refs):
    lc_ref, ls_ref = refs[4:6]
    for high, out_ref in zip((refs[:2], refs[2:4]), refs[6:]):
        basis_kernel(per_step, low_rows, *high, lc_ref, ls_ref, out_ref)


def two_bases(first, second, span):
    low_rows = math.gcd(span, 64)
    tables = []
    for start in (first, second):
        tables += cos_sin(start + jnp.arange(0, span, low_rows, dtype=jnp.int32))
    tables += cos_sin(jnp.arange(low_rows, dtype=jnp.int32))
    per_step = math.gcd(span // low_rows, 4)
    block = pl.BlockSpec((per_step * low_rows, 2 * NF), lambda i: (i, 0))
    return pl.pallas_call(
        functools.partial(two_bases_kernel, per_step, low_rows),
        grid=(span // low_rows // per_step,),
        in_specs=[pl.BlockSpec(table.shape, lambda i: (0, 0)) for table in tables],
        out_specs=[block, block],
        out_shape=[jax.ShapeDtypeStruct((span, 2 * NF), jnp.bfloat16)] * 2,
        compiler_params=pltpu.CompilerParams(vmem_limit_bytes=12 << 20),
        cost_estimate=pl.CostEstimate(
            flops=16 * span * NF, bytes_accessed=8 * span * NF, transcendentals=0
        ),
        name="two_bases",
    )(*tables)


def own_parts_kernel(count, *refs):
    basis_ref = refs[count]
    for block_ref, out_ref in zip(refs[:count], refs[count + 1 :]):
        out_ref[...] = jnp.dot(
            block_ref[...], basis_ref[...], preferred_element_type=jnp.float32
        )


def own_parts(blocks, basis):
    rows, span = blocks[0].shape
    return pl.pallas_call(
        functools.partial(own_parts_kernel, len(blocks)),
        in_specs=[VMEM] * (len(blocks) + 1),
        out_specs=[VMEM] * len(blocks),
        out_shape=[jax.ShapeDtypeStruct((rows, 2 * NF), jnp.float32)] * len(blocks),
        compiler_params=pltpu.CompilerParams(vmem_limit_bytes=12 << 20),
        cost_estimate=pl.CostEstimate(
            flops=4 * len(blocks) * rows * span * NF,
            bytes_accessed=4 * span * NF,
            transcendentals=0,
        ),
        name="own_parts",
    )(*blocks, basis)


def sum_kernel(part_ref, near_ref, basis_ref, *rest):
    total = part_ref[...] + jnp.dot(
        near_ref[...], basis_ref[...], preferred_element_type=jnp.float32
    )
    total = total * (1.0 / math.sqrt(NT))
    if len(rest) == 3:
        rest_ref, own_ref, sum_ref = rest
        own_ref[...] = (total + rest_ref[...].astype(jnp.float32)).astype(jnp.bfloat16)
    else:
        sum_ref = rest[0]
    sum_ref[...] = total.astype(jnp.bfloat16)


def spectra(part, near, basis, others=None):
    rows, span = near.shape
    args = [part, near, basis] + ([] if others is None else [others])
    outs = 1 if others is None else 2
    return pl.pallas_call(
        sum_kernel,
        in_specs=[VMEM] * len(args),
        out_specs=[VMEM] * outs,
        out_shape=[jax.ShapeDtypeStruct((rows, 2 * NF), jnp.bfloat16)] * outs,
        compiler_params=pltpu.CompilerParams(vmem_limit_bytes=12 << 20),
        cost_estimate=pl.CostEstimate(
            flops=4 * rows * span * NF, bytes_accessed=4 * span * NF, transcendentals=0
        ),
        name="spectra",
    )(*args)


def inner_body(synthetic, observed, station_weights, pair_mask):
    levels = lax.axis_size("blk")
    subs = lax.axis_size("sub")
    pairs = lax.axis_size("pair")
    level = lax.axis_index("blk")
    sub = lax.axis_index("sub")
    pair = lax.axis_index("pair")
    span = synthetic.shape[1]
    half = synthetic.shape[0] // 2
    per_half = levels // 2
    stations = station_weights.shape[0]
    piece = half // per_half
    side = level // 2
    inward, swapped, outward = [(0, 1), (3, 2)], [(1, 2), (2, 1)], [(1, 0), (2, 3)]

    def pieces_of(which):
        return [
            jnp.concatenate(
                [
                    lax.dynamic_slice_in_dim(source, which * half + at, piece, 0)
                    for source in (synthetic, observed)
                ],
                axis=0,
            )
            for at in range(0, half, piece)
        ]

    passed, kept = pieces_of(1 - side), pieces_of(side)
    near_passed, near_kept = [], []
    for blocks, arrived in ((passed, near_passed), (kept, near_kept)):
        for block in blocks:
            arrived.append(lax.ppermute(block, "blk", inward))

    here_basis, near_basis = two_bases(level * span, (level ^ 1) * span, span)
    passed_parts = own_parts(passed, here_basis)
    kept_parts = own_parts(kept, here_basis)
    to_pass, kept_rest = [], []
    for place in range(per_half):
        (summed,) = spectra(passed_parts[place], near_passed[place], near_basis)
        to_pass.append(summed)
        kept_rest.append(lax.ppermute(summed, "blk", swapped))
    hops = [(s, q) for s in range(subs) for q in range(pairs)]
    own, passed_rest, cols = [], [], {}
    for place in range(per_half):
        whole, summed = spectra(
            kept_parts[place], near_kept[place], near_basis, kept_rest[place]
        )
        own.append(whole)
        for s, q in hops:
            if q == 0:
                cols[s, q, place] = whole if s == 0 else shift(whole, "sub", s)
            else:
                cols[s, q, place] = shift(cols[s, 0, place], "pair", q)
        passed_rest.append(lax.ppermute(summed, "blk", swapped))
    other = [
        (mine.astype(jnp.float32) + theirs.astype(jnp.float32)).astype(jnp.bfloat16)
        for mine, theirs in zip(to_pass, passed_rest)
    ]

    early = (subs - 1, 0, 0)
    station_weights, pair_mask, cols[early] = lax.optimization_barrier(
        (station_weights, pair_mask, cols[early])
    )
    member = sub * pairs + pair
    members = jnp.stack([(sub - s) % subs * pairs + (pair - q) % pairs for s, q in hops])
    within = jnp.arange(per_half, dtype=jnp.int32)
    row_pieces = member * levels + jnp.concatenate(
        [side * per_half + within, (1 - side) * per_half + within]
    )
    col_pieces = (members[:, None] * levels + side * per_half + within[None, :]).reshape(-1)
    gains = station_weights.astype(jnp.float32).reshape(-1, piece)
    link = jnp.maximum(pair_mask, pair_mask.T).astype(jnp.float32)
    active = link[row_pieces][:, col_pieces]
    weights = (
        4.0
        / math.sqrt(stations)
        * gains[row_pieces].reshape(-1, 1)
        * gains[col_pieces].reshape(1, -1)
        * jnp.repeat(jnp.repeat(active, piece, axis=0), piece, axis=1)
    )
    own_weights, other_weights = weights[:half], weights[half:]

    cols = [cols[s, q, place] for s, q in hops for place in range(per_half)]
    other_part = couple(other, cols, other_weights, piece)
    own_rest = lax.ppermute(other_part, "blk", swapped)
    own_part = couple(own, cols, own_weights, piece)
    other_rest = lax.ppermute(own_part, "blk", swapped)
    widen = lambda a: a.astype(jnp.float32)
    own_adjoint = (widen(own_part) + widen(own_rest)).astype(jnp.bfloat16)
    near_own = lax.ppermute(own_adjoint, "blk", outward)
    other_adjoint = (widen(other_part) + widen(other_rest)).astype(jnp.bfloat16)
    near_other = lax.ppermute(other_adjoint, "blk", outward)
    is_inner = (level == 1) | (level == 2)
    rows = synthetic.shape[0]
    traces = to_time(side, is_inner, own_adjoint, near_own, here_basis, span, rows, None)
    return to_time(1 - side, is_inner, other_adjoint, near_other, here_basis, span, rows, traces)


def shards(*args):
    body = inner_body if lax.axis_size("blk") == 4 else ring_body
    return body(*args)


def solution(mesh):
    placed = (
        P(("events", "sub", "pair"), "blk"),
        P(("events", "sub", "pair"), "blk"),
        P("events"),
        P("events", None),
    )
    return jax.shard_map(
        shards,
        mesh=mesh,
        in_specs=placed,
        out_specs=P(("events", "sub", "pair"), "blk"),
        check_vma=False,
    )
```

```python
import functools
import math

import jax
import jax.numpy as jnp
from jax import lax
from jax.experimental import pallas as pl
from jax.experimental.pallas import tpu as pltpu
from jax.sharding import PartitionSpec as P


NT = 4096
NF = 512
F_LO = 64

epsilon = 1e-06
CONTRACT_LAST = (((1,), (1,)), ((), ()))


def shift(value, axis, steps):
    count = lax.axis_size(axis)
    pairs = [(source, (source + steps) % count) for source in range(count)]
    return lax.ppermute(value, axis, pairs)


def sweep(count):
    order = []
    for near in range(1, count // 2 + 1):
        order.append(near)
        if (count - near) % count != near:
            order.append(count - near)
    return order


def cos_sin(samples):
    bins = F_LO + jnp.arange(NF, dtype=jnp.int32)
    phases = samples[:, None] * bins[None, :] % NT
    angles = phases.astype(jnp.float32) * (2.0 * math.pi / NT)
    return jnp.cos(angles), jnp.sin(angles)


def basis_kernel(per_step, low_rows, hc_ref, hs_ref, lc_ref, ls_ref, out_ref):
    step = pl.program_id(0)
    for h in range(per_step):
        hc = hc_ref[pl.ds(step * per_step + h, 1), :]
        hs = hs_ref[pl.ds(step * per_step + h, 1), :]
        lc = lc_ref[...]
        ls = ls_ref[...]
        rows = slice(h * low_rows, (h + 1) * low_rows)
        out_ref[rows, :NF] = (hc * lc - hs * ls).astype(jnp.bfloat16)
        out_ref[rows, NF:] = (-(hs * lc + hc * ls)).astype(jnp.bfloat16)


def make_basis(firsts, span):
    low_rows = math.gcd(span, 64)
    low_c, low_s = cos_sin(jnp.arange(low_rows, dtype=jnp.int32))
    highs = (firsts[:, None] + jnp.arange(0, span, low_rows, dtype=jnp.int32)[None, :]).reshape(-1)
    high_c, high_s = cos_sin(highs)
    per_step = math.gcd(highs.shape[0], 4)
    whole = lambda a: pl.BlockSpec(a.shape, lambda i: (0, 0))
    rows = highs.shape[0] * low_rows
    return pl.pallas_call(
        functools.partial(basis_kernel, per_step, low_rows),
        grid=(highs.shape[0] // per_step,),
        in_specs=[whole(high_c), whole(high_s), whole(low_c), whole(low_s)],
        out_specs=pl.BlockSpec((per_step * low_rows, 2 * NF), lambda i: (i, 0)),
        out_shape=jax.ShapeDtypeStruct((rows, 2 * NF), jnp.bfloat16),
        cost_estimate=pl.CostEstimate(
            flops=8 * rows * NF, bytes_accessed=4 * rows * NF, transcendentals=0
        ),
        compiler_params=pltpu.CompilerParams(vmem_limit_bytes=16 << 20),
        name="basis",
    )(high_c, high_s, low_c, low_s)


def angular_row():
    bins = F_LO + lax.broadcasted_iota(jnp.int32, (1, NF), 1)
    return 2.0 * math.pi / NT * bins.astype(jnp.float32)


def rate_of(re, im):
    angular = angular_row()
    return jnp.concatenate([-angular * im, angular * re], axis=1).astype(jnp.bfloat16)


def tile_kernel(first, rows_ref, power_ref, coef_ref, gain_ref, col_ref, *rest):
    out_ref = rest[-1]
    col = col_ref[...].astype(jnp.float32)
    model_rate = rate_of(col[:, :NF], col[:, NF : 2 * NF])
    data_rate = rate_of(-col[:, 2 * NF : 3 * NF], -col[:, 3 * NF :])
    both = jnp.concatenate([model_rate, data_rate], axis=1)
    cross = lax.dot_general(
        rows_ref[...], both, CONTRACT_LAST, preferred_element_type=jnp.float32
    )
    col_power = lax.dot_general(
        jnp.ones((8, 2 * NF), jnp.float32),
        jnp.square(model_rate.astype(jnp.float32)),
        CONTRACT_LAST,
        precision=lax.Precision.HIGHEST,
        preferred_element_type=jnp.float32,
    )[0:1, :]
    normalizer = 0.5 * (power_ref[...] + col_power) + epsilon
    coupling = (coef_ref[...] * gain_ref[...] * cross / normalizer).astype(jnp.bfloat16)
    update = jnp.dot(coupling, model_rate, preferred_element_type=jnp.float32)
    if first:
        out_ref[...] = update
    else:
        out_ref[...] = rest[0][...] + update


def pair_tile(running, rows, row_power, coef, gain, col):
    args = [rows, row_power, coef, gain, col]
    aliases = {}
    if running is not None:
        aliases = {len(args): 0}
        args.append(running)
    height, width = rows.shape[0], col.shape[0]
    return pl.pallas_call(
        functools.partial(tile_kernel, running is None),
        in_specs=[pl.BlockSpec(memory_space=pltpu.VMEM)] * len(args),
        out_specs=pl.BlockSpec(memory_space=pltpu.VMEM),
        out_shape=jax.ShapeDtypeStruct((height, 2 * NF), jnp.float32),
        input_output_aliases=aliases,
        cost_estimate=pl.CostEstimate(
            flops=12 * height * width * NF,
            bytes_accessed=16 * height * NF,
            transcendentals=0,
        ),
        name="pair_tile",
    )(*args)


def ring_body(synthetic, observed, station_weights, pair_mask):
    levels = lax.axis_size("blk")
    subs = lax.axis_size("sub")
    pairs = lax.axis_size("pair")
    level = lax.axis_index("blk")
    sub = lax.axis_index("sub")
    pair = lax.axis_index("pair")
    span = synthetic.shape[1]
    piece = synthetic.shape[0] // levels
    stations = station_weights.shape[0]

    def owned_by(steps):
        owner = (level + steps) % levels
        return jnp.concatenate(
            [
                lax.dynamic_slice_in_dim(synthetic, owner * piece, piece, 0),
                lax.dynamic_slice_in_dim(observed, owner * piece, piece, 0),
            ],
            axis=0,
        )

    order = sweep(levels)
    blocks = {0: owned_by(0)}
    for steps in order:
        blocks[steps] = shift(owned_by(steps), "blk", steps)
    arrivals = [0] + order
    firsts = jnp.stack([(level - steps) % levels * span for steps in arrivals]).astype(jnp.int32)
    basis = make_basis(firsts, span)
    member = sub * pairs + pair
    members = jnp.stack(
        [
            (sub - s) % subs * pairs + (pair - q) % pairs
            for s in range(subs)
            for q in range(pairs)
        ]
    )
    gains = station_weights.astype(jnp.float32).reshape(-1, piece)
    link = jnp.maximum(pair_mask, pair_mask.T).astype(jnp.float32)
    row_pieces = members * levels + level
    row_gain = gains[row_pieces].reshape(-1, 1)
    row_link = link[row_pieces]
    factor = 4.0 / math.sqrt(stations)
    coefs, col_gains = [], []
    for steps in arrivals:
        column_piece = member * levels + (level - steps) % levels
        active = lax.dynamic_slice_in_dim(row_link, column_piece, 1, 1)
        coefs.append(factor * row_gain * jnp.repeat(active, piece, axis=0))
        col_gains.append(lax.dynamic_slice_in_dim(gains, column_piece, 1, 0))
    last = order[-1]
    blocks[last], coefs, col_gains = lax.optimization_barrier((blocks[last], coefs, col_gains))
    total = None
    for place, steps in enumerate(arrivals):
        part = jnp.dot(
            blocks[steps],
            basis[place * span : (place + 1) * span],
            preferred_element_type=jnp.float32,
        )
        total = part if total is None else total + part
    spec = (total * (1.0 / math.sqrt(NT))).astype(jnp.bfloat16)
    own = jnp.concatenate([spec[:piece], spec[piece:]], axis=1)

    columns = {0: own}
    for steps in order:
        columns[steps] = shift(own, "blk", steps)
    blocks_of_rows = []
    for s in range(subs):
        here = own if s == 0 else shift(own, "sub", s)
        for q in range(pairs):
            blocks_of_rows.append(here if q == 0 else shift(here, "pair", q))
    rows = jnp.concatenate(blocks_of_rows, axis=0)
    widened = rows[:, : 2 * NF].astype(jnp.float32)
    row_rate = rate_of(widened[:, :NF], widened[:, NF:])
    row_power = jnp.sum(jnp.square(row_rate.astype(jnp.float32)), axis=1, keepdims=True)

    running = None
    for place, steps in enumerate(arrivals):
        running = pair_tile(
            running, rows, row_power, coefs[place], col_gains[place], columns[steps]
        )

    partial = running.reshape(subs, pairs, piece, 2 * NF)
    held = partial[:, 0]
    for q in range(1, pairs):
        sent = partial[:, q].astype(jnp.bfloat16)
        held = held + shift(sent, "pair", -q).astype(jnp.float32)
    adjoint = held[0]
    for s in range(1, subs):
        adjoint = adjoint + shift(held[s].astype(jnp.bfloat16), "sub", -s).astype(jnp.float32)
    adjoint = adjoint.astype(jnp.bfloat16)

    gathered = jnp.zeros((levels * piece, 2 * NF), jnp.bfloat16)
    for steps in arrivals:
        arrived = adjoint if steps == 0 else shift(adjoint, "blk", steps)
        gathered = lax.dynamic_update_slice_in_dim(
            gathered, arrived, (level - steps) % levels * piece, 0
        )
    return (
        lax.dot_general(
            gathered, basis[:span], CONTRACT_LAST, preferred_element_type=jnp.float32
        )
        * (1.0 / math.sqrt(NF))
    ).astype(jnp.bfloat16)


def power_of(spec):
    wide = spec.astype(jnp.float32)
    rate = rate_of(wide[:, :NF], wide[:, NF:])
    return rate, jnp.sum(jnp.square(rate.astype(jnp.float32)), axis=1, keepdims=True)


def couple_kernel(piece, row_count, col_count, *refs):
    row_refs = refs[:row_count]
    col_refs = refs[row_count : row_count + col_count]
    gain_ref, weight_ref, out_ref = refs[-3:]
    sums = row_count // (gain_ref.shape[1] // piece)
    row_models, row_datas = [], []
    for at in range(0, row_count, sums):
        block = row_refs[at][...]
        if sums == 2:
            block = (
                block.astype(jnp.float32) + row_refs[at + 1][...].astype(jnp.float32)
            ).astype(jnp.bfloat16)
        row_models.append(block[:piece])
        row_datas.append(block[piece:])
    row_model = jnp.concatenate(row_models, axis=0)
    row_data = jnp.concatenate(row_datas, axis=0)
    row_power = power_of(row_model)[1]
    models, datas, powers = [], [], []
    for ref in col_refs:
        rate, power = power_of(ref[:piece])
        models.append(rate)
        powers.append(power)
        wide = ref[piece:].astype(jnp.float32)
        datas.append(rate_of(wide[:, :NF], wide[:, NF:]))
    col_model = jnp.concatenate(models, axis=0)
    col_data = jnp.concatenate(datas, axis=0)
    powers = jnp.concatenate(powers, axis=0)

    def diagonal(width):
        return lax.broadcasted_iota(jnp.int32, (width, width), 0) == lax.broadcasted_iota(
            jnp.int32, (width, width), 1
        )

    col_power = jnp.sum(
        jnp.where(diagonal(powers.shape[0]), powers, 0.0), axis=0, keepdims=True
    )
    height = gain_ref.shape[1]
    row_gain = jnp.sum(
        jnp.where(diagonal(height), gain_ref[...], 0.0), axis=1, keepdims=True
    )
    cross = lax.dot_general(
        row_model, col_model, CONTRACT_LAST, preferred_element_type=jnp.float32
    ) - lax.dot_general(row_data, col_data, CONTRACT_LAST, preferred_element_type=jnp.float32)
    normalizer = 0.5 * (row_power + col_power) + epsilon
    ratio = row_gain * cross / normalizer
    coupling = jnp.concatenate(
        [
            (weight_ref[at : at + 1, :] * ratio[at * piece : (at + 1) * piece]).astype(
                jnp.bfloat16
            )
            for at in range(height // piece)
        ],
        axis=0,
    )
    out_ref[...] = jnp.dot(
        coupling, col_model, preferred_element_type=jnp.float32
    ).astype(out_ref.dtype)


def couple(rows, cols, gains, weights, piece):
    args = [*rows, *cols, gains, weights]
    height, width = gains.shape[1], weights.shape[1]
    return pl.pallas_call(
        functools.partial(couple_kernel, piece, len(rows), len(cols)),
        in_specs=[pl.BlockSpec(memory_space=pltpu.VMEM)] * len(args),
        out_specs=pl.BlockSpec(memory_space=pltpu.VMEM),
        out_shape=jax.ShapeDtypeStruct((height, 2 * NF), jnp.bfloat16),
        compiler_params=pltpu.CompilerParams(vmem_limit_bytes=16 << 20),
        cost_estimate=pl.CostEstimate(
            flops=12 * height * width * NF,
            bytes_accessed=8 * (height + width) * NF,
            transcendentals=0,
        ),
        name="couple",
    )(*args)


def to_time_kernel(flag_ref, here_ref, there_ref, basis_ref, *rest):
    out_ref = rest[-1]
    adjoint = jnp.where(flag_ref[1] == 1, here_ref[...], there_ref[...])
    traces = lax.dot_general(
        adjoint, basis_ref[...], CONTRACT_LAST, preferred_element_type=jnp.float32
    )
    out_ref[...] = (traces * (1.0 / math.sqrt(NF))).astype(jnp.bfloat16)


def to_time(place, is_inner, here, there, basis, span, rows, before):
    half = here.shape[0]
    wide = math.gcd(span, 512)
    whole = pl.BlockSpec(here.shape, lambda j, flags: (0, 0))
    specs = [whole, whole, pl.BlockSpec((wide, 2 * NF), lambda j, flags: (j, 0))]
    args = [here, there, basis]
    aliases = {}
    if before is not None:
        specs.append(pl.BlockSpec(memory_space=pl.ANY))
        args.append(before)
        aliases = {4: 0}
    return pl.pallas_call(
        to_time_kernel,
        grid_spec=pltpu.PrefetchScalarGridSpec(
            num_scalar_prefetch=1,
            grid=(span // wide,),
            in_specs=specs,
            out_specs=pl.BlockSpec((half, wide), lambda j, flags: (flags[0], j)),
        ),
        out_shape=jax.ShapeDtypeStruct((rows, span), jnp.bfloat16),
        input_output_aliases=aliases,
        cost_estimate=pl.CostEstimate(
            flops=4 * half * span * NF, bytes_accessed=4 * span * NF, transcendentals=0
        ),
        compiler_params=pltpu.CompilerParams(vmem_limit_bytes=12 << 20),
        name="to_time",
    )(jnp.stack([place, is_inner.astype(jnp.int32)]).astype(jnp.int32), *args)


VMEM = pl.BlockSpec(memory_space=pltpu.VMEM)


def two_bases_kernel(per_step, low_rows, *refs):
    lc_ref, ls_ref = refs[4:6]
    for high, out_ref in zip((refs[:2], refs[2:4]), refs[6:]):
        basis_kernel(per_step, low_rows, *high, lc_ref, ls_ref, out_ref)


def two_bases(first, second, span):
    low_rows = math.gcd(span, 64)
    tables = []
    for start in (first, second):
        tables += cos_sin(start + jnp.arange(0, span, low_rows, dtype=jnp.int32))
    tables += cos_sin(jnp.arange(low_rows, dtype=jnp.int32))
    per_step = math.gcd(span // low_rows, 4)
    block = pl.BlockSpec((per_step * low_rows, 2 * NF), lambda i: (i, 0))
    return pl.pallas_call(
        functools.partial(two_bases_kernel, per_step, low_rows),
        grid=(span // low_rows // per_step,),
        in_specs=[pl.BlockSpec(table.shape, lambda i: (0, 0)) for table in tables],
        out_specs=[block, block],
        out_shape=[jax.ShapeDtypeStruct((span, 2 * NF), jnp.bfloat16)] * 2,
        compiler_params=pltpu.CompilerParams(vmem_limit_bytes=12 << 20),
        cost_estimate=pl.CostEstimate(
            flops=16 * span * NF, bytes_accessed=8 * span * NF, transcendentals=0
        ),
        name="two_bases",
    )(*tables)


def own_parts_kernel(count, *refs):
    basis_ref = refs[count]
    for block_ref, out_ref in zip(refs[:count], refs[count + 1 :]):
        out_ref[...] = jnp.dot(
            block_ref[...], basis_ref[...], preferred_element_type=jnp.float32
        )


def own_parts(blocks, basis):
    rows, span = blocks[0].shape
    return pl.pallas_call(
        functools.partial(own_parts_kernel, len(blocks)),
        in_specs=[VMEM] * (len(blocks) + 1),
        out_specs=[VMEM] * len(blocks),
        out_shape=[jax.ShapeDtypeStruct((rows, 2 * NF), jnp.float32)] * len(blocks),
        compiler_params=pltpu.CompilerParams(vmem_limit_bytes=12 << 20),
        cost_estimate=pl.CostEstimate(
            flops=4 * len(blocks) * rows * span * NF,
            bytes_accessed=4 * span * NF,
            transcendentals=0,
        ),
        name="own_parts",
    )(*blocks, basis)


def sum_kernel(part_ref, near_ref, basis_ref, *rest):
    total = part_ref[...] + jnp.dot(
        near_ref[...], basis_ref[...], preferred_element_type=jnp.float32
    )
    total = total * (1.0 / math.sqrt(NT))
    if len(rest) == 3:
        rest_ref, own_ref, sum_ref = rest
        own_ref[...] = (total + rest_ref[...].astype(jnp.float32)).astype(jnp.bfloat16)
    else:
        sum_ref = rest[0]
    sum_ref[...] = total.astype(jnp.bfloat16)


def spectra(part, near, basis, others=None):
    rows, span = near.shape
    args = [part, near, basis] + ([] if others is None else [others])
    outs = 1 if others is None else 2
    return pl.pallas_call(
        sum_kernel,
        in_specs=[VMEM] * len(args),
        out_specs=[VMEM] * outs,
        out_shape=[jax.ShapeDtypeStruct((rows, 2 * NF), jnp.bfloat16)] * outs,
        compiler_params=pltpu.CompilerParams(vmem_limit_bytes=12 << 20),
        cost_estimate=pl.CostEstimate(
            flops=4 * rows * span * NF, bytes_accessed=4 * span * NF, transcendentals=0
        ),
        name="spectra",
    )(*args)


def inner_body(synthetic, observed, station_weights, pair_mask):
    levels = lax.axis_size("blk")
    subs = lax.axis_size("sub")
    pairs = lax.axis_size("pair")
    level = lax.axis_index("blk")
    sub = lax.axis_index("sub")
    pair = lax.axis_index("pair")
    span = synthetic.shape[1]
    half = synthetic.shape[0] // 2
    per_half = levels // 2
    stations = station_weights.shape[0]
    piece = half // per_half
    side = level // 2
    inward, swapped, outward = [(0, 1), (3, 2)], [(1, 2), (2, 1)], [(1, 0), (2, 3)]

    def pieces_of(which):
        return [
            jnp.concatenate(
                [
                    lax.dynamic_slice_in_dim(source, which * half + at, piece, 0)
                    for source in (synthetic, observed)
                ],
                axis=0,
            )
            for at in range(0, half, piece)
        ]

    passed, kept = pieces_of(1 - side), pieces_of(side)
    near_passed, near_kept = [], []
    for blocks, arrived in ((passed, near_passed), (kept, near_kept)):
        for block in blocks:
            arrived.append(lax.ppermute(block, "blk", inward))

    member = sub * pairs + pair
    hops = [(s, q) for s in range(subs) for q in range(pairs)]
    halves = [
        ((sub - s) % subs * pairs + (pair - q) % pairs) * 2 * half + side * half for s, q in hops
    ]
    gains = station_weights.astype(jnp.float32)
    col_gains = jnp.concatenate(
        [lax.dynamic_slice_in_dim(gains, start, half, 0) for start in halves]
    )[None, :]
    firsts = [member * 2 * half + which * half for which in (side, 1 - side)]
    own_gains, other_gains = [
        lax.dynamic_slice_in_dim(gains, start, half, 0)[None, :] for start in firsts
    ]
    link = jnp.maximum(pair_mask, pair_mask.T).astype(jnp.float32)
    link_rows = jnp.concatenate(
        [lax.dynamic_slice_in_dim(link, start // piece, per_half, 0) for start in firsts], axis=0
    )
    col_pieces = jnp.concatenate(
        [start + jnp.arange(half, dtype=jnp.int32) for start in halves]
    ) // piece
    chosen = jnp.arange(link.shape[0], dtype=jnp.int32)[:, None] == col_pieces[None, :]
    active = jnp.dot(
        link_rows, chosen.astype(jnp.float32), preferred_element_type=jnp.float32
    )
    weights = 4.0 / math.sqrt(stations) * col_gains * active
    here, own_gains, other_gains, weights = lax.optimization_barrier(
        (level, own_gains, other_gains, weights)
    )
    own_weights, other_weights = weights[:per_half], weights[per_half:]

    here_basis, near_basis = two_bases(here * span, (here ^ 1) * span, span)
    passed_parts = own_parts(passed, here_basis)
    kept_parts = own_parts(kept, here_basis)
    to_pass, kept_rest = [], []
    for place in range(per_half):
        (summed,) = spectra(passed_parts[place], near_passed[place], near_basis)
        to_pass.append(summed)
        kept_rest.append(lax.ppermute(summed, "blk", swapped))
    own, passed_rest, cols = [], [], {}
    for place in range(per_half):
        whole, summed = spectra(
            kept_parts[place], near_kept[place], near_basis, kept_rest[place]
        )
        own.append(whole)
        for s, q in hops:
            if q == 0:
                cols[s, q, place] = whole if s == 0 else shift(whole, "sub", s)
            else:
                cols[s, q, place] = shift(cols[s, 0, place], "pair", q)
        passed_rest.append(lax.ppermute(summed, "blk", swapped))
    cols = [cols[s, q, place] for s, q in hops for place in range(per_half)]
    other = [block for both in zip(to_pass, passed_rest) for block in both]
    other_part = couple(other, cols, other_gains, other_weights, piece)
    own_rest = lax.ppermute(other_part, "blk", swapped)
    own_part = couple(own, cols, own_gains, own_weights, piece)
    other_rest = lax.ppermute(own_part, "blk", swapped)
    widen = lambda a: a.astype(jnp.float32)
    own_adjoint = (widen(own_part) + widen(own_rest)).astype(jnp.bfloat16)
    near_own = lax.ppermute(own_adjoint, "blk", outward)
    other_adjoint = (widen(other_part) + widen(other_rest)).astype(jnp.bfloat16)
    near_other = lax.ppermute(other_adjoint, "blk", outward)
    is_inner = (level == 1) | (level == 2)
    rows = synthetic.shape[0]
    traces = to_time(side, is_inner, own_adjoint, near_own, here_basis, span, rows, None)
    return to_time(1 - side, is_inner, other_adjoint, near_other, here_basis, span, rows, traces)


def shards(*args):
    body = inner_body if lax.axis_size("blk") == 4 else ring_body
    return body(*args)


def solution(mesh):
    placed = (
        P(("events", "sub", "pair"), "blk"),
        P(("events", "sub", "pair"), "blk"),
        P("events"),
        P("events", None),
    )
    return jax.shard_map(
        shards,
        mesh=mesh,
        in_specs=placed,
        out_specs=P(("events", "sub", "pair"), "blk"),
        check_vma=False,
    )
```

```python
import functools
import math

import jax
import jax.numpy as jnp
from jax import lax
from jax.experimental import pallas as pl
from jax.experimental.pallas import tpu as pltpu
from jax.sharding import PartitionSpec as P


NT = 4096
NF = 512
F_LO = 64

epsilon = 1e-06
CONTRACT_LAST = (((1,), (1,)), ((), ()))


def shift(value, axis, steps):
    count = lax.axis_size(axis)
    pairs = [(source, (source + steps) % count) for source in range(count)]
    return lax.ppermute(value, axis, pairs)


def sweep(count):
    order = []
    for near in range(1, count // 2 + 1):
        order.append(near)
        if (count - near) % count != near:
            order.append(count - near)
    return order


def cos_sin(samples):
    bins = F_LO + jnp.arange(NF, dtype=jnp.int32)
    phases = samples[:, None] * bins[None, :] % NT
    angles = phases.astype(jnp.float32) * (2.0 * math.pi / NT)
    return jnp.cos(angles), jnp.sin(angles)


def basis_kernel(per_step, low_rows, hc_ref, hs_ref, lc_ref, ls_ref, out_ref):
    step = pl.program_id(0)
    for h in range(per_step):
        hc = hc_ref[pl.ds(step * per_step + h, 1), :]
        hs = hs_ref[pl.ds(step * per_step + h, 1), :]
        lc = lc_ref[...]
        ls = ls_ref[...]
        rows = slice(h * low_rows, (h + 1) * low_rows)
        out_ref[rows, :NF] = (hc * lc - hs * ls).astype(jnp.bfloat16)
        out_ref[rows, NF:] = (-(hs * lc + hc * ls)).astype(jnp.bfloat16)


def make_basis(firsts, span):
    low_rows = math.gcd(span, 64)
    low_c, low_s = cos_sin(jnp.arange(low_rows, dtype=jnp.int32))
    highs = (firsts[:, None] + jnp.arange(0, span, low_rows, dtype=jnp.int32)[None, :]).reshape(-1)
    high_c, high_s = cos_sin(highs)
    per_step = math.gcd(highs.shape[0], 4)
    whole = lambda a: pl.BlockSpec(a.shape, lambda i: (0, 0))
    rows = highs.shape[0] * low_rows
    return pl.pallas_call(
        functools.partial(basis_kernel, per_step, low_rows),
        grid=(highs.shape[0] // per_step,),
        in_specs=[whole(high_c), whole(high_s), whole(low_c), whole(low_s)],
        out_specs=pl.BlockSpec((per_step * low_rows, 2 * NF), lambda i: (i, 0)),
        out_shape=jax.ShapeDtypeStruct((rows, 2 * NF), jnp.bfloat16),
        cost_estimate=pl.CostEstimate(
            flops=8 * rows * NF, bytes_accessed=4 * rows * NF, transcendentals=0
        ),
        compiler_params=pltpu.CompilerParams(vmem_limit_bytes=16 << 20),
        name="basis",
    )(high_c, high_s, low_c, low_s)


def angular_row():
    bins = F_LO + lax.broadcasted_iota(jnp.int32, (1, NF), 1)
    return 2.0 * math.pi / NT * bins.astype(jnp.float32)


def rate_of(re, im):
    angular = angular_row()
    return jnp.concatenate([-angular * im, angular * re], axis=1).astype(jnp.bfloat16)


def tile_kernel(first, rows_ref, power_ref, coef_ref, gain_ref, col_ref, *rest):
    out_ref = rest[-1]
    col = col_ref[...].astype(jnp.float32)
    model_rate = rate_of(col[:, :NF], col[:, NF : 2 * NF])
    data_rate = rate_of(-col[:, 2 * NF : 3 * NF], -col[:, 3 * NF :])
    both = jnp.concatenate([model_rate, data_rate], axis=1)
    cross = lax.dot_general(
        rows_ref[...], both, CONTRACT_LAST, preferred_element_type=jnp.float32
    )
    col_power = lax.dot_general(
        jnp.ones((8, 2 * NF), jnp.float32),
        jnp.square(model_rate.astype(jnp.float32)),
        CONTRACT_LAST,
        precision=lax.Precision.HIGHEST,
        preferred_element_type=jnp.float32,
    )[0:1, :]
    normalizer = 0.5 * (power_ref[...] + col_power) + epsilon
    coupling = (coef_ref[...] * gain_ref[...] * cross / normalizer).astype(jnp.bfloat16)
    update = jnp.dot(coupling, model_rate, preferred_element_type=jnp.float32)
    if first:
        out_ref[...] = update
    else:
        out_ref[...] = rest[0][...] + update


def pair_tile(running, rows, row_power, coef, gain, col):
    args = [rows, row_power, coef, gain, col]
    aliases = {}
    if running is not None:
        aliases = {len(args): 0}
        args.append(running)
    height, width = rows.shape[0], col.shape[0]
    return pl.pallas_call(
        functools.partial(tile_kernel, running is None),
        in_specs=[pl.BlockSpec(memory_space=pltpu.VMEM)] * len(args),
        out_specs=pl.BlockSpec(memory_space=pltpu.VMEM),
        out_shape=jax.ShapeDtypeStruct((height, 2 * NF), jnp.float32),
        input_output_aliases=aliases,
        cost_estimate=pl.CostEstimate(
            flops=12 * height * width * NF,
            bytes_accessed=16 * height * NF,
            transcendentals=0,
        ),
        name="pair_tile",
    )(*args)


def ring_body(synthetic, observed, station_weights, pair_mask):
    levels = lax.axis_size("blk")
    subs = lax.axis_size("sub")
    pairs = lax.axis_size("pair")
    level = lax.axis_index("blk")
    sub = lax.axis_index("sub")
    pair = lax.axis_index("pair")
    span = synthetic.shape[1]
    piece = synthetic.shape[0] // levels
    stations = station_weights.shape[0]

    def owned_by(steps):
        owner = (level + steps) % levels
        return jnp.concatenate(
            [
                lax.dynamic_slice_in_dim(synthetic, owner * piece, piece, 0),
                lax.dynamic_slice_in_dim(observed, owner * piece, piece, 0),
            ],
            axis=0,
        )

    order = sweep(levels)
    blocks = {0: owned_by(0)}
    for steps in order:
        blocks[steps] = shift(owned_by(steps), "blk", steps)
    arrivals = [0] + order
    firsts = jnp.stack([(level - steps) % levels * span for steps in arrivals]).astype(jnp.int32)
    basis = make_basis(firsts, span)
    member = sub * pairs + pair
    members = jnp.stack(
        [
            (sub - s) % subs * pairs + (pair - q) % pairs
            for s in range(subs)
            for q in range(pairs)
        ]
    )
    gains = station_weights.astype(jnp.float32).reshape(-1, piece)
    link = jnp.maximum(pair_mask, pair_mask.T).astype(jnp.float32)
    row_pieces = members * levels + level
    row_gain = gains[row_pieces].reshape(-1, 1)
    row_link = link[row_pieces]
    factor = 4.0 / math.sqrt(stations)
    coefs, col_gains = [], []
    for steps in arrivals:
        column_piece = member * levels + (level - steps) % levels
        active = lax.dynamic_slice_in_dim(row_link, column_piece, 1, 1)
        coefs.append(factor * row_gain * jnp.repeat(active, piece, axis=0))
        col_gains.append(lax.dynamic_slice_in_dim(gains, column_piece, 1, 0))
    last = order[-1]
    blocks[last], coefs, col_gains = lax.optimization_barrier((blocks[last], coefs, col_gains))
    total = None
    for place, steps in enumerate(arrivals):
        part = jnp.dot(
            blocks[steps],
            basis[place * span : (place + 1) * span],
            preferred_element_type=jnp.float32,
        )
        total = part if total is None else total + part
    spec = (total * (1.0 / math.sqrt(NT))).astype(jnp.bfloat16)
    own = jnp.concatenate([spec[:piece], spec[piece:]], axis=1)

    columns = {0: own}
    for steps in order:
        columns[steps] = shift(own, "blk", steps)
    blocks_of_rows = []
    for s in range(subs):
        here = own if s == 0 else shift(own, "sub", s)
        for q in range(pairs):
            blocks_of_rows.append(here if q == 0 else shift(here, "pair", q))
    rows = jnp.concatenate(blocks_of_rows, axis=0)
    widened = rows[:, : 2 * NF].astype(jnp.float32)
    row_rate = rate_of(widened[:, :NF], widened[:, NF:])
    row_power = jnp.sum(jnp.square(row_rate.astype(jnp.float32)), axis=1, keepdims=True)

    running = None
    for place, steps in enumerate(arrivals):
        running = pair_tile(
            running, rows, row_power, coefs[place], col_gains[place], columns[steps]
        )

    partial = running.reshape(subs, pairs, piece, 2 * NF)
    held = partial[:, 0]
    for q in range(1, pairs):
        sent = partial[:, q].astype(jnp.bfloat16)
        held = held + shift(sent, "pair", -q).astype(jnp.float32)
    adjoint = held[0]
    for s in range(1, subs):
        adjoint = adjoint + shift(held[s].astype(jnp.bfloat16), "sub", -s).astype(jnp.float32)
    adjoint = adjoint.astype(jnp.bfloat16)

    gathered = jnp.zeros((levels * piece, 2 * NF), jnp.bfloat16)
    for steps in arrivals:
        arrived = adjoint if steps == 0 else shift(adjoint, "blk", steps)
        gathered = lax.dynamic_update_slice_in_dim(
            gathered, arrived, (level - steps) % levels * piece, 0
        )
    return (
        lax.dot_general(
            gathered, basis[:span], CONTRACT_LAST, preferred_element_type=jnp.float32
        )
        * (1.0 / math.sqrt(NF))
    ).astype(jnp.bfloat16)


def power_of(spec):
    wide = spec.astype(jnp.float32)
    rate = rate_of(wide[:, :NF], wide[:, NF:])
    return rate, jnp.sum(jnp.square(rate.astype(jnp.float32)), axis=1, keepdims=True)


def couple_kernel(piece, row_count, col_count, *refs):
    row_refs = refs[:row_count]
    col_refs = refs[row_count : row_count + col_count]
    gain_ref, weight_ref, out_ref = refs[-3:]
    sums = row_count // (gain_ref.shape[1] // piece)
    row_models, row_datas = [], []
    for at in range(0, row_count, sums):
        block = row_refs[at][...]
        if sums == 2:
            block = (
                block.astype(jnp.float32) + row_refs[at + 1][...].astype(jnp.float32)
            ).astype(jnp.bfloat16)
        row_models.append(block[:piece])
        row_datas.append(block[piece:])
    row_model = jnp.concatenate(row_models, axis=0)
    row_data = jnp.concatenate(row_datas, axis=0)
    row_power = power_of(row_model)[1]
    models, datas, powers = [], [], []
    for ref in col_refs:
        rate, power = power_of(ref[:piece])
        models.append(rate)
        powers.append(power)
        wide = ref[piece:].astype(jnp.float32)
        datas.append(rate_of(wide[:, :NF], wide[:, NF:]))
    col_model = jnp.concatenate(models, axis=0)
    col_data = jnp.concatenate(datas, axis=0)
    powers = jnp.concatenate(powers, axis=0)

    def diagonal(width):
        return lax.broadcasted_iota(jnp.int32, (width, width), 0) == lax.broadcasted_iota(
            jnp.int32, (width, width), 1
        )

    col_power = jnp.sum(
        jnp.where(diagonal(powers.shape[0]), powers, 0.0), axis=0, keepdims=True
    )
    height = gain_ref.shape[1]
    row_gain = jnp.sum(
        jnp.where(diagonal(height), gain_ref[...], 0.0), axis=1, keepdims=True
    )
    cross = lax.dot_general(
        row_model, col_model, CONTRACT_LAST, preferred_element_type=jnp.float32
    ) - lax.dot_general(row_data, col_data, CONTRACT_LAST, preferred_element_type=jnp.float32)
    normalizer = 0.5 * (row_power + col_power) + epsilon
    ratio = row_gain * cross / normalizer
    coupling = jnp.concatenate(
        [
            (weight_ref[at : at + 1, :] * ratio[at * piece : (at + 1) * piece]).astype(
                jnp.bfloat16
            )
            for at in range(height // piece)
        ],
        axis=0,
    )
    out_ref[...] = jnp.dot(
        coupling, col_model, preferred_element_type=jnp.float32
    ).astype(out_ref.dtype)


def couple(rows, cols, gains, weights, piece):
    args = [*rows, *cols, gains, weights]
    height, width = gains.shape[1], weights.shape[1]
    return pl.pallas_call(
        functools.partial(couple_kernel, piece, len(rows), len(cols)),
        in_specs=[pl.BlockSpec(memory_space=pltpu.VMEM)] * len(args),
        out_specs=pl.BlockSpec(memory_space=pltpu.VMEM),
        out_shape=jax.ShapeDtypeStruct((height, 2 * NF), jnp.bfloat16),
        compiler_params=pltpu.CompilerParams(vmem_limit_bytes=16 << 20),
        cost_estimate=pl.CostEstimate(
            flops=12 * height * width * NF,
            bytes_accessed=8 * (height + width) * NF,
            transcendentals=0,
        ),
        name="couple",
    )(*args)


def to_time_kernel(flag_ref, here_ref, there_ref, basis_ref, *rest):
    out_ref = rest[-1]
    adjoint = jnp.where(flag_ref[1] == 1, here_ref[...], there_ref[...])
    traces = lax.dot_general(
        adjoint, basis_ref[...], CONTRACT_LAST, preferred_element_type=jnp.float32
    )
    out_ref[...] = (traces * (1.0 / math.sqrt(NF))).astype(jnp.bfloat16)


def to_time(place, is_inner, here, there, basis, span, rows, before):
    half = here.shape[0]
    wide = span
    whole = pl.BlockSpec(here.shape, lambda j, flags: (0, 0))
    specs = [whole, whole, pl.BlockSpec((wide, 2 * NF), lambda j, flags: (j, 0))]
    args = [here, there, basis]
    aliases = {}
    if before is not None:
        specs.append(pl.BlockSpec(memory_space=pl.ANY))
        args.append(before)
        aliases = {4: 0}
    return pl.pallas_call(
        to_time_kernel,
        grid_spec=pltpu.PrefetchScalarGridSpec(
            num_scalar_prefetch=1,
            grid=(span // wide,),
            in_specs=specs,
            out_specs=pl.BlockSpec((half, wide), lambda j, flags: (flags[0], j)),
        ),
        out_shape=jax.ShapeDtypeStruct((rows, span), jnp.bfloat16),
        input_output_aliases=aliases,
        cost_estimate=pl.CostEstimate(
            flops=4 * half * span * NF, bytes_accessed=4 * span * NF, transcendentals=0
        ),
        compiler_params=pltpu.CompilerParams(vmem_limit_bytes=12 << 20),
        name="to_time",
    )(jnp.stack([place, is_inner.astype(jnp.int32)]).astype(jnp.int32), *args)


VMEM = pl.BlockSpec(memory_space=pltpu.VMEM)


def two_bases_kernel(per_step, low_rows, *refs):
    lc_ref, ls_ref = refs[4:6]
    for high, out_ref in zip((refs[:2], refs[2:4]), refs[6:]):
        basis_kernel(per_step, low_rows, *high, lc_ref, ls_ref, out_ref)


def two_bases(first, second, span):
    low_rows = math.gcd(span, 64)
    tables = []
    for start in (first, second):
        tables += cos_sin(start + jnp.arange(0, span, low_rows, dtype=jnp.int32))
    tables += cos_sin(jnp.arange(low_rows, dtype=jnp.int32))
    per_step = math.gcd(span // low_rows, 4)
    block = pl.BlockSpec((per_step * low_rows, 2 * NF), lambda i: (i, 0))
    return pl.pallas_call(
        functools.partial(two_bases_kernel, per_step, low_rows),
        grid=(span // low_rows // per_step,),
        in_specs=[pl.BlockSpec(table.shape, lambda i: (0, 0)) for table in tables],
        out_specs=[block, block],
        out_shape=[jax.ShapeDtypeStruct((span, 2 * NF), jnp.bfloat16)] * 2,
        compiler_params=pltpu.CompilerParams(vmem_limit_bytes=12 << 20),
        cost_estimate=pl.CostEstimate(
            flops=16 * span * NF, bytes_accessed=8 * span * NF, transcendentals=0
        ),
        name="two_bases",
    )(*tables)


def own_parts_kernel(count, *refs):
    basis_ref = refs[count]
    for block_ref, out_ref in zip(refs[:count], refs[count + 1 :]):
        out_ref[...] = jnp.dot(
            block_ref[...], basis_ref[...], preferred_element_type=jnp.float32
        )


def own_parts(blocks, basis):
    rows, span = blocks[0].shape
    return pl.pallas_call(
        functools.partial(own_parts_kernel, len(blocks)),
        in_specs=[VMEM] * (len(blocks) + 1),
        out_specs=[VMEM] * len(blocks),
        out_shape=[jax.ShapeDtypeStruct((rows, 2 * NF), jnp.float32)] * len(blocks),
        compiler_params=pltpu.CompilerParams(vmem_limit_bytes=12 << 20),
        cost_estimate=pl.CostEstimate(
            flops=4 * len(blocks) * rows * span * NF,
            bytes_accessed=4 * span * NF,
            transcendentals=0,
        ),
        name="own_parts",
    )(*blocks, basis)


def sum_kernel(part_ref, near_ref, basis_ref, *rest):
    total = part_ref[...] + jnp.dot(
        near_ref[...], basis_ref[...], preferred_element_type=jnp.float32
    )
    total = total * (1.0 / math.sqrt(NT))
    if len(rest) == 3:
        rest_ref, own_ref, sum_ref = rest
        own_ref[...] = (total + rest_ref[...].astype(jnp.float32)).astype(jnp.bfloat16)
    else:
        sum_ref = rest[0]
    sum_ref[...] = total.astype(jnp.bfloat16)


def spectra(part, near, basis, others=None):
    rows, span = near.shape
    args = [part, near, basis] + ([] if others is None else [others])
    outs = 1 if others is None else 2
    return pl.pallas_call(
        sum_kernel,
        in_specs=[VMEM] * len(args),
        out_specs=[VMEM] * outs,
        out_shape=[jax.ShapeDtypeStruct((rows, 2 * NF), jnp.bfloat16)] * outs,
        compiler_params=pltpu.CompilerParams(vmem_limit_bytes=12 << 20),
        cost_estimate=pl.CostEstimate(
            flops=4 * rows * span * NF, bytes_accessed=4 * span * NF, transcendentals=0
        ),
        name="spectra",
    )(*args)


def inner_body(synthetic, observed, station_weights, pair_mask):
    levels = lax.axis_size("blk")
    subs = lax.axis_size("sub")
    pairs = lax.axis_size("pair")
    level = lax.axis_index("blk")
    sub = lax.axis_index("sub")
    pair = lax.axis_index("pair")
    span = synthetic.shape[1]
    half = synthetic.shape[0] // 2
    per_half = levels // 2
    stations = station_weights.shape[0]
    piece = half // per_half
    side = level // 2
    inward, swapped, outward = [(0, 1), (3, 2)], [(1, 2), (2, 1)], [(1, 0), (2, 3)]

    def piece_of(which, at, sources):
        return jnp.concatenate(
            [
                lax.dynamic_slice_in_dim(source, which * half + at, piece, 0)
                for source in sources
            ],
            axis=0,
        )

    sources = (synthetic, observed)
    front = piece_of(1 - side, 0, sources)
    front, sources = lax.optimization_barrier((front, sources))
    passed = [front] + [piece_of(1 - side, at, sources) for at in range(piece, half, piece)]
    kept = [piece_of(side, at, sources) for at in range(0, half, piece)]
    near_passed, near_kept = [], []
    for blocks, arrived in ((passed, near_passed), (kept, near_kept)):
        for block in blocks:
            arrived.append(lax.ppermute(block, "blk", inward))

    member = sub * pairs + pair
    hops = [(s, q) for s in range(subs) for q in range(pairs)]
    halves = [
        ((sub - s) % subs * pairs + (pair - q) % pairs) * 2 * half + side * half for s, q in hops
    ]
    gains = station_weights.astype(jnp.float32)
    col_gains = jnp.concatenate(
        [lax.dynamic_slice_in_dim(gains, start, half, 0) for start in halves]
    )[None, :]
    firsts = [member * 2 * half + which * half for which in (side, 1 - side)]
    own_gains, other_gains = [
        lax.dynamic_slice_in_dim(gains, start, half, 0)[None, :] for start in firsts
    ]
    link = jnp.maximum(pair_mask, pair_mask.T).astype(jnp.float32)
    link_rows = jnp.concatenate(
        [lax.dynamic_slice_in_dim(link, start // piece, per_half, 0) for start in firsts], axis=0
    )
    col_pieces = jnp.concatenate(
        [start + jnp.arange(half, dtype=jnp.int32) for start in halves]
    ) // piece
    chosen = jnp.arange(link.shape[0], dtype=jnp.int32)[:, None] == col_pieces[None, :]
    active = jnp.dot(
        link_rows, chosen.astype(jnp.float32), preferred_element_type=jnp.float32
    )
    weights = 4.0 / math.sqrt(stations) * col_gains * active
    here, own_gains, other_gains, weights = lax.optimization_barrier(
        (level, own_gains, other_gains, weights)
    )
    own_weights, other_weights = weights[:per_half], weights[per_half:]

    here_basis, near_basis = two_bases(here * span, (here ^ 1) * span, span)
    passed_parts = own_parts(passed, here_basis)
    kept_parts = own_parts(kept, here_basis)
    to_pass, kept_rest = [], []
    for place in range(per_half):
        (summed,) = spectra(passed_parts[place], near_passed[place], near_basis)
        to_pass.append(summed)
        kept_rest.append(lax.ppermute(summed, "blk", swapped))
    own, passed_rest, cols = [], [], {}
    for place in range(per_half):
        whole, summed = spectra(
            kept_parts[place], near_kept[place], near_basis, kept_rest[place]
        )
        own.append(whole)
        for s, q in hops:
            if q == 0:
                cols[s, q, place] = whole if s == 0 else shift(whole, "sub", s)
            else:
                cols[s, q, place] = shift(cols[s, 0, place], "pair", q)
        passed_rest.append(lax.ppermute(summed, "blk", swapped))
    cols = [cols[s, q, place] for s, q in hops for place in range(per_half)]
    other = [block for both in zip(to_pass, passed_rest) for block in both]
    other_part = couple(other, cols, other_gains, other_weights, piece)
    own_rest = lax.ppermute(other_part, "blk", swapped)
    own_part = couple(own, cols, own_gains, own_weights, piece)
    other_rest = lax.ppermute(own_part, "blk", swapped)
    widen = lambda a: a.astype(jnp.float32)
    own_adjoint = (widen(own_part) + widen(own_rest)).astype(jnp.bfloat16)
    near_own = lax.ppermute(own_adjoint, "blk", outward)
    other_adjoint = (widen(other_part) + widen(other_rest)).astype(jnp.bfloat16)
    near_other = lax.ppermute(other_adjoint, "blk", outward)
    is_inner = (level == 1) | (level == 2)
    rows = synthetic.shape[0]
    traces = to_time(side, is_inner, own_adjoint, near_own, here_basis, span, rows, None)
    return to_time(1 - side, is_inner, other_adjoint, near_other, here_basis, span, rows, traces)


def shards(*args):
    body = inner_body if lax.axis_size("blk") == 4 else ring_body
    return body(*args)


def solution(mesh):
    placed = (
        P(("events", "sub", "pair"), "blk"),
        P(("events", "sub", "pair"), "blk"),
        P("events"),
        P("events", None),
    )
    return jax.shard_map(
        shards,
        mesh=mesh,
        in_specs=placed,
        out_specs=P(("events", "sub", "pair"), "blk"),
        check_vma=False,
    )
```

```python
import functools
import math

import jax
import jax.numpy as jnp
from jax import lax
from jax.experimental import pallas as pl
from jax.experimental.pallas import tpu as pltpu
from jax.sharding import PartitionSpec as P


NT = 4096
NF = 512
F_LO = 64

epsilon = 1e-06
CONTRACT_LAST = (((1,), (1,)), ((), ()))
VMEM = pl.BlockSpec(memory_space=pltpu.VMEM)


def shift(value, axis, steps):
    count = lax.axis_size(axis)
    pairs = [(source, (source + steps) % count) for source in range(count)]
    return lax.ppermute(value, axis, pairs)


def sweep(count):
    order = []
    for near in range(1, count // 2 + 1):
        order.append(near)
        if (count - near) % count != near:
            order.append(count - near)
    return order


def cos_sin(samples):
    bins = F_LO + jnp.arange(NF, dtype=jnp.int32)
    phases = samples[:, None] * bins[None, :] % NT
    angles = phases.astype(jnp.float32) * (2.0 * math.pi / NT)
    return jnp.cos(angles), jnp.sin(angles)


def basis_kernel(per_step, low_rows, hc_ref, hs_ref, lc_ref, ls_ref, out_ref):
    step = pl.program_id(0)
    for h in range(per_step):
        hc = hc_ref[pl.ds(step * per_step + h, 1), :]
        hs = hs_ref[pl.ds(step * per_step + h, 1), :]
        lc = lc_ref[...]
        ls = ls_ref[...]
        rows = slice(h * low_rows, (h + 1) * low_rows)
        out_ref[rows, :NF] = (hc * lc - hs * ls).astype(jnp.bfloat16)
        out_ref[rows, NF:] = (-(hs * lc + hc * ls)).astype(jnp.bfloat16)


def make_basis(firsts, span):
    low_rows = math.gcd(span, 64)
    low_c, low_s = cos_sin(jnp.arange(low_rows, dtype=jnp.int32))
    highs = (firsts[:, None] + jnp.arange(0, span, low_rows, dtype=jnp.int32)[None, :]).reshape(-1)
    high_c, high_s = cos_sin(highs)
    per_step = math.gcd(highs.shape[0], 4)
    whole = lambda a: pl.BlockSpec(a.shape, lambda i: (0, 0))
    rows = highs.shape[0] * low_rows
    return pl.pallas_call(
        functools.partial(basis_kernel, per_step, low_rows),
        grid=(highs.shape[0] // per_step,),
        in_specs=[whole(high_c), whole(high_s), whole(low_c), whole(low_s)],
        out_specs=pl.BlockSpec((per_step * low_rows, 2 * NF), lambda i: (i, 0)),
        out_shape=jax.ShapeDtypeStruct((rows, 2 * NF), jnp.bfloat16),
        cost_estimate=pl.CostEstimate(
            flops=8 * rows * NF, bytes_accessed=4 * rows * NF, transcendentals=0
        ),
        compiler_params=pltpu.CompilerParams(vmem_limit_bytes=16 << 20),
        name="basis",
    )(high_c, high_s, low_c, low_s)


def angular_row():
    bins = F_LO + lax.broadcasted_iota(jnp.int32, (1, NF), 1)
    return 2.0 * math.pi / NT * bins.astype(jnp.float32)


def rate_of(re, im):
    angular = angular_row()
    return jnp.concatenate([-angular * im, angular * re], axis=1).astype(jnp.bfloat16)


def tile_kernel(first, rows_ref, power_ref, coef_ref, gain_ref, col_ref, *rest):
    out_ref = rest[-1]
    col = col_ref[...].astype(jnp.float32)
    model_rate = rate_of(col[:, :NF], col[:, NF : 2 * NF])
    data_rate = rate_of(-col[:, 2 * NF : 3 * NF], -col[:, 3 * NF :])
    both = jnp.concatenate([model_rate, data_rate], axis=1)
    cross = lax.dot_general(
        rows_ref[...], both, CONTRACT_LAST, preferred_element_type=jnp.float32
    )
    col_power = lax.dot_general(
        jnp.ones((8, 2 * NF), jnp.float32),
        jnp.square(model_rate.astype(jnp.float32)),
        CONTRACT_LAST,
        precision=lax.Precision.HIGHEST,
        preferred_element_type=jnp.float32,
    )[0:1, :]
    normalizer = 0.5 * (power_ref[...] + col_power) + epsilon
    coupling = (coef_ref[...] * gain_ref[...] * cross / normalizer).astype(jnp.bfloat16)
    update = jnp.dot(coupling, model_rate, preferred_element_type=jnp.float32)
    if first:
        out_ref[...] = update
    else:
        out_ref[...] = rest[0][...] + update


def pair_tile(running, rows, row_power, coef, gain, col):
    args = [rows, row_power, coef, gain, col]
    aliases = {}
    if running is not None:
        aliases = {len(args): 0}
        args.append(running)
    height, width = rows.shape[0], col.shape[0]
    return pl.pallas_call(
        functools.partial(tile_kernel, running is None),
        in_specs=[pl.BlockSpec(memory_space=pltpu.VMEM)] * len(args),
        out_specs=pl.BlockSpec(memory_space=pltpu.VMEM),
        out_shape=jax.ShapeDtypeStruct((height, 2 * NF), jnp.float32),
        input_output_aliases=aliases,
        cost_estimate=pl.CostEstimate(
            flops=12 * height * width * NF,
            bytes_accessed=16 * height * NF,
            transcendentals=0,
        ),
        name="pair_tile",
    )(*args)


def ring_body(synthetic, observed, station_weights, pair_mask):
    levels = lax.axis_size("blk")
    subs = lax.axis_size("sub")
    pairs = lax.axis_size("pair")
    level = lax.axis_index("blk")
    sub = lax.axis_index("sub")
    pair = lax.axis_index("pair")
    span = synthetic.shape[1]
    piece = synthetic.shape[0] // levels
    stations = station_weights.shape[0]

    def owned_by(steps):
        owner = (level + steps) % levels
        return jnp.concatenate(
            [
                lax.dynamic_slice_in_dim(synthetic, owner * piece, piece, 0),
                lax.dynamic_slice_in_dim(observed, owner * piece, piece, 0),
            ],
            axis=0,
        )

    order = sweep(levels)
    blocks = {0: owned_by(0)}
    for steps in order:
        blocks[steps] = shift(owned_by(steps), "blk", steps)
    arrivals = [0] + order
    firsts = jnp.stack([(level - steps) % levels * span for steps in arrivals]).astype(jnp.int32)
    basis = make_basis(firsts, span)
    member = sub * pairs + pair
    members = jnp.stack(
        [
            (sub - s) % subs * pairs + (pair - q) % pairs
            for s in range(subs)
            for q in range(pairs)
        ]
    )
    gains = station_weights.astype(jnp.float32).reshape(-1, piece)
    link = jnp.maximum(pair_mask, pair_mask.T).astype(jnp.float32)
    row_pieces = members * levels + level
    row_gain = gains[row_pieces].reshape(-1, 1)
    row_link = link[row_pieces]
    factor = 4.0 / math.sqrt(stations)
    coefs, col_gains = [], []
    for steps in arrivals:
        column_piece = member * levels + (level - steps) % levels
        active = lax.dynamic_slice_in_dim(row_link, column_piece, 1, 1)
        coefs.append(factor * row_gain * jnp.repeat(active, piece, axis=0))
        col_gains.append(lax.dynamic_slice_in_dim(gains, column_piece, 1, 0))
    last = order[-1]
    blocks[last], coefs, col_gains = lax.optimization_barrier((blocks[last], coefs, col_gains))
    total = None
    for place, steps in enumerate(arrivals):
        part = jnp.dot(
            blocks[steps],
            basis[place * span : (place + 1) * span],
            preferred_element_type=jnp.float32,
        )
        total = part if total is None else total + part
    spec = (total * (1.0 / math.sqrt(NT))).astype(jnp.bfloat16)
    own = jnp.concatenate([spec[:piece], spec[piece:]], axis=1)

    columns = {0: own}
    for steps in order:
        columns[steps] = shift(own, "blk", steps)
    blocks_of_rows = []
    for s in range(subs):
        here = own if s == 0 else shift(own, "sub", s)
        for q in range(pairs):
            blocks_of_rows.append(here if q == 0 else shift(here, "pair", q))
    rows = jnp.concatenate(blocks_of_rows, axis=0)
    widened = rows[:, : 2 * NF].astype(jnp.float32)
    row_rate = rate_of(widened[:, :NF], widened[:, NF:])
    row_power = jnp.sum(jnp.square(row_rate.astype(jnp.float32)), axis=1, keepdims=True)

    running = None
    for place, steps in enumerate(arrivals):
        running = pair_tile(
            running, rows, row_power, coefs[place], col_gains[place], columns[steps]
        )

    partial = running.reshape(subs, pairs, piece, 2 * NF)
    held = partial[:, 0]
    for q in range(1, pairs):
        sent = partial[:, q].astype(jnp.bfloat16)
        held = held + shift(sent, "pair", -q).astype(jnp.float32)
    adjoint = held[0]
    for s in range(1, subs):
        adjoint = adjoint + shift(held[s].astype(jnp.bfloat16), "sub", -s).astype(jnp.float32)
    adjoint = adjoint.astype(jnp.bfloat16)

    gathered = jnp.zeros((levels * piece, 2 * NF), jnp.bfloat16)
    for steps in arrivals:
        arrived = adjoint if steps == 0 else shift(adjoint, "blk", steps)
        gathered = lax.dynamic_update_slice_in_dim(
            gathered, arrived, (level - steps) % levels * piece, 0
        )
    return (
        lax.dot_general(
            gathered, basis[:span], CONTRACT_LAST, preferred_element_type=jnp.float32
        )
        * (1.0 / math.sqrt(NF))
    ).astype(jnp.bfloat16)


def power_of(spec):
    wide = spec.astype(jnp.float32)
    rate = rate_of(wide[:, :NF], wide[:, NF:])
    return rate, jnp.sum(jnp.square(rate.astype(jnp.float32)), axis=1, keepdims=True)


def couple_kernel(piece, row_count, col_count, before, *refs):
    row_refs = refs[:row_count]
    col_refs = refs[row_count : row_count + col_count]
    gain_ref, weight_ref, out_ref = refs[-3:]
    sums = row_count // (gain_ref.shape[1] // piece)
    row_models, row_datas = [], []
    for at in range(0, row_count, sums):
        block = row_refs[at][...]
        if sums == 2:
            block = (
                block.astype(jnp.float32) + row_refs[at + 1][...].astype(jnp.float32)
            ).astype(jnp.bfloat16)
        row_models.append(block[:piece])
        row_datas.append(block[piece:])
    row_model = jnp.concatenate(row_models, axis=0)
    row_data = jnp.concatenate(row_datas, axis=0)
    row_power = power_of(row_model)[1]
    models, datas, powers = [], [], []
    for ref in col_refs:
        rate, power = power_of(ref[:piece])
        models.append(rate)
        powers.append(power)
        wide = ref[piece:].astype(jnp.float32)
        datas.append(rate_of(wide[:, :NF], wide[:, NF:]))
    col_model = jnp.concatenate(models, axis=0)
    col_data = jnp.concatenate(datas, axis=0)
    powers = jnp.concatenate(powers, axis=0)

    def diagonal(width):
        return lax.broadcasted_iota(jnp.int32, (width, width), 0) == lax.broadcasted_iota(
            jnp.int32, (width, width), 1
        )

    col_power = jnp.sum(
        jnp.where(diagonal(powers.shape[0]), powers, 0.0), axis=0, keepdims=True
    )
    height = gain_ref.shape[1]
    row_gain = jnp.sum(
        jnp.where(diagonal(height), gain_ref[...], 0.0), axis=1, keepdims=True
    )
    cross = lax.dot_general(
        row_model, col_model, CONTRACT_LAST, preferred_element_type=jnp.float32
    ) - lax.dot_general(row_data, col_data, CONTRACT_LAST, preferred_element_type=jnp.float32)
    normalizer = 0.5 * (row_power + col_power) + epsilon
    ratio = row_gain * cross / normalizer
    coupling = jnp.concatenate(
        [
            (weight_ref[at : at + 1, :] * ratio[at * piece : (at + 1) * piece]).astype(
                jnp.bfloat16
            )
            for at in range(height // piece)
        ],
        axis=0,
    )
    update = jnp.dot(coupling, col_model, preferred_element_type=jnp.float32)
    if before:
        update = update + refs[row_count + col_count][...]
    out_ref[...] = update.astype(out_ref.dtype)


def couple(rows, cols, gains, weights, piece, before=None, kind=jnp.bfloat16):
    args = [*rows, *cols] + ([] if before is None else [before]) + [gains, weights]
    height, width = gains.shape[1], weights.shape[1]
    return pl.pallas_call(
        functools.partial(couple_kernel, piece, len(rows), len(cols), before is not None),
        in_specs=[VMEM] * len(args),
        out_specs=VMEM,
        out_shape=jax.ShapeDtypeStruct((height, 2 * NF), kind),
        compiler_params=pltpu.CompilerParams(vmem_limit_bytes=16 << 20),
        cost_estimate=pl.CostEstimate(
            flops=12 * height * width * NF,
            bytes_accessed=8 * (height + width) * NF,
            transcendentals=0,
        ),
        name="couple",
    )(*args)


def to_time_kernel(flag_ref, here_ref, there_ref, basis_ref, *rest):
    out_ref = rest[-1]
    adjoint = jnp.where(flag_ref[1] == 1, here_ref[...], there_ref[...])
    traces = lax.dot_general(
        adjoint, basis_ref[...], CONTRACT_LAST, preferred_element_type=jnp.float32
    )
    out_ref[...] = (traces * (1.0 / math.sqrt(NF))).astype(jnp.bfloat16)


def to_time(place, is_inner, here, there, basis, span, rows, before):
    half = here.shape[0]
    wide = span
    whole = pl.BlockSpec(here.shape, lambda j, flags: (0, 0))
    specs = [whole, whole, pl.BlockSpec((wide, 2 * NF), lambda j, flags: (j, 0))]
    args = [here, there, basis]
    aliases = {}
    if before is not None:
        specs.append(pl.BlockSpec(memory_space=pl.ANY))
        args.append(before)
        aliases = {4: 0}
    return pl.pallas_call(
        to_time_kernel,
        grid_spec=pltpu.PrefetchScalarGridSpec(
            num_scalar_prefetch=1,
            grid=(span // wide,),
            in_specs=specs,
            out_specs=pl.BlockSpec((half, wide), lambda j, flags: (flags[0], j)),
        ),
        out_shape=jax.ShapeDtypeStruct((rows, span), jnp.bfloat16),
        input_output_aliases=aliases,
        cost_estimate=pl.CostEstimate(
            flops=4 * half * span * NF, bytes_accessed=4 * span * NF, transcendentals=0
        ),
        compiler_params=pltpu.CompilerParams(vmem_limit_bytes=12 << 20),
        name="to_time",
    )(jnp.stack([place, is_inner.astype(jnp.int32)]).astype(jnp.int32), *args)


def two_bases_kernel(per_step, low_rows, *refs):
    lc_ref, ls_ref = refs[4:6]
    for high, out_ref in zip((refs[:2], refs[2:4]), refs[6:]):
        basis_kernel(per_step, low_rows, *high, lc_ref, ls_ref, out_ref)


def two_bases(first, second, span):
    low_rows = math.gcd(span, 64)
    tables = []
    for start in (first, second):
        tables += cos_sin(start + jnp.arange(0, span, low_rows, dtype=jnp.int32))
    tables += cos_sin(jnp.arange(low_rows, dtype=jnp.int32))
    per_step = math.gcd(span // low_rows, 4)
    block = pl.BlockSpec((per_step * low_rows, 2 * NF), lambda i: (i, 0))
    return pl.pallas_call(
        functools.partial(two_bases_kernel, per_step, low_rows),
        grid=(span // low_rows // per_step,),
        in_specs=[pl.BlockSpec(table.shape, lambda i: (0, 0)) for table in tables],
        out_specs=[block, block],
        out_shape=[jax.ShapeDtypeStruct((span, 2 * NF), jnp.bfloat16)] * 2,
        compiler_params=pltpu.CompilerParams(vmem_limit_bytes=12 << 20),
        cost_estimate=pl.CostEstimate(
            flops=16 * span * NF, bytes_accessed=8 * span * NF, transcendentals=0
        ),
        name="two_bases",
    )(*tables)


def own_parts_kernel(count, *refs):
    basis_ref = refs[count]
    for block_ref, out_ref in zip(refs[:count], refs[count + 1 :]):
        out_ref[...] = jnp.dot(
            block_ref[...], basis_ref[...], preferred_element_type=jnp.float32
        )


def own_parts(blocks, basis):
    rows, span = blocks[0].shape
    return pl.pallas_call(
        functools.partial(own_parts_kernel, len(blocks)),
        in_specs=[VMEM] * (len(blocks) + 1),
        out_specs=[VMEM] * len(blocks),
        out_shape=[jax.ShapeDtypeStruct((rows, 2 * NF), jnp.float32)] * len(blocks),
        compiler_params=pltpu.CompilerParams(vmem_limit_bytes=12 << 20),
        cost_estimate=pl.CostEstimate(
            flops=4 * len(blocks) * rows * span * NF,
            bytes_accessed=4 * span * NF,
            transcendentals=0,
        ),
        name="own_parts",
    )(*blocks, basis)


def sum_kernel(part_ref, near_ref, basis_ref, *rest):
    total = part_ref[...] + jnp.dot(
        near_ref[...], basis_ref[...], preferred_element_type=jnp.float32
    )
    total = total * (1.0 / math.sqrt(NT))
    if len(rest) == 3:
        rest_ref, own_ref, sum_ref = rest
        own_ref[...] = (total + rest_ref[...].astype(jnp.float32)).astype(jnp.bfloat16)
    else:
        sum_ref = rest[0]
    sum_ref[...] = total.astype(jnp.bfloat16)


def spectra(part, near, basis, others=None):
    rows, span = near.shape
    args = [part, near, basis] + ([] if others is None else [others])
    outs = 1 if others is None else 2
    return pl.pallas_call(
        sum_kernel,
        in_specs=[VMEM] * len(args),
        out_specs=[VMEM] * outs,
        out_shape=[jax.ShapeDtypeStruct((rows, 2 * NF), jnp.bfloat16)] * outs,
        compiler_params=pltpu.CompilerParams(vmem_limit_bytes=12 << 20),
        cost_estimate=pl.CostEstimate(
            flops=4 * rows * span * NF, bytes_accessed=4 * span * NF, transcendentals=0
        ),
        name="spectra",
    )(*args)


def inner_body(synthetic, observed, station_weights, pair_mask):
    levels = lax.axis_size("blk")
    subs = lax.axis_size("sub")
    pairs = lax.axis_size("pair")
    level = lax.axis_index("blk")
    sub = lax.axis_index("sub")
    pair = lax.axis_index("pair")
    span = synthetic.shape[1]
    half = synthetic.shape[0] // 2
    per_half = levels // 2
    stations = station_weights.shape[0]
    piece = half // per_half
    side = level // 2
    inward, swapped, outward = [(0, 1), (3, 2)], [(1, 2), (2, 1)], [(1, 0), (2, 3)]

    def piece_of(which, at, sources):
        return jnp.concatenate(
            [
                lax.dynamic_slice_in_dim(source, which * half + at, piece, 0)
                for source in sources
            ],
            axis=0,
        )

    sources = (synthetic, observed)
    front = piece_of(1 - side, 0, sources)
    front, sources = lax.optimization_barrier((front, sources))
    passed = [front] + [piece_of(1 - side, at, sources) for at in range(piece, half, piece)]
    kept = [piece_of(side, at, sources) for at in range(0, half, piece)]
    near_passed, near_kept = [], []
    for blocks, arrived in ((passed, near_passed), (kept, near_kept)):
        for block in blocks:
            arrived.append(lax.ppermute(block, "blk", inward))

    member = sub * pairs + pair
    hops = [(s, q) for s in range(subs) for q in range(pairs)]
    starts = [
        ((sub - s) % subs * pairs + (pair - q) % pairs) * 2 * half + side * half + at
        for at in range(0, half, piece)
        for s, q in hops
    ]
    gains = station_weights.astype(jnp.float32)
    col_gains = jnp.concatenate(
        [lax.dynamic_slice_in_dim(gains, start, piece, 0) for start in starts]
    )[None, :]
    firsts = [member * 2 * half + which * half for which in (side, 1 - side)]
    own_gains, other_gains = [
        lax.dynamic_slice_in_dim(gains, start, half, 0)[None, :] for start in firsts
    ]
    link = jnp.maximum(pair_mask, pair_mask.T).astype(jnp.float32)
    link_rows = jnp.concatenate(
        [lax.dynamic_slice_in_dim(link, start // piece, per_half, 0) for start in firsts], axis=0
    )
    col_pieces = jnp.repeat(jnp.stack(starts) // piece, piece)
    chosen = jnp.arange(link.shape[0], dtype=jnp.int32)[:, None] == col_pieces[None, :]
    active = jnp.dot(
        link_rows, chosen.astype(jnp.float32), preferred_element_type=jnp.float32
    )
    weights = 4.0 / math.sqrt(stations) * col_gains * active
    late = (subs - 1) * pairs
    early_width = (len(starts) - late) * piece
    own_early, own_late = weights[:per_half, :early_width], weights[:per_half, early_width:]
    here, own_gains, other_gains, own_early, own_late, other_weights = lax.optimization_barrier(
        (level, own_gains, other_gains, own_early, own_late, weights[per_half:])
    )

    here_basis, near_basis = two_bases(here * span, (here ^ 1) * span, span)
    passed_parts = own_parts(passed, here_basis)
    kept_parts = own_parts(kept, here_basis)
    to_pass, kept_rest = [], []
    for place in range(per_half):
        (summed,) = spectra(passed_parts[place], near_passed[place], near_basis)
        to_pass.append(summed)
        kept_rest.append(lax.ppermute(summed, "blk", swapped))
    own, passed_rest, cols = [], [], {}
    for place in range(per_half):
        whole, summed = spectra(
            kept_parts[place], near_kept[place], near_basis, kept_rest[place]
        )
        own.append(whole)
        for s, q in hops:
            if q == 0:
                cols[s, q, place] = whole if s == 0 else shift(whole, "sub", s)
            else:
                cols[s, q, place] = shift(cols[s, 0, place], "pair", q)
        passed_rest.append(lax.ppermute(summed, "blk", swapped))
    cols = [cols[s, q, place] for place in range(per_half) for s, q in hops]
    begun = couple(own, cols[:-late], own_gains, own_early, piece, None, jnp.float32)
    own_part = couple(own, cols[-late:], own_gains, own_late, piece, begun)
    other_rest = lax.ppermute(own_part, "blk", swapped)
    other = [block for both in zip(to_pass, passed_rest) for block in both]
    other_part = couple(other, cols, other_gains, other_weights, piece)
    own_rest = lax.ppermute(other_part, "blk", swapped)
    widen = lambda a: a.astype(jnp.float32)
    other_adjoint = (widen(other_part) + widen(other_rest)).astype(jnp.bfloat16)
    near_other = lax.ppermute(other_adjoint, "blk", outward)
    own_adjoint = (widen(own_part) + widen(own_rest)).astype(jnp.bfloat16)
    near_own = lax.ppermute(own_adjoint, "blk", outward)
    is_inner = (level == 1) | (level == 2)
    rows = synthetic.shape[0]
    traces = to_time(
        1 - side, is_inner, other_adjoint, near_other, here_basis, span, rows, None
    )
    return to_time(side, is_inner, own_adjoint, near_own, here_basis, span, rows, traces)


def shards(*args):
    body = inner_body if lax.axis_size("blk") == 4 else ring_body
    return body(*args)


def solution(mesh):
    placed = (
        P(("events", "sub", "pair"), "blk"),
        P(("events", "sub", "pair"), "blk"),
        P("events"),
        P("events", None),
    )
    return jax.shard_map(
        shards,
        mesh=mesh,
        in_specs=placed,
        out_specs=P(("events", "sub", "pair"), "blk"),
        check_vma=False,
    )
```

```python
import functools
import math

import jax
import jax.numpy as jnp
from jax import lax
from jax.experimental import pallas as pl
from jax.experimental.pallas import tpu as pltpu
from jax.sharding import PartitionSpec as P


NT = 4096
NF = 512
F_LO = 64

epsilon = 1e-06
CONTRACT_LAST = (((1,), (1,)), ((), ()))
VMEM = pl.BlockSpec(memory_space=pltpu.VMEM)


def shift(value, axis, steps):
    count = lax.axis_size(axis)
    pairs = [(source, (source + steps) % count) for source in range(count)]
    return lax.ppermute(value, axis, pairs)


def sweep(count):
    order = []
    for near in range(1, count // 2 + 1):
        order.append(near)
        if (count - near) % count != near:
            order.append(count - near)
    return order


def cos_sin(samples):
    bins = F_LO + jnp.arange(NF, dtype=jnp.int32)
    phases = samples[:, None] * bins[None, :] % NT
    angles = phases.astype(jnp.float32) * (2.0 * math.pi / NT)
    return jnp.cos(angles), jnp.sin(angles)


def basis_kernel(per_step, low_rows, hc_ref, hs_ref, lc_ref, ls_ref, out_ref):
    step = pl.program_id(0)
    for h in range(per_step):
        hc = hc_ref[pl.ds(step * per_step + h, 1), :]
        hs = hs_ref[pl.ds(step * per_step + h, 1), :]
        lc = lc_ref[...]
        ls = ls_ref[...]
        rows = slice(h * low_rows, (h + 1) * low_rows)
        out_ref[rows, :NF] = (hc * lc - hs * ls).astype(jnp.bfloat16)
        out_ref[rows, NF:] = (-(hs * lc + hc * ls)).astype(jnp.bfloat16)


def make_basis(firsts, span):
    low_rows = math.gcd(span, 64)
    low_c, low_s = cos_sin(jnp.arange(low_rows, dtype=jnp.int32))
    highs = (firsts[:, None] + jnp.arange(0, span, low_rows, dtype=jnp.int32)[None, :]).reshape(-1)
    high_c, high_s = cos_sin(highs)
    per_step = math.gcd(highs.shape[0], 4)
    whole = lambda a: pl.BlockSpec(a.shape, lambda i: (0, 0))
    rows = highs.shape[0] * low_rows
    return pl.pallas_call(
        functools.partial(basis_kernel, per_step, low_rows),
        grid=(highs.shape[0] // per_step,),
        in_specs=[whole(high_c), whole(high_s), whole(low_c), whole(low_s)],
        out_specs=pl.BlockSpec((per_step * low_rows, 2 * NF), lambda i: (i, 0)),
        out_shape=jax.ShapeDtypeStruct((rows, 2 * NF), jnp.bfloat16),
        cost_estimate=pl.CostEstimate(
            flops=8 * rows * NF, bytes_accessed=4 * rows * NF, transcendentals=0
        ),
        compiler_params=pltpu.CompilerParams(vmem_limit_bytes=16 << 20),
        name="basis",
    )(high_c, high_s, low_c, low_s)


def angular_row():
    bins = F_LO + lax.broadcasted_iota(jnp.int32, (1, NF), 1)
    return 2.0 * math.pi / NT * bins.astype(jnp.float32)


def rate_of(re, im):
    angular = angular_row()
    return jnp.concatenate([-angular * im, angular * re], axis=1).astype(jnp.bfloat16)


def tile_kernel(first, rows_ref, power_ref, coef_ref, gain_ref, col_ref, *rest):
    out_ref = rest[-1]
    col = col_ref[...].astype(jnp.float32)
    model_rate = rate_of(col[:, :NF], col[:, NF : 2 * NF])
    data_rate = rate_of(-col[:, 2 * NF : 3 * NF], -col[:, 3 * NF :])
    both = jnp.concatenate([model_rate, data_rate], axis=1)
    cross = lax.dot_general(
        rows_ref[...], both, CONTRACT_LAST, preferred_element_type=jnp.float32
    )
    col_power = lax.dot_general(
        jnp.ones((8, 2 * NF), jnp.float32),
        jnp.square(model_rate.astype(jnp.float32)),
        CONTRACT_LAST,
        precision=lax.Precision.HIGHEST,
        preferred_element_type=jnp.float32,
    )[0:1, :]
    normalizer = 0.5 * (power_ref[...] + col_power) + epsilon
    coupling = (coef_ref[...] * gain_ref[...] * cross / normalizer).astype(jnp.bfloat16)
    update = jnp.dot(coupling, model_rate, preferred_element_type=jnp.float32)
    if first:
        out_ref[...] = update
    else:
        out_ref[...] = rest[0][...] + update


def pair_tile(running, rows, row_power, coef, gain, col):
    args = [rows, row_power, coef, gain, col]
    aliases = {}
    if running is not None:
        aliases = {len(args): 0}
        args.append(running)
    height, width = rows.shape[0], col.shape[0]
    return pl.pallas_call(
        functools.partial(tile_kernel, running is None),
        in_specs=[pl.BlockSpec(memory_space=pltpu.VMEM)] * len(args),
        out_specs=pl.BlockSpec(memory_space=pltpu.VMEM),
        out_shape=jax.ShapeDtypeStruct((height, 2 * NF), jnp.float32),
        input_output_aliases=aliases,
        cost_estimate=pl.CostEstimate(
            flops=12 * height * width * NF,
            bytes_accessed=16 * height * NF,
            transcendentals=0,
        ),
        name="pair_tile",
    )(*args)


def ring_body(synthetic, observed, station_weights, pair_mask):
    levels = lax.axis_size("blk")
    subs = lax.axis_size("sub")
    pairs = lax.axis_size("pair")
    level = lax.axis_index("blk")
    sub = lax.axis_index("sub")
    pair = lax.axis_index("pair")
    span = synthetic.shape[1]
    piece = synthetic.shape[0] // levels
    stations = station_weights.shape[0]

    def owned_by(steps):
        owner = (level + steps) % levels
        return jnp.concatenate(
            [
                lax.dynamic_slice_in_dim(synthetic, owner * piece, piece, 0),
                lax.dynamic_slice_in_dim(observed, owner * piece, piece, 0),
            ],
            axis=0,
        )

    order = sweep(levels)
    blocks = {0: owned_by(0)}
    for steps in order:
        blocks[steps] = shift(owned_by(steps), "blk", steps)
    arrivals = [0] + order
    firsts = jnp.stack([(level - steps) % levels * span for steps in arrivals]).astype(jnp.int32)
    basis = make_basis(firsts, span)
    member = sub * pairs + pair
    members = jnp.stack(
        [
            (sub - s) % subs * pairs + (pair - q) % pairs
            for s in range(subs)
            for q in range(pairs)
        ]
    )
    gains = station_weights.astype(jnp.float32).reshape(-1, piece)
    link = jnp.maximum(pair_mask, pair_mask.T).astype(jnp.float32)
    row_pieces = members * levels + level
    row_gain = gains[row_pieces].reshape(-1, 1)
    row_link = link[row_pieces]
    factor = 4.0 / math.sqrt(stations)
    coefs, col_gains = [], []
    for steps in arrivals:
        column_piece = member * levels + (level - steps) % levels
        active = lax.dynamic_slice_in_dim(row_link, column_piece, 1, 1)
        coefs.append(factor * row_gain * jnp.repeat(active, piece, axis=0))
        col_gains.append(lax.dynamic_slice_in_dim(gains, column_piece, 1, 0))
    last = order[-1]
    blocks[last], coefs, col_gains = lax.optimization_barrier((blocks[last], coefs, col_gains))
    total = None
    for place, steps in enumerate(arrivals):
        part = jnp.dot(
            blocks[steps],
            basis[place * span : (place + 1) * span],
            preferred_element_type=jnp.float32,
        )
        total = part if total is None else total + part
    spec = (total * (1.0 / math.sqrt(NT))).astype(jnp.bfloat16)
    own = jnp.concatenate([spec[:piece], spec[piece:]], axis=1)

    columns = {0: own}
    for steps in order:
        columns[steps] = shift(own, "blk", steps)
    blocks_of_rows = []
    for s in range(subs):
        here = own if s == 0 else shift(own, "sub", s)
        for q in range(pairs):
            blocks_of_rows.append(here if q == 0 else shift(here, "pair", q))
    rows = jnp.concatenate(blocks_of_rows, axis=0)
    widened = rows[:, : 2 * NF].astype(jnp.float32)
    row_rate = rate_of(widened[:, :NF], widened[:, NF:])
    row_power = jnp.sum(jnp.square(row_rate.astype(jnp.float32)), axis=1, keepdims=True)

    running = None
    for place, steps in enumerate(arrivals):
        running = pair_tile(
            running, rows, row_power, coefs[place], col_gains[place], columns[steps]
        )

    partial = running.reshape(subs, pairs, piece, 2 * NF)
    held = partial[:, 0]
    for q in range(1, pairs):
        sent = partial[:, q].astype(jnp.bfloat16)
        held = held + shift(sent, "pair", -q).astype(jnp.float32)
    adjoint = held[0]
    for s in range(1, subs):
        adjoint = adjoint + shift(held[s].astype(jnp.bfloat16), "sub", -s).astype(jnp.float32)
    adjoint = adjoint.astype(jnp.bfloat16)

    gathered = jnp.zeros((levels * piece, 2 * NF), jnp.bfloat16)
    for steps in arrivals:
        arrived = adjoint if steps == 0 else shift(adjoint, "blk", steps)
        gathered = lax.dynamic_update_slice_in_dim(
            gathered, arrived, (level - steps) % levels * piece, 0
        )
    return (
        lax.dot_general(
            gathered, basis[:span], CONTRACT_LAST, preferred_element_type=jnp.float32
        )
        * (1.0 / math.sqrt(NF))
    ).astype(jnp.bfloat16)


def power_of(spec):
    wide = spec.astype(jnp.float32)
    rate = rate_of(wide[:, :NF], wide[:, NF:])
    return rate, jnp.sum(jnp.square(rate.astype(jnp.float32)), axis=1, keepdims=True)


def couple_kernel(piece, row_count, col_count, before, out_count, *refs):
    row_refs = refs[:row_count]
    col_refs = refs[row_count : row_count + col_count]
    gain_ref, weight_ref = refs[-out_count - 2 : -out_count]
    sums = row_count // (gain_ref.shape[1] // piece)
    row_models, row_datas = [], []
    for at in range(0, row_count, sums):
        block = row_refs[at][...]
        if sums == 2:
            block = (
                block.astype(jnp.float32) + row_refs[at + 1][...].astype(jnp.float32)
            ).astype(jnp.bfloat16)
        row_models.append(block[:piece])
        row_datas.append(block[piece:])
    row_model = jnp.concatenate(row_models, axis=0)
    row_data = jnp.concatenate(row_datas, axis=0)
    row_power = power_of(row_model)[1]
    models, datas, powers = [], [], []
    for ref in col_refs:
        rate, power = power_of(ref[:piece])
        models.append(rate)
        powers.append(power)
        wide = ref[piece:].astype(jnp.float32)
        datas.append(rate_of(wide[:, :NF], wide[:, NF:]))
    col_model = jnp.concatenate(models, axis=0)
    col_data = jnp.concatenate(datas, axis=0)
    powers = jnp.concatenate(powers, axis=0)

    def diagonal(width):
        return lax.broadcasted_iota(jnp.int32, (width, width), 0) == lax.broadcasted_iota(
            jnp.int32, (width, width), 1
        )

    col_power = jnp.sum(
        jnp.where(diagonal(powers.shape[0]), powers, 0.0), axis=0, keepdims=True
    )
    height = gain_ref.shape[1]
    row_gain = jnp.sum(
        jnp.where(diagonal(height), gain_ref[...], 0.0), axis=1, keepdims=True
    )
    cross = lax.dot_general(
        row_model, col_model, CONTRACT_LAST, preferred_element_type=jnp.float32
    ) - lax.dot_general(row_data, col_data, CONTRACT_LAST, preferred_element_type=jnp.float32)
    normalizer = 0.5 * (row_power + col_power) + epsilon
    ratio = row_gain * cross / normalizer
    coupling = jnp.concatenate(
        [
            (weight_ref[at : at + 1, :] * ratio[at * piece : (at + 1) * piece]).astype(
                jnp.bfloat16
            )
            for at in range(height // piece)
        ],
        axis=0,
    )
    update = jnp.dot(coupling, col_model, preferred_element_type=jnp.float32)
    if before:
        update = update + refs[row_count + col_count][...]
    for place, out_ref in enumerate(refs[-out_count:]):
        rows = out_ref.shape[0]
        out_ref[...] = update[place * rows : (place + 1) * rows].astype(out_ref.dtype)


def couple(rows, cols, gains, weights, piece, outs, before=None, kind=jnp.bfloat16):
    args = [*rows, *cols] + ([] if before is None else [before]) + [gains, weights]
    height, width = gains.shape[1], weights.shape[1]
    return pl.pallas_call(
        functools.partial(
            couple_kernel, piece, len(rows), len(cols), before is not None, outs
        ),
        in_specs=[VMEM] * len(args),
        out_specs=[VMEM] * outs,
        out_shape=[jax.ShapeDtypeStruct((height // outs, 2 * NF), kind)] * outs,
        compiler_params=pltpu.CompilerParams(vmem_limit_bytes=16 << 20),
        cost_estimate=pl.CostEstimate(
            flops=12 * height * width * NF,
            bytes_accessed=8 * (height + width) * NF,
            transcendentals=0,
        ),
        name="couple",
    )(*args)


def to_time_kernel(count, flag_ref, *refs):
    basis_ref, out_ref = refs[2 * count], refs[-1]
    adjoint = jnp.concatenate(
        [
            jnp.where(flag_ref[1] == 1, here_ref[...], there_ref[...])
            for here_ref, there_ref in zip(refs[:count], refs[count : 2 * count])
        ],
        axis=0,
    )
    traces = lax.dot_general(
        adjoint, basis_ref[...], CONTRACT_LAST, preferred_element_type=jnp.float32
    )
    out_ref[...] = (traces * (1.0 / math.sqrt(NF))).astype(jnp.bfloat16)


def to_time(place, is_inner, here, there, basis, rows, before):
    span = basis.shape[0]
    half = sum(block.shape[0] for block in here)
    args = [*here, *there, basis]
    specs = [pl.BlockSpec(arg.shape, lambda j, flags: (0, 0)) for arg in args]
    aliases = {}
    if before is not None:
        aliases = {len(args) + 1: 0}
        specs.append(pl.BlockSpec(memory_space=pl.ANY))
        args.append(before)
    return pl.pallas_call(
        functools.partial(to_time_kernel, len(here)),
        grid_spec=pltpu.PrefetchScalarGridSpec(
            num_scalar_prefetch=1,
            grid=(1,),
            in_specs=specs,
            out_specs=pl.BlockSpec((half, span), lambda j, flags: (flags[0], j)),
        ),
        out_shape=jax.ShapeDtypeStruct((rows, span), jnp.bfloat16),
        input_output_aliases=aliases,
        compiler_params=pltpu.CompilerParams(vmem_limit_bytes=12 << 20),
        cost_estimate=pl.CostEstimate(
            flops=4 * half * span * NF, bytes_accessed=4 * span * NF, transcendentals=0
        ),
        name="to_time",
    )(jnp.stack([place, is_inner.astype(jnp.int32)]).astype(jnp.int32), *args)


def two_bases_kernel(per_step, low_rows, *refs):
    lc_ref, ls_ref = refs[4:6]
    for high, out_ref in zip((refs[:2], refs[2:4]), refs[6:]):
        basis_kernel(per_step, low_rows, *high, lc_ref, ls_ref, out_ref)


def two_bases(first, second, span):
    low_rows = math.gcd(span, 64)
    tables = []
    for start in (first, second):
        tables += cos_sin(start + jnp.arange(0, span, low_rows, dtype=jnp.int32))
    tables += cos_sin(jnp.arange(low_rows, dtype=jnp.int32))
    per_step = math.gcd(span // low_rows, 4)
    block = pl.BlockSpec((per_step * low_rows, 2 * NF), lambda i: (i, 0))
    return pl.pallas_call(
        functools.partial(two_bases_kernel, per_step, low_rows),
        grid=(span // low_rows // per_step,),
        in_specs=[pl.BlockSpec(table.shape, lambda i: (0, 0)) for table in tables],
        out_specs=[block, block],
        out_shape=[jax.ShapeDtypeStruct((span, 2 * NF), jnp.bfloat16)] * 2,
        compiler_params=pltpu.CompilerParams(vmem_limit_bytes=12 << 20),
        cost_estimate=pl.CostEstimate(
            flops=16 * span * NF, bytes_accessed=8 * span * NF, transcendentals=0
        ),
        name="two_bases",
    )(*tables)


def own_parts_kernel(count, *refs):
    basis_ref = refs[count]
    for block_ref, out_ref in zip(refs[:count], refs[count + 1 :]):
        out_ref[...] = jnp.dot(
            block_ref[...], basis_ref[...], preferred_element_type=jnp.float32
        )


def own_parts(blocks, basis):
    rows, span = blocks[0].shape
    return pl.pallas_call(
        functools.partial(own_parts_kernel, len(blocks)),
        in_specs=[VMEM] * (len(blocks) + 1),
        out_specs=[VMEM] * len(blocks),
        out_shape=[jax.ShapeDtypeStruct((rows, 2 * NF), jnp.float32)] * len(blocks),
        compiler_params=pltpu.CompilerParams(vmem_limit_bytes=12 << 20),
        cost_estimate=pl.CostEstimate(
            flops=4 * len(blocks) * rows * span * NF,
            bytes_accessed=4 * span * NF,
            transcendentals=0,
        ),
        name="own_parts",
    )(*blocks, basis)


def sum_kernel(part_ref, near_ref, basis_ref, *rest):
    total = part_ref[...] + jnp.dot(
        near_ref[...], basis_ref[...], preferred_element_type=jnp.float32
    )
    total = total * (1.0 / math.sqrt(NT))
    if len(rest) == 3:
        rest_ref, own_ref, sum_ref = rest
        own_ref[...] = (total + rest_ref[...].astype(jnp.float32)).astype(jnp.bfloat16)
    else:
        sum_ref = rest[0]
    sum_ref[...] = total.astype(jnp.bfloat16)


def spectra(part, near, basis, others=None):
    rows, span = near.shape
    args = [part, near, basis] + ([] if others is None else [others])
    outs = 1 if others is None else 2
    return pl.pallas_call(
        sum_kernel,
        in_specs=[VMEM] * len(args),
        out_specs=[VMEM] * outs,
        out_shape=[jax.ShapeDtypeStruct((rows, 2 * NF), jnp.bfloat16)] * outs,
        compiler_params=pltpu.CompilerParams(vmem_limit_bytes=12 << 20),
        cost_estimate=pl.CostEstimate(
            flops=4 * rows * span * NF, bytes_accessed=4 * span * NF, transcendentals=0
        ),
        name="spectra",
    )(*args)


def inner_body(synthetic, observed, station_weights, pair_mask):
    levels = lax.axis_size("blk")
    subs = lax.axis_size("sub")
    pairs = lax.axis_size("pair")
    level = lax.axis_index("blk")
    sub = lax.axis_index("sub")
    pair = lax.axis_index("pair")
    span = synthetic.shape[1]
    half = synthetic.shape[0] // 2
    per_half = levels // 2
    stations = station_weights.shape[0]
    piece = half // per_half
    side = level // 2
    inward, swapped, outward = [(0, 1), (3, 2)], [(1, 2), (2, 1)], [(1, 0), (2, 3)]

    def piece_of(which, at, sources):
        return jnp.concatenate(
            [
                lax.dynamic_slice_in_dim(source, which * half + at, piece, 0)
                for source in sources
            ],
            axis=0,
        )

    sources = (synthetic, observed)
    front = piece_of(1 - side, 0, sources)
    front, sources = lax.optimization_barrier((front, sources))
    passed = [front] + [piece_of(1 - side, at, sources) for at in range(piece, half, piece)]
    kept = [piece_of(side, at, sources) for at in range(0, half, piece)]
    near_passed, near_kept = [], []
    for blocks, arrived in ((passed, near_passed), (kept, near_kept)):
        for block in blocks:
            arrived.append(lax.ppermute(block, "blk", inward))

    member = sub * pairs + pair
    hops = [(s, q) for s in range(subs) for q in range(pairs)]
    starts = [
        ((sub - s) % subs * pairs + (pair - q) % pairs) * 2 * half + side * half + at
        for at in range(0, half, piece)
        for s, q in hops
    ]
    gains = station_weights.astype(jnp.float32)
    col_gains = jnp.concatenate(
        [lax.dynamic_slice_in_dim(gains, start, piece, 0) for start in starts]
    )[None, :]
    firsts = [member * 2 * half + which * half for which in (side, 1 - side)]
    own_gains, other_gains = [
        lax.dynamic_slice_in_dim(gains, start, half, 0)[None, :] for start in firsts
    ]
    link = jnp.maximum(pair_mask, pair_mask.T).astype(jnp.float32)
    link_rows = jnp.concatenate(
        [lax.dynamic_slice_in_dim(link, start // piece, per_half, 0) for start in firsts], axis=0
    )
    col_pieces = jnp.repeat(jnp.stack(starts) // piece, piece)
    chosen = jnp.arange(link.shape[0], dtype=jnp.int32)[:, None] == col_pieces[None, :]
    active = jnp.dot(
        link_rows, chosen.astype(jnp.float32), preferred_element_type=jnp.float32
    )
    weights = 4.0 / math.sqrt(stations) * col_gains * active
    late = (subs - 1) * pairs
    early_width = (len(starts) - late) * piece
    own_early, own_late = weights[:per_half, :early_width], weights[:per_half, early_width:]
    here, own_gains, other_gains, own_early, own_late, other_weights = lax.optimization_barrier(
        (level, own_gains, other_gains, own_early, own_late, weights[per_half:])
    )

    here_basis, near_basis = two_bases(here * span, (here ^ 1) * span, span)
    passed_parts = own_parts(passed, here_basis)
    kept_parts = own_parts(kept, here_basis)
    to_pass, kept_rest = [], []
    for place in range(per_half):
        (summed,) = spectra(passed_parts[place], near_passed[place], near_basis)
        to_pass.append(summed)
        kept_rest.append(lax.ppermute(summed, "blk", swapped))
    own, passed_rest, cols = [], [], {}
    for place in range(per_half):
        whole, summed = spectra(
            kept_parts[place], near_kept[place], near_basis, kept_rest[place]
        )
        own.append(whole)
        for s, q in hops:
            if q == 0:
                cols[s, q, place] = whole if s == 0 else shift(whole, "sub", s)
            else:
                cols[s, q, place] = shift(cols[s, 0, place], "pair", q)
        passed_rest.append(lax.ppermute(summed, "blk", swapped))
    cols = [cols[s, q, place] for place in range(per_half) for s, q in hops]
    (begun,) = couple(own, cols[:-late], own_gains, own_early, piece, 1, None, jnp.float32)
    own_part = couple(own, cols[-late:], own_gains, own_late, piece, per_half, begun)
    other = [block for both in zip(to_pass, passed_rest) for block in both]
    other_part = couple(other, cols, other_gains, other_weights, piece, per_half)

    def finish(sent, mine):
        sums, arrived = [], []
        for place in range(per_half):
            rest = lax.ppermute(sent[place], "blk", swapped)
            whole = mine[place].astype(jnp.float32) + rest.astype(jnp.float32)
            sums.append(whole.astype(jnp.bfloat16))
            arrived.append(lax.ppermute(sums[-1], "blk", outward))
        return sums, arrived

    first = finish(own_part, other_part)
    second = finish(other_part, own_part)
    is_inner = (level == 1) | (level == 2)
    rows = synthetic.shape[0]
    traces = to_time(1 - side, is_inner, *first, here_basis, rows, None)
    return to_time(side, is_inner, *second, here_basis, rows, traces)


def shards(*args):
    body = inner_body if lax.axis_size("blk") == 4 else ring_body
    return body(*args)


def solution(mesh):
    placed = (
        P(("events", "sub", "pair"), "blk"),
        P(("events", "sub", "pair"), "blk"),
        P("events"),
        P("events", None),
    )
    return jax.shard_map(
        shards,
        mesh=mesh,
        in_specs=placed,
        out_specs=P(("events", "sub", "pair"), "blk"),
        check_vma=False,
    )
```

```python
import functools
import math

import jax
import jax.numpy as jnp
from jax import lax
from jax.experimental import pallas as pl
from jax.experimental.pallas import tpu as pltpu
from jax.sharding import PartitionSpec as P


NT = 4096
NF = 512
F_LO = 64

epsilon = 1e-06
CONTRACT_LAST = (((1,), (1,)), ((), ()))
VMEM = pl.BlockSpec(memory_space=pltpu.VMEM)


def shift(value, axis, steps):
    count = lax.axis_size(axis)
    pairs = [(source, (source + steps) % count) for source in range(count)]
    return lax.ppermute(value, axis, pairs)


def sweep(count):
    order = []
    for near in range(1, count // 2 + 1):
        order.append(near)
        if (count - near) % count != near:
            order.append(count - near)
    return order


def cos_sin(samples):
    bins = F_LO + jnp.arange(NF, dtype=jnp.int32)
    phases = samples[:, None] * bins[None, :] % NT
    angles = phases.astype(jnp.float32) * (2.0 * math.pi / NT)
    return jnp.cos(angles), jnp.sin(angles)


def basis_kernel(per_step, low_rows, hc_ref, hs_ref, lc_ref, ls_ref, out_ref):
    step = pl.program_id(0)
    for h in range(per_step):
        hc = hc_ref[pl.ds(step * per_step + h, 1), :]
        hs = hs_ref[pl.ds(step * per_step + h, 1), :]
        lc = lc_ref[...]
        ls = ls_ref[...]
        rows = slice(h * low_rows, (h + 1) * low_rows)
        out_ref[rows, :NF] = (hc * lc - hs * ls).astype(jnp.bfloat16)
        out_ref[rows, NF:] = (-(hs * lc + hc * ls)).astype(jnp.bfloat16)


def make_basis(firsts, span):
    low_rows = math.gcd(span, 64)
    low_c, low_s = cos_sin(jnp.arange(low_rows, dtype=jnp.int32))
    highs = (firsts[:, None] + jnp.arange(0, span, low_rows, dtype=jnp.int32)[None, :]).reshape(-1)
    high_c, high_s = cos_sin(highs)
    per_step = math.gcd(highs.shape[0], 4)
    whole = lambda a: pl.BlockSpec(a.shape, lambda i: (0, 0))
    rows = highs.shape[0] * low_rows
    return pl.pallas_call(
        functools.partial(basis_kernel, per_step, low_rows),
        grid=(highs.shape[0] // per_step,),
        in_specs=[whole(high_c), whole(high_s), whole(low_c), whole(low_s)],
        out_specs=pl.BlockSpec((per_step * low_rows, 2 * NF), lambda i: (i, 0)),
        out_shape=jax.ShapeDtypeStruct((rows, 2 * NF), jnp.bfloat16),
        cost_estimate=pl.CostEstimate(
            flops=8 * rows * NF, bytes_accessed=4 * rows * NF, transcendentals=0
        ),
        compiler_params=pltpu.CompilerParams(vmem_limit_bytes=16 << 20),
        name="basis",
    )(high_c, high_s, low_c, low_s)


def angular_row():
    bins = F_LO + lax.broadcasted_iota(jnp.int32, (1, NF), 1)
    return 2.0 * math.pi / NT * bins.astype(jnp.float32)


def rate_of(re, im):
    angular = angular_row()
    return jnp.concatenate([-angular * im, angular * re], axis=1).astype(jnp.bfloat16)


def tile_kernel(first, rows_ref, power_ref, coef_ref, gain_ref, col_ref, *rest):
    out_ref = rest[-1]
    col = col_ref[...].astype(jnp.float32)
    model_rate = rate_of(col[:, :NF], col[:, NF : 2 * NF])
    data_rate = rate_of(-col[:, 2 * NF : 3 * NF], -col[:, 3 * NF :])
    both = jnp.concatenate([model_rate, data_rate], axis=1)
    cross = lax.dot_general(
        rows_ref[...], both, CONTRACT_LAST, preferred_element_type=jnp.float32
    )
    col_power = lax.dot_general(
        jnp.ones((8, 2 * NF), jnp.float32),
        jnp.square(model_rate.astype(jnp.float32)),
        CONTRACT_LAST,
        precision=lax.Precision.HIGHEST,
        preferred_element_type=jnp.float32,
    )[0:1, :]
    normalizer = 0.5 * (power_ref[...] + col_power) + epsilon
    coupling = (coef_ref[...] * gain_ref[...] * cross / normalizer).astype(jnp.bfloat16)
    update = jnp.dot(coupling, model_rate, preferred_element_type=jnp.float32)
    if first:
        out_ref[...] = update
    else:
        out_ref[...] = rest[0][...] + update


def pair_tile(running, rows, row_power, coef, gain, col):
    args = [rows, row_power, coef, gain, col]
    aliases = {}
    if running is not None:
        aliases = {len(args): 0}
        args.append(running)
    height, width = rows.shape[0], col.shape[0]
    return pl.pallas_call(
        functools.partial(tile_kernel, running is None),
        in_specs=[pl.BlockSpec(memory_space=pltpu.VMEM)] * len(args),
        out_specs=pl.BlockSpec(memory_space=pltpu.VMEM),
        out_shape=jax.ShapeDtypeStruct((height, 2 * NF), jnp.float32),
        input_output_aliases=aliases,
        cost_estimate=pl.CostEstimate(
            flops=12 * height * width * NF,
            bytes_accessed=16 * height * NF,
            transcendentals=0,
        ),
        name="pair_tile",
    )(*args)


def ring_body(synthetic, observed, station_weights, pair_mask):
    levels = lax.axis_size("blk")
    subs = lax.axis_size("sub")
    pairs = lax.axis_size("pair")
    level = lax.axis_index("blk")
    sub = lax.axis_index("sub")
    pair = lax.axis_index("pair")
    span = synthetic.shape[1]
    piece = synthetic.shape[0] // levels
    stations = station_weights.shape[0]

    def owned_by(steps):
        owner = (level + steps) % levels
        return jnp.concatenate(
            [
                lax.dynamic_slice_in_dim(synthetic, owner * piece, piece, 0),
                lax.dynamic_slice_in_dim(observed, owner * piece, piece, 0),
            ],
            axis=0,
        )

    order = sweep(levels)
    blocks = {0: owned_by(0)}
    for steps in order:
        blocks[steps] = shift(owned_by(steps), "blk", steps)
    arrivals = [0] + order
    firsts = jnp.stack([(level - steps) % levels * span for steps in arrivals]).astype(jnp.int32)
    basis = make_basis(firsts, span)
    member = sub * pairs + pair
    members = jnp.stack(
        [
            (sub - s) % subs * pairs + (pair - q) % pairs
            for s in range(subs)
            for q in range(pairs)
        ]
    )
    gains = station_weights.astype(jnp.float32).reshape(-1, piece)
    link = jnp.maximum(pair_mask, pair_mask.T).astype(jnp.float32)
    row_pieces = members * levels + level
    row_gain = gains[row_pieces].reshape(-1, 1)
    row_link = link[row_pieces]
    factor = 4.0 / math.sqrt(stations)
    coefs, col_gains = [], []
    for steps in arrivals:
        column_piece = member * levels + (level - steps) % levels
        active = lax.dynamic_slice_in_dim(row_link, column_piece, 1, 1)
        coefs.append(factor * row_gain * jnp.repeat(active, piece, axis=0))
        col_gains.append(lax.dynamic_slice_in_dim(gains, column_piece, 1, 0))
    last = order[-1]
    blocks[last], coefs, col_gains = lax.optimization_barrier((blocks[last], coefs, col_gains))
    total = None
    for place, steps in enumerate(arrivals):
        part = jnp.dot(
            blocks[steps],
            basis[place * span : (place + 1) * span],
            preferred_element_type=jnp.float32,
        )
        total = part if total is None else total + part
    spec = (total * (1.0 / math.sqrt(NT))).astype(jnp.bfloat16)
    own = jnp.concatenate([spec[:piece], spec[piece:]], axis=1)

    columns = {0: own}
    for steps in order:
        columns[steps] = shift(own, "blk", steps)
    blocks_of_rows = []
    for s in range(subs):
        here = own if s == 0 else shift(own, "sub", s)
        for q in range(pairs):
            blocks_of_rows.append(here if q == 0 else shift(here, "pair", q))
    rows = jnp.concatenate(blocks_of_rows, axis=0)
    widened = rows[:, : 2 * NF].astype(jnp.float32)
    row_rate = rate_of(widened[:, :NF], widened[:, NF:])
    row_power = jnp.sum(jnp.square(row_rate.astype(jnp.float32)), axis=1, keepdims=True)

    running = None
    for place, steps in enumerate(arrivals):
        running = pair_tile(
            running, rows, row_power, coefs[place], col_gains[place], columns[steps]
        )

    partial = running.reshape(subs, pairs, piece, 2 * NF)
    held = partial[:, 0]
    for q in range(1, pairs):
        sent = partial[:, q].astype(jnp.bfloat16)
        held = held + shift(sent, "pair", -q).astype(jnp.float32)
    adjoint = held[0]
    for s in range(1, subs):
        adjoint = adjoint + shift(held[s].astype(jnp.bfloat16), "sub", -s).astype(jnp.float32)
    adjoint = adjoint.astype(jnp.bfloat16)

    gathered = jnp.zeros((levels * piece, 2 * NF), jnp.bfloat16)
    for steps in arrivals:
        arrived = adjoint if steps == 0 else shift(adjoint, "blk", steps)
        gathered = lax.dynamic_update_slice_in_dim(
            gathered, arrived, (level - steps) % levels * piece, 0
        )
    return (
        lax.dot_general(
            gathered, basis[:span], CONTRACT_LAST, preferred_element_type=jnp.float32
        )
        * (1.0 / math.sqrt(NF))
    ).astype(jnp.bfloat16)


def power_of(spec):
    wide = spec.astype(jnp.float32)
    rate = rate_of(wide[:, :NF], wide[:, NF:])
    return rate, jnp.sum(jnp.square(rate.astype(jnp.float32)), axis=1, keepdims=True)


def couple_kernel(piece, row_count, col_count, before, out_count, *refs):
    row_refs = refs[:row_count]
    col_refs = refs[row_count : row_count + col_count]
    gain_ref, weight_ref = refs[-out_count - 2 : -out_count]
    sums = row_count // (gain_ref.shape[1] // piece)
    row_models, row_datas = [], []
    for at in range(0, row_count, sums):
        block = row_refs[at][...]
        if sums == 2:
            block = (
                block.astype(jnp.float32) + row_refs[at + 1][...].astype(jnp.float32)
            ).astype(jnp.bfloat16)
        row_models.append(block[:piece])
        row_datas.append(block[piece:])
    row_model = jnp.concatenate(row_models, axis=0)
    row_data = jnp.concatenate(row_datas, axis=0)
    row_power = power_of(row_model)[1]
    models, datas, powers = [], [], []
    for ref in col_refs:
        rate, power = power_of(ref[:piece])
        models.append(rate)
        powers.append(power)
        wide = ref[piece:].astype(jnp.float32)
        datas.append(rate_of(wide[:, :NF], wide[:, NF:]))
    col_model = jnp.concatenate(models, axis=0)
    col_data = jnp.concatenate(datas, axis=0)
    powers = jnp.concatenate(powers, axis=0)

    def diagonal(width):
        return lax.broadcasted_iota(jnp.int32, (width, width), 0) == lax.broadcasted_iota(
            jnp.int32, (width, width), 1
        )

    col_power = jnp.sum(
        jnp.where(diagonal(powers.shape[0]), powers, 0.0), axis=0, keepdims=True
    )
    height = gain_ref.shape[1]
    row_gain = jnp.sum(
        jnp.where(diagonal(height), gain_ref[...], 0.0), axis=1, keepdims=True
    )
    cross = lax.dot_general(
        row_model, col_model, CONTRACT_LAST, preferred_element_type=jnp.float32
    ) - lax.dot_general(row_data, col_data, CONTRACT_LAST, preferred_element_type=jnp.float32)
    normalizer = 0.5 * (row_power + col_power) + epsilon
    ratio = row_gain * cross / normalizer
    coupling = jnp.concatenate(
        [
            (weight_ref[at : at + 1, :] * ratio[at * piece : (at + 1) * piece]).astype(
                jnp.bfloat16
            )
            for at in range(height // piece)
        ],
        axis=0,
    )
    update = jnp.dot(coupling, col_model, preferred_element_type=jnp.float32)
    if before:
        update = update + refs[row_count + col_count][...]
    for place, out_ref in enumerate(refs[-out_count:]):
        rows = out_ref.shape[0]
        out_ref[...] = update[place * rows : (place + 1) * rows].astype(out_ref.dtype)


def couple(rows, cols, gains, weights, piece, outs, before=None, kind=jnp.bfloat16):
    args = [*rows, *cols] + ([] if before is None else [before]) + [gains, weights]
    height, width = gains.shape[1], weights.shape[1]
    return pl.pallas_call(
        functools.partial(
            couple_kernel, piece, len(rows), len(cols), before is not None, outs
        ),
        in_specs=[VMEM] * len(args),
        out_specs=[VMEM] * outs,
        out_shape=[jax.ShapeDtypeStruct((height // outs, 2 * NF), kind)] * outs,
        compiler_params=pltpu.CompilerParams(vmem_limit_bytes=16 << 20),
        cost_estimate=pl.CostEstimate(
            flops=12 * height * width * NF,
            bytes_accessed=8 * (height + width) * NF,
            transcendentals=0,
        ),
        name="couple",
    )(*args)


def to_time_kernel(count, flag_ref, *refs):
    basis_ref, out_ref = refs[2 * count], refs[-1]
    adjoint = jnp.concatenate(
        [
            jnp.where(flag_ref[1] == 1, here_ref[...], there_ref[...])
            for here_ref, there_ref in zip(refs[:count], refs[count : 2 * count])
        ],
        axis=0,
    )
    traces = lax.dot_general(
        adjoint, basis_ref[...], CONTRACT_LAST, preferred_element_type=jnp.float32
    )
    out_ref[...] = (traces * (1.0 / math.sqrt(NF))).astype(jnp.bfloat16)


def to_time(place, is_inner, here, there, basis, rows, before):
    span = basis.shape[0]
    half = sum(block.shape[0] for block in here)
    args = [*here, *there, basis]
    specs = [pl.BlockSpec(arg.shape, lambda j, flags: (0, 0)) for arg in args]
    aliases = {}
    if before is not None:
        aliases = {len(args) + 1: 0}
        specs.append(pl.BlockSpec(memory_space=pl.ANY))
        args.append(before)
    return pl.pallas_call(
        functools.partial(to_time_kernel, len(here)),
        grid_spec=pltpu.PrefetchScalarGridSpec(
            num_scalar_prefetch=1,
            grid=(1,),
            in_specs=specs,
            out_specs=pl.BlockSpec((half, span), lambda j, flags: (flags[0], j)),
        ),
        out_shape=jax.ShapeDtypeStruct((rows, span), jnp.bfloat16),
        input_output_aliases=aliases,
        compiler_params=pltpu.CompilerParams(vmem_limit_bytes=12 << 20),
        cost_estimate=pl.CostEstimate(
            flops=4 * half * span * NF, bytes_accessed=4 * span * NF, transcendentals=0
        ),
        name="to_time",
    )(jnp.stack([place, is_inner.astype(jnp.int32)]).astype(jnp.int32), *args)


def two_bases_kernel(per_step, low_rows, *refs):
    lc_ref, ls_ref = refs[4:6]
    for high, out_ref in zip((refs[:2], refs[2:4]), refs[6:]):
        basis_kernel(per_step, low_rows, *high, lc_ref, ls_ref, out_ref)


def two_bases(first, second, span):
    low_rows = math.gcd(span, 64)
    tables = []
    for start in (first, second):
        tables += cos_sin(start + jnp.arange(0, span, low_rows, dtype=jnp.int32))
    tables += cos_sin(jnp.arange(low_rows, dtype=jnp.int32))
    per_step = math.gcd(span // low_rows, 4)
    block = pl.BlockSpec((per_step * low_rows, 2 * NF), lambda i: (i, 0))
    return pl.pallas_call(
        functools.partial(two_bases_kernel, per_step, low_rows),
        grid=(span // low_rows // per_step,),
        in_specs=[pl.BlockSpec(table.shape, lambda i: (0, 0)) for table in tables],
        out_specs=[block, block],
        out_shape=[jax.ShapeDtypeStruct((span, 2 * NF), jnp.bfloat16)] * 2,
        compiler_params=pltpu.CompilerParams(vmem_limit_bytes=12 << 20),
        cost_estimate=pl.CostEstimate(
            flops=16 * span * NF, bytes_accessed=8 * span * NF, transcendentals=0
        ),
        name="two_bases",
    )(*tables)


def own_parts_kernel(count, *refs):
    basis_ref = refs[count]
    for block_ref, out_ref in zip(refs[:count], refs[count + 1 :]):
        out_ref[...] = jnp.dot(
            block_ref[...], basis_ref[...], preferred_element_type=jnp.float32
        )


def own_parts(blocks, basis):
    rows, span = blocks[0].shape
    return pl.pallas_call(
        functools.partial(own_parts_kernel, len(blocks)),
        in_specs=[VMEM] * (len(blocks) + 1),
        out_specs=[VMEM] * len(blocks),
        out_shape=[jax.ShapeDtypeStruct((rows, 2 * NF), jnp.float32)] * len(blocks),
        compiler_params=pltpu.CompilerParams(vmem_limit_bytes=12 << 20),
        cost_estimate=pl.CostEstimate(
            flops=4 * len(blocks) * rows * span * NF,
            bytes_accessed=4 * span * NF,
            transcendentals=0,
        ),
        name="own_parts",
    )(*blocks, basis)


def sum_kernel(part_ref, near_ref, basis_ref, *rest):
    total = part_ref[...] + jnp.dot(
        near_ref[...], basis_ref[...], preferred_element_type=jnp.float32
    )
    total = total * (1.0 / math.sqrt(NT))
    if len(rest) == 3:
        rest_ref, own_ref, sum_ref = rest
        own_ref[...] = (total + rest_ref[...].astype(jnp.float32)).astype(jnp.bfloat16)
    else:
        sum_ref = rest[0]
    sum_ref[...] = total.astype(jnp.bfloat16)


def spectra(part, near, basis, others=None):
    rows, span = near.shape
    args = [part, near, basis] + ([] if others is None else [others])
    outs = 1 if others is None else 2
    return pl.pallas_call(
        sum_kernel,
        in_specs=[VMEM] * len(args),
        out_specs=[VMEM] * outs,
        out_shape=[jax.ShapeDtypeStruct((rows, 2 * NF), jnp.bfloat16)] * outs,
        compiler_params=pltpu.CompilerParams(vmem_limit_bytes=12 << 20),
        cost_estimate=pl.CostEstimate(
            flops=4 * rows * span * NF, bytes_accessed=4 * span * NF, transcendentals=0
        ),
        name="spectra",
    )(*args)


def inner_body(synthetic, observed, station_weights, pair_mask):
    levels = lax.axis_size("blk")
    subs = lax.axis_size("sub")
    pairs = lax.axis_size("pair")
    level = lax.axis_index("blk")
    sub = lax.axis_index("sub")
    pair = lax.axis_index("pair")
    span = synthetic.shape[1]
    half = synthetic.shape[0] // 2
    per_half = levels // 2
    stations = station_weights.shape[0]
    piece = half // per_half
    side = level // 2
    inward, swapped, outward = [(0, 1), (3, 2)], [(1, 2), (2, 1)], [(1, 0), (2, 3)]

    def piece_of(which, at, sources):
        return jnp.concatenate(
            [
                lax.dynamic_slice_in_dim(source, which * half + at, piece, 0)
                for source in sources
            ],
            axis=0,
        )

    sources = (synthetic, observed)
    front = piece_of(1 - side, 0, sources)
    front, sources = lax.optimization_barrier((front, sources))
    passed = [front] + [piece_of(1 - side, at, sources) for at in range(piece, half, piece)]
    kept = [piece_of(side, at, sources) for at in range(0, half, piece)]
    near_passed, near_kept = [], []
    for blocks, arrived in ((passed, near_passed), (kept, near_kept)):
        for block in blocks:
            arrived.append(lax.ppermute(block, "blk", inward))

    member = sub * pairs + pair
    hops = [(s, q) for s in range(subs) for q in range(pairs)]
    starts = [
        ((sub - s) % subs * pairs + (pair - q) % pairs) * 2 * half + side * half + at
        for at in range(0, half, piece)
        for s, q in hops
    ]
    gains = station_weights.astype(jnp.float32)
    col_gains = jnp.concatenate(
        [lax.dynamic_slice_in_dim(gains, start, piece, 0) for start in starts]
    )[None, :]
    firsts = [member * 2 * half + which * half for which in (side, 1 - side)]
    own_gains, other_gains = [
        lax.dynamic_slice_in_dim(gains, start, half, 0)[None, :] for start in firsts
    ]
    link = jnp.maximum(pair_mask, pair_mask.T).astype(jnp.float32)
    link_rows = jnp.concatenate(
        [lax.dynamic_slice_in_dim(link, start // piece, per_half, 0) for start in firsts], axis=0
    )
    col_pieces = jnp.repeat(jnp.stack(starts) // piece, piece)
    chosen = jnp.arange(link.shape[0], dtype=jnp.int32)[:, None] == col_pieces[None, :]
    active = jnp.dot(
        link_rows, chosen.astype(jnp.float32), preferred_element_type=jnp.float32
    )
    weights = 4.0 / math.sqrt(stations) * col_gains * active
    late = (subs - 1) * pairs
    early_width = (len(starts) - late) * piece
    own_early, own_late = weights[:per_half, :early_width], weights[:per_half, early_width:]
    here, own_gains, other_gains, own_early, own_late, other_weights = lax.optimization_barrier(
        (level, own_gains, other_gains, own_early, own_late, weights[per_half:])
    )

    here_basis, near_basis = two_bases(here * span, (here ^ 1) * span, span)
    passed_parts = own_parts(passed, here_basis)
    kept_parts = own_parts(kept, here_basis)
    to_pass, kept_rest = [], []
    for place in range(per_half):
        (summed,) = spectra(passed_parts[place], near_passed[place], near_basis)
        to_pass.append(summed)
        kept_rest.append(lax.ppermute(summed, "blk", swapped))
    own, passed_rest, cols = [], [], {}
    for place in range(per_half):
        whole, summed = spectra(
            kept_parts[place], near_kept[place], near_basis, kept_rest[place]
        )
        own.append(whole)
        for s, q in hops:
            if q == 0:
                cols[s, q, place] = whole if s == 0 else shift(whole, "sub", s)
            else:
                cols[s, q, place] = shift(cols[s, 0, place], "pair", q)
        passed_rest.append(lax.ppermute(summed, "blk", swapped))
    cols = [cols[s, q, place] for place in range(per_half) for s, q in hops]
    (begun,) = couple(own, cols[:-late], own_gains, own_early, piece, 1, None, jnp.float32)
    own_part = couple(own, cols[-late:], own_gains, own_late, piece, per_half, begun)
    other = [block for both in zip(to_pass, passed_rest) for block in both]
    other_part = couple(other, cols, other_gains, other_weights, piece, per_half)

    def finish(sent, mine):
        sums, arrived = [], []
        for place in range(per_half):
            rest = lax.ppermute(sent[place], "blk", swapped)
            whole = mine[place].astype(jnp.float32) + rest.astype(jnp.float32)
            sums.append(whole.astype(jnp.bfloat16))
            arrived.append(lax.ppermute(sums[-1], "blk", outward))
        return sums, arrived

    first = finish(own_part, other_part)
    second = finish(other_part, own_part)
    is_inner = (level == 1) | (level == 2)
    rows = synthetic.shape[0]
    traces = to_time(1 - side, is_inner, *first, here_basis, rows, None)
    for place, (mine, arrived) in enumerate(zip(*second)):
        block = side * per_half + place
        traces = to_time(block, is_inner, [mine], [arrived], here_basis, rows, traces)
    return traces


def shards(*args):
    body = inner_body if lax.axis_size("blk") == 4 else ring_body
    return body(*args)


def solution(mesh):
    placed = (
        P(("events", "sub", "pair"), "blk"),
        P(("events", "sub", "pair"), "blk"),
        P("events"),
        P("events", None),
    )
    return jax.shard_map(
        shards,
        mesh=mesh,
        in_specs=placed,
        out_specs=P(("events", "sub", "pair"), "blk"),
        check_vma=False,
    )
```

```python
import functools
import math

import jax
import jax.numpy as jnp
from jax import lax
from jax.experimental import pallas as pl
from jax.experimental.pallas import tpu as pltpu
from jax.sharding import PartitionSpec as P


NT = 4096
NF = 512
F_LO = 64

epsilon = 1e-06
CONTRACT_LAST = (((1,), (1,)), ((), ()))
VMEM = pl.BlockSpec(memory_space=pltpu.VMEM)


def shift(value, axis, steps):
    count = lax.axis_size(axis)
    pairs = [(source, (source + steps) % count) for source in range(count)]
    return lax.ppermute(value, axis, pairs)


def sweep(count):
    order = []
    for near in range(1, count // 2 + 1):
        order.append(near)
        if (count - near) % count != near:
            order.append(count - near)
    return order


def cos_sin(samples):
    bins = F_LO + jnp.arange(NF, dtype=jnp.int32)
    phases = samples[:, None] * bins[None, :] % NT
    angles = phases.astype(jnp.float32) * (2.0 * math.pi / NT)
    return jnp.cos(angles), jnp.sin(angles)


def basis_kernel(per_step, low_rows, hc_ref, hs_ref, lc_ref, ls_ref, out_ref):
    step = pl.program_id(0)
    for h in range(per_step):
        hc = hc_ref[pl.ds(step * per_step + h, 1), :]
        hs = hs_ref[pl.ds(step * per_step + h, 1), :]
        lc = lc_ref[...]
        ls = ls_ref[...]
        rows = slice(h * low_rows, (h + 1) * low_rows)
        out_ref[rows, :NF] = (hc * lc - hs * ls).astype(jnp.bfloat16)
        out_ref[rows, NF:] = (-(hs * lc + hc * ls)).astype(jnp.bfloat16)


def make_basis(firsts, span):
    low_rows = math.gcd(span, 64)
    low_c, low_s = cos_sin(jnp.arange(low_rows, dtype=jnp.int32))
    highs = (firsts[:, None] + jnp.arange(0, span, low_rows, dtype=jnp.int32)[None, :]).reshape(-1)
    high_c, high_s = cos_sin(highs)
    per_step = math.gcd(highs.shape[0], 4)
    whole = lambda a: pl.BlockSpec(a.shape, lambda i: (0, 0))
    rows = highs.shape[0] * low_rows
    return pl.pallas_call(
        functools.partial(basis_kernel, per_step, low_rows),
        grid=(highs.shape[0] // per_step,),
        in_specs=[whole(high_c), whole(high_s), whole(low_c), whole(low_s)],
        out_specs=pl.BlockSpec((per_step * low_rows, 2 * NF), lambda i: (i, 0)),
        out_shape=jax.ShapeDtypeStruct((rows, 2 * NF), jnp.bfloat16),
        cost_estimate=pl.CostEstimate(
            flops=8 * rows * NF, bytes_accessed=4 * rows * NF, transcendentals=0
        ),
        compiler_params=pltpu.CompilerParams(vmem_limit_bytes=16 << 20),
        name="basis",
    )(high_c, high_s, low_c, low_s)


def angular_row():
    bins = F_LO + lax.broadcasted_iota(jnp.int32, (1, NF), 1)
    return 2.0 * math.pi / NT * bins.astype(jnp.float32)


def rate_of(re, im):
    angular = angular_row()
    return jnp.concatenate([-angular * im, angular * re], axis=1).astype(jnp.bfloat16)


def tile_kernel(first, rows_ref, power_ref, coef_ref, gain_ref, col_ref, *rest):
    out_ref = rest[-1]
    col = col_ref[...].astype(jnp.float32)
    model_rate = rate_of(col[:, :NF], col[:, NF : 2 * NF])
    data_rate = rate_of(-col[:, 2 * NF : 3 * NF], -col[:, 3 * NF :])
    both = jnp.concatenate([model_rate, data_rate], axis=1)
    cross = lax.dot_general(
        rows_ref[...], both, CONTRACT_LAST, preferred_element_type=jnp.float32
    )
    col_power = lax.dot_general(
        jnp.ones((8, 2 * NF), jnp.float32),
        jnp.square(model_rate.astype(jnp.float32)),
        CONTRACT_LAST,
        precision=lax.Precision.HIGHEST,
        preferred_element_type=jnp.float32,
    )[0:1, :]
    normalizer = 0.5 * (power_ref[...] + col_power) + epsilon
    coupling = (coef_ref[...] * gain_ref[...] * cross / normalizer).astype(jnp.bfloat16)
    update = jnp.dot(coupling, model_rate, preferred_element_type=jnp.float32)
    if first:
        out_ref[...] = update
    else:
        out_ref[...] = rest[0][...] + update


def pair_tile(running, rows, row_power, coef, gain, col):
    args = [rows, row_power, coef, gain, col]
    aliases = {}
    if running is not None:
        aliases = {len(args): 0}
        args.append(running)
    height, width = rows.shape[0], col.shape[0]
    return pl.pallas_call(
        functools.partial(tile_kernel, running is None),
        in_specs=[pl.BlockSpec(memory_space=pltpu.VMEM)] * len(args),
        out_specs=pl.BlockSpec(memory_space=pltpu.VMEM),
        out_shape=jax.ShapeDtypeStruct((height, 2 * NF), jnp.float32),
        input_output_aliases=aliases,
        cost_estimate=pl.CostEstimate(
            flops=12 * height * width * NF,
            bytes_accessed=16 * height * NF,
            transcendentals=0,
        ),
        name="pair_tile",
    )(*args)


def ring_body(synthetic, observed, station_weights, pair_mask):
    levels = lax.axis_size("blk")
    subs = lax.axis_size("sub")
    pairs = lax.axis_size("pair")
    level = lax.axis_index("blk")
    sub = lax.axis_index("sub")
    pair = lax.axis_index("pair")
    span = synthetic.shape[1]
    piece = synthetic.shape[0] // levels
    stations = station_weights.shape[0]

    def owned_by(steps):
        owner = (level + steps) % levels
        return jnp.concatenate(
            [
                lax.dynamic_slice_in_dim(synthetic, owner * piece, piece, 0),
                lax.dynamic_slice_in_dim(observed, owner * piece, piece, 0),
            ],
            axis=0,
        )

    order = sweep(levels)
    blocks = {0: owned_by(0)}
    for steps in order:
        blocks[steps] = shift(owned_by(steps), "blk", steps)
    arrivals = [0] + order
    firsts = jnp.stack([(level - steps) % levels * span for steps in arrivals]).astype(jnp.int32)
    basis = make_basis(firsts, span)
    member = sub * pairs + pair
    members = jnp.stack(
        [
            (sub - s) % subs * pairs + (pair - q) % pairs
            for s in range(subs)
            for q in range(pairs)
        ]
    )
    gains = station_weights.astype(jnp.float32).reshape(-1, piece)
    link = jnp.maximum(pair_mask, pair_mask.T).astype(jnp.float32)
    row_pieces = members * levels + level
    row_gain = gains[row_pieces].reshape(-1, 1)
    row_link = link[row_pieces]
    factor = 4.0 / math.sqrt(stations)
    coefs, col_gains = [], []
    for steps in arrivals:
        column_piece = member * levels + (level - steps) % levels
        active = lax.dynamic_slice_in_dim(row_link, column_piece, 1, 1)
        coefs.append(factor * row_gain * jnp.repeat(active, piece, axis=0))
        col_gains.append(lax.dynamic_slice_in_dim(gains, column_piece, 1, 0))
    last = order[-1]
    blocks[last], coefs, col_gains = lax.optimization_barrier((blocks[last], coefs, col_gains))
    total = None
    for place, steps in enumerate(arrivals):
        part = jnp.dot(
            blocks[steps],
            basis[place * span : (place + 1) * span],
            preferred_element_type=jnp.float32,
        )
        total = part if total is None else total + part
    spec = (total * (1.0 / math.sqrt(NT))).astype(jnp.bfloat16)
    own = jnp.concatenate([spec[:piece], spec[piece:]], axis=1)

    columns = {0: own}
    for steps in order:
        columns[steps] = shift(own, "blk", steps)
    blocks_of_rows = []
    for s in range(subs):
        here = own if s == 0 else shift(own, "sub", s)
        for q in range(pairs):
            blocks_of_rows.append(here if q == 0 else shift(here, "pair", q))
    rows = jnp.concatenate(blocks_of_rows, axis=0)
    widened = rows[:, : 2 * NF].astype(jnp.float32)
    row_rate = rate_of(widened[:, :NF], widened[:, NF:])
    row_power = jnp.sum(jnp.square(row_rate.astype(jnp.float32)), axis=1, keepdims=True)

    running = None
    for place, steps in enumerate(arrivals):
        running = pair_tile(
            running, rows, row_power, coefs[place], col_gains[place], columns[steps]
        )

    partial = running.reshape(subs, pairs, piece, 2 * NF)
    held = partial[:, 0]
    for q in range(1, pairs):
        sent = partial[:, q].astype(jnp.bfloat16)
        held = held + shift(sent, "pair", -q).astype(jnp.float32)
    adjoint = held[0]
    for s in range(1, subs):
        adjoint = adjoint + shift(held[s].astype(jnp.bfloat16), "sub", -s).astype(jnp.float32)
    adjoint = adjoint.astype(jnp.bfloat16)

    gathered = jnp.zeros((levels * piece, 2 * NF), jnp.bfloat16)
    for steps in arrivals:
        arrived = adjoint if steps == 0 else shift(adjoint, "blk", steps)
        gathered = lax.dynamic_update_slice_in_dim(
            gathered, arrived, (level - steps) % levels * piece, 0
        )
    return (
        lax.dot_general(
            gathered, basis[:span], CONTRACT_LAST, preferred_element_type=jnp.float32
        )
        * (1.0 / math.sqrt(NF))
    ).astype(jnp.bfloat16)


def power_of(spec):
    wide = spec.astype(jnp.float32)
    rate = rate_of(wide[:, :NF], wide[:, NF:])
    return rate, jnp.sum(jnp.square(rate.astype(jnp.float32)), axis=1, keepdims=True)


def couple_kernel(piece, row_count, col_count, before, out_count, *refs):
    row_refs = refs[:row_count]
    col_refs = refs[row_count : row_count + col_count]
    gain_ref, weight_ref = refs[-out_count - 2 : -out_count]
    sums = row_count // (gain_ref.shape[1] // piece)
    row_models, row_datas = [], []
    for at in range(0, row_count, sums):
        block = row_refs[at][...]
        if sums == 2:
            block = (
                block.astype(jnp.float32) + row_refs[at + 1][...].astype(jnp.float32)
            ).astype(jnp.bfloat16)
        row_models.append(block[:piece])
        row_datas.append(block[piece:])
    row_model = jnp.concatenate(row_models, axis=0)
    row_data = jnp.concatenate(row_datas, axis=0)
    row_power = power_of(row_model)[1]
    models, datas, powers = [], [], []
    for ref in col_refs:
        rate, power = power_of(ref[:piece])
        models.append(rate)
        powers.append(power)
        wide = ref[piece:].astype(jnp.float32)
        datas.append(rate_of(wide[:, :NF], wide[:, NF:]))
    col_model = jnp.concatenate(models, axis=0)
    col_data = jnp.concatenate(datas, axis=0)
    powers = jnp.concatenate(powers, axis=0)

    def diagonal(width):
        return lax.broadcasted_iota(jnp.int32, (width, width), 0) == lax.broadcasted_iota(
            jnp.int32, (width, width), 1
        )

    col_power = jnp.sum(
        jnp.where(diagonal(powers.shape[0]), powers, 0.0), axis=0, keepdims=True
    )
    height = gain_ref.shape[1]
    row_gain = jnp.sum(
        jnp.where(diagonal(height), gain_ref[...], 0.0), axis=1, keepdims=True
    )
    cross = lax.dot_general(
        row_model, col_model, CONTRACT_LAST, preferred_element_type=jnp.float32
    ) - lax.dot_general(row_data, col_data, CONTRACT_LAST, preferred_element_type=jnp.float32)
    normalizer = 0.5 * (row_power + col_power) + epsilon
    ratio = row_gain * cross / normalizer
    coupling = jnp.concatenate(
        [
            (weight_ref[at : at + 1, :] * ratio[at * piece : (at + 1) * piece]).astype(
                jnp.bfloat16
            )
            for at in range(height // piece)
        ],
        axis=0,
    )
    update = jnp.dot(coupling, col_model, preferred_element_type=jnp.float32)
    if before:
        update = update + refs[row_count + col_count][...]
    for place, out_ref in enumerate(refs[-out_count:]):
        rows = out_ref.shape[0]
        out_ref[...] = update[place * rows : (place + 1) * rows].astype(out_ref.dtype)


def couple(rows, cols, gains, weights, piece, outs, before=None, kind=jnp.bfloat16):
    args = [*rows, *cols] + ([] if before is None else [before]) + [gains, weights]
    height, width = gains.shape[1], weights.shape[1]
    return pl.pallas_call(
        functools.partial(
            couple_kernel, piece, len(rows), len(cols), before is not None, outs
        ),
        in_specs=[VMEM] * len(args),
        out_specs=[VMEM] * outs,
        out_shape=[jax.ShapeDtypeStruct((height // outs, 2 * NF), kind)] * outs,
        compiler_params=pltpu.CompilerParams(vmem_limit_bytes=16 << 20),
        cost_estimate=pl.CostEstimate(
            flops=12 * height * width * NF,
            bytes_accessed=8 * (height + width) * NF,
            transcendentals=0,
        ),
        name="couple",
    )(*args)


def to_time_kernel(count, own_side, *refs):
    basis_ref = refs[2 * count]
    out_ref, stage_ref, done_sem = refs[-3:]
    level = lax.axis_index("blk")
    is_inner = (level == 1) | (level == 2)
    upper = level >= 2
    block = jnp.where(upper, 1, 0) if own_side else jnp.where(upper, 0, 1)
    adjoint = jnp.concatenate(
        [
            jnp.where(is_inner, here_ref[...], there_ref[...])
            for here_ref, there_ref in zip(refs[:count], refs[count : 2 * count])
        ],
        axis=0,
    )
    half, span = stage_ref.shape
    start = pl.multiple_of(block * half, half)
    wide = span // 2
    copies = []
    for part in range(2):
        columns = slice(part * wide, (part + 1) * wide)
        traces = lax.dot_general(
            adjoint, basis_ref[columns, :], CONTRACT_LAST, preferred_element_type=jnp.float32
        )
        stage_ref[:, columns] = (traces * (1.0 / math.sqrt(NF))).astype(jnp.bfloat16)
        copies.append(
            pltpu.make_async_copy(
                stage_ref.at[:, columns],
                out_ref.at[pl.ds(start, half), columns],
                done_sem.at[part],
            )
        )
        copies[-1].start()
    for copy in copies:
        copy.wait()


def to_time(own_side, here, there, basis, rows, before):
    span = basis.shape[0]
    half = sum(block.shape[0] for block in here)
    args = [*here, *there, basis]
    specs = [VMEM] * len(args)
    aliases = {}
    if before is not None:
        aliases = {len(args): 0}
        specs.append(pl.BlockSpec(memory_space=pl.ANY))
        args.append(before)
    return pl.pallas_call(
        functools.partial(to_time_kernel, len(here), own_side),
        in_specs=specs,
        out_specs=pl.BlockSpec(memory_space=pl.ANY),
        out_shape=jax.ShapeDtypeStruct((rows, span), jnp.bfloat16),
        scratch_shapes=[
            pltpu.VMEM((half, span), jnp.bfloat16),
            pltpu.SemaphoreType.DMA((2,)),
        ],
        input_output_aliases=aliases,
        compiler_params=pltpu.CompilerParams(vmem_limit_bytes=12 << 20),
        cost_estimate=pl.CostEstimate(
            flops=4 * half * span * NF, bytes_accessed=4 * span * NF, transcendentals=0
        ),
        name="to_time",
    )(*args)


def two_bases_kernel(per_step, low_rows, *refs):
    lc_ref, ls_ref = refs[4:6]
    for high, out_ref in zip((refs[:2], refs[2:4]), refs[6:]):
        basis_kernel(per_step, low_rows, *high, lc_ref, ls_ref, out_ref)


def two_bases(first, second, span):
    low_rows = math.gcd(span, 64)
    tables = []
    for start in (first, second):
        tables += cos_sin(start + jnp.arange(0, span, low_rows, dtype=jnp.int32))
    tables += cos_sin(jnp.arange(low_rows, dtype=jnp.int32))
    per_step = math.gcd(span // low_rows, 4)
    block = pl.BlockSpec((per_step * low_rows, 2 * NF), lambda i: (i, 0))
    return pl.pallas_call(
        functools.partial(two_bases_kernel, per_step, low_rows),
        grid=(span // low_rows // per_step,),
        in_specs=[pl.BlockSpec(table.shape, lambda i: (0, 0)) for table in tables],
        out_specs=[block, block],
        out_shape=[jax.ShapeDtypeStruct((span, 2 * NF), jnp.bfloat16)] * 2,
        compiler_params=pltpu.CompilerParams(vmem_limit_bytes=12 << 20),
        cost_estimate=pl.CostEstimate(
            flops=16 * span * NF, bytes_accessed=8 * span * NF, transcendentals=0
        ),
        name="two_bases",
    )(*tables)


def own_parts_kernel(count, *refs):
    basis_ref = refs[count]
    for block_ref, out_ref in zip(refs[:count], refs[count + 1 :]):
        out_ref[...] = jnp.dot(
            block_ref[...], basis_ref[...], preferred_element_type=jnp.float32
        )


def own_parts(blocks, basis):
    rows, span = blocks[0].shape
    return pl.pallas_call(
        functools.partial(own_parts_kernel, len(blocks)),
        in_specs=[VMEM] * (len(blocks) + 1),
        out_specs=[VMEM] * len(blocks),
        out_shape=[jax.ShapeDtypeStruct((rows, 2 * NF), jnp.float32)] * len(blocks),
        compiler_params=pltpu.CompilerParams(vmem_limit_bytes=12 << 20),
        cost_estimate=pl.CostEstimate(
            flops=4 * len(blocks) * rows * span * NF,
            bytes_accessed=4 * span * NF,
            transcendentals=0,
        ),
        name="own_parts",
    )(*blocks, basis)


def sum_kernel(part_ref, near_ref, basis_ref, *rest):
    total = part_ref[...] + jnp.dot(
        near_ref[...], basis_ref[...], preferred_element_type=jnp.float32
    )
    total = total * (1.0 / math.sqrt(NT))
    if len(rest) == 3:
        rest_ref, own_ref, sum_ref = rest
        own_ref[...] = (total + rest_ref[...].astype(jnp.float32)).astype(jnp.bfloat16)
    else:
        sum_ref = rest[0]
    sum_ref[...] = total.astype(jnp.bfloat16)


def spectra(part, near, basis, others=None):
    rows, span = near.shape
    args = [part, near, basis] + ([] if others is None else [others])
    outs = 1 if others is None else 2
    return pl.pallas_call(
        sum_kernel,
        in_specs=[VMEM] * len(args),
        out_specs=[VMEM] * outs,
        out_shape=[jax.ShapeDtypeStruct((rows, 2 * NF), jnp.bfloat16)] * outs,
        compiler_params=pltpu.CompilerParams(vmem_limit_bytes=12 << 20),
        cost_estimate=pl.CostEstimate(
            flops=4 * rows * span * NF, bytes_accessed=4 * span * NF, transcendentals=0
        ),
        name="spectra",
    )(*args)


def inner_body(synthetic, observed, station_weights, pair_mask):
    levels = lax.axis_size("blk")
    subs = lax.axis_size("sub")
    pairs = lax.axis_size("pair")
    level = lax.axis_index("blk")
    sub = lax.axis_index("sub")
    pair = lax.axis_index("pair")
    span = synthetic.shape[1]
    half = synthetic.shape[0] // 2
    per_half = levels // 2
    stations = station_weights.shape[0]
    piece = half // per_half
    side = level // 2
    inward, swapped, outward = [(0, 1), (3, 2)], [(1, 2), (2, 1)], [(1, 0), (2, 3)]

    def piece_of(which, at, sources):
        return jnp.concatenate(
            [
                lax.dynamic_slice_in_dim(source, which * half + at, piece, 0)
                for source in sources
            ],
            axis=0,
        )

    sources = (synthetic, observed)
    front = piece_of(1 - side, 0, sources)
    front, sources = lax.optimization_barrier((front, sources))
    passed = [front] + [piece_of(1 - side, at, sources) for at in range(piece, half, piece)]
    kept = [piece_of(side, at, sources) for at in range(0, half, piece)]
    near_passed, near_kept = [], []
    for blocks, arrived in ((passed, near_passed), (kept, near_kept)):
        for block in blocks:
            arrived.append(lax.ppermute(block, "blk", inward))

    member = sub * pairs + pair
    hops = [(s, q) for s in range(subs) for q in range(pairs)]
    starts = [
        ((sub - s) % subs * pairs + (pair - q) % pairs) * 2 * half + side * half + at
        for at in range(0, half, piece)
        for s, q in hops
    ]
    gains = station_weights.astype(jnp.float32)
    col_gains = jnp.concatenate(
        [lax.dynamic_slice_in_dim(gains, start, piece, 0) for start in starts]
    )[None, :]
    firsts = [member * 2 * half + which * half for which in (side, 1 - side)]
    own_gains, other_gains = [
        lax.dynamic_slice_in_dim(gains, start, half, 0)[None, :] for start in firsts
    ]
    link = jnp.maximum(pair_mask, pair_mask.T).astype(jnp.float32)
    link_rows = jnp.concatenate(
        [lax.dynamic_slice_in_dim(link, start // piece, per_half, 0) for start in firsts], axis=0
    )
    col_pieces = jnp.repeat(jnp.stack(starts) // piece, piece)
    chosen = jnp.arange(link.shape[0], dtype=jnp.int32)[:, None] == col_pieces[None, :]
    active = jnp.sum(jnp.where(chosen[None], link_rows[:, :, None], 0.0), axis=1)
    weights = 4.0 / math.sqrt(stations) * col_gains * active
    late = (subs - 1) * pairs
    early_width = (len(starts) - late) * piece
    own_early, own_late = weights[:per_half, :early_width], weights[:per_half, early_width:]
    here, own_gains, other_gains, own_early, own_late, other_weights = lax.optimization_barrier(
        (level, own_gains, other_gains, own_early, own_late, weights[per_half:])
    )

    here_basis, near_basis = two_bases(here * span, (here ^ 1) * span, span)
    passed_parts = own_parts(passed, here_basis)
    kept_parts = own_parts(kept, here_basis)
    to_pass, kept_rest = [], []
    for place in range(per_half):
        (summed,) = spectra(passed_parts[place], near_passed[place], near_basis)
        to_pass.append(summed)
        kept_rest.append(lax.ppermute(summed, "blk", swapped))
    own, passed_rest, cols = [], [], {}
    for place in range(per_half):
        whole, summed = spectra(
            kept_parts[place], near_kept[place], near_basis, kept_rest[place]
        )
        own.append(whole)
        for s, q in hops:
            if q == 0:
                cols[s, q, place] = whole if s == 0 else shift(whole, "sub", s)
            else:
                cols[s, q, place] = shift(cols[s, 0, place], "pair", q)
        passed_rest.append(lax.ppermute(summed, "blk", swapped))
    cols = [cols[s, q, place] for place in range(per_half) for s, q in hops]
    (begun,) = couple(own, cols[:-late], own_gains, own_early, piece, 1, None, jnp.float32)
    own_part = couple(own, cols[-late:], own_gains, own_late, piece, per_half, begun)
    other = [block for both in zip(to_pass, passed_rest) for block in both]
    other_part = couple(other, cols, other_gains, other_weights, piece, per_half)

    def finish(sent, mine):
        sums, arrived = [], []
        for place in range(per_half):
            rest = lax.ppermute(sent[place], "blk", swapped)
            whole = mine[place].astype(jnp.float32) + rest.astype(jnp.float32)
            sums.append(whole.astype(jnp.bfloat16))
            arrived.append(lax.ppermute(sums[-1], "blk", outward))
        return sums, arrived

    first = finish(own_part, other_part)
    second = finish(other_part, own_part)
    rows = synthetic.shape[0]
    traces = to_time(False, *first, here_basis, rows, None)
    return to_time(True, *second, here_basis, rows, traces)


def shards(*args):
    body = inner_body if lax.axis_size("blk") == 4 else ring_body
    return body(*args)


def solution(mesh):
    placed = (
        P(("events", "sub", "pair"), "blk"),
        P(("events", "sub", "pair"), "blk"),
        P("events"),
        P("events", None),
    )
    return jax.shard_map(
        shards,
        mesh=mesh,
        in_specs=placed,
        out_specs=P(("events", "sub", "pair"), "blk"),
        check_vma=False,
    )
```

```python
import functools
import math

import jax
import jax.numpy as jnp
from jax import lax
from jax.experimental import pallas as pl
from jax.experimental.pallas import tpu as pltpu
from jax.sharding import PartitionSpec as P


NT = 4096
NF = 512
F_LO = 64

epsilon = 1e-06
CONTRACT_LAST = (((1,), (1,)), ((), ()))
VMEM = pl.BlockSpec(memory_space=pltpu.VMEM)


def shift(value, axis, steps):
    count = lax.axis_size(axis)
    pairs = [(source, (source + steps) % count) for source in range(count)]
    return lax.ppermute(value, axis, pairs)


def sweep(count):
    order = []
    for near in range(1, count // 2 + 1):
        order.append(near)
        if (count - near) % count != near:
            order.append(count - near)
    return order


def cos_sin(samples):
    bins = F_LO + jnp.arange(NF, dtype=jnp.int32)
    phases = samples[:, None] * bins[None, :] % NT
    angles = phases.astype(jnp.float32) * (2.0 * math.pi / NT)
    return jnp.cos(angles), jnp.sin(angles)


def basis_kernel(per_step, low_rows, hc_ref, hs_ref, lc_ref, ls_ref, out_ref):
    step = pl.program_id(0)
    for h in range(per_step):
        hc = hc_ref[pl.ds(step * per_step + h, 1), :]
        hs = hs_ref[pl.ds(step * per_step + h, 1), :]
        lc = lc_ref[...]
        ls = ls_ref[...]
        rows = slice(h * low_rows, (h + 1) * low_rows)
        out_ref[rows, :NF] = (hc * lc - hs * ls).astype(jnp.bfloat16)
        out_ref[rows, NF:] = (-(hs * lc + hc * ls)).astype(jnp.bfloat16)


def make_basis(firsts, span):
    low_rows = math.gcd(span, 64)
    low_c, low_s = cos_sin(jnp.arange(low_rows, dtype=jnp.int32))
    highs = (firsts[:, None] + jnp.arange(0, span, low_rows, dtype=jnp.int32)[None, :]).reshape(-1)
    high_c, high_s = cos_sin(highs)
    per_step = math.gcd(highs.shape[0], 4)
    whole = lambda a: pl.BlockSpec(a.shape, lambda i: (0, 0))
    rows = highs.shape[0] * low_rows
    return pl.pallas_call(
        functools.partial(basis_kernel, per_step, low_rows),
        grid=(highs.shape[0] // per_step,),
        in_specs=[whole(high_c), whole(high_s), whole(low_c), whole(low_s)],
        out_specs=pl.BlockSpec((per_step * low_rows, 2 * NF), lambda i: (i, 0)),
        out_shape=jax.ShapeDtypeStruct((rows, 2 * NF), jnp.bfloat16),
        cost_estimate=pl.CostEstimate(
            flops=8 * rows * NF, bytes_accessed=4 * rows * NF, transcendentals=0
        ),
        compiler_params=pltpu.CompilerParams(vmem_limit_bytes=16 << 20),
        name="basis",
    )(high_c, high_s, low_c, low_s)


def angular_row():
    bins = F_LO + lax.broadcasted_iota(jnp.int32, (1, NF), 1)
    return 2.0 * math.pi / NT * bins.astype(jnp.float32)


def rate_of(re, im):
    angular = angular_row()
    return jnp.concatenate([-angular * im, angular * re], axis=1).astype(jnp.bfloat16)


def tile_kernel(first, rows_ref, power_ref, coef_ref, gain_ref, col_ref, *rest):
    out_ref = rest[-1]
    col = col_ref[...].astype(jnp.float32)
    model_rate = rate_of(col[:, :NF], col[:, NF : 2 * NF])
    data_rate = rate_of(-col[:, 2 * NF : 3 * NF], -col[:, 3 * NF :])
    both = jnp.concatenate([model_rate, data_rate], axis=1)
    cross = lax.dot_general(
        rows_ref[...], both, CONTRACT_LAST, preferred_element_type=jnp.float32
    )
    col_power = lax.dot_general(
        jnp.ones((8, 2 * NF), jnp.float32),
        jnp.square(model_rate.astype(jnp.float32)),
        CONTRACT_LAST,
        precision=lax.Precision.HIGHEST,
        preferred_element_type=jnp.float32,
    )[0:1, :]
    normalizer = 0.5 * (power_ref[...] + col_power) + epsilon
    coupling = (coef_ref[...] * gain_ref[...] * cross / normalizer).astype(jnp.bfloat16)
    update = jnp.dot(coupling, model_rate, preferred_element_type=jnp.float32)
    if first:
        out_ref[...] = update
    else:
        out_ref[...] = rest[0][...] + update


def pair_tile(running, rows, row_power, coef, gain, col):
    args = [rows, row_power, coef, gain, col]
    aliases = {}
    if running is not None:
        aliases = {len(args): 0}
        args.append(running)
    height, width = rows.shape[0], col.shape[0]
    return pl.pallas_call(
        functools.partial(tile_kernel, running is None),
        in_specs=[pl.BlockSpec(memory_space=pltpu.VMEM)] * len(args),
        out_specs=pl.BlockSpec(memory_space=pltpu.VMEM),
        out_shape=jax.ShapeDtypeStruct((height, 2 * NF), jnp.float32),
        input_output_aliases=aliases,
        cost_estimate=pl.CostEstimate(
            flops=12 * height * width * NF,
            bytes_accessed=16 * height * NF,
            transcendentals=0,
        ),
        name="pair_tile",
    )(*args)


def ring_body(synthetic, observed, station_weights, pair_mask):
    levels = lax.axis_size("blk")
    subs = lax.axis_size("sub")
    pairs = lax.axis_size("pair")
    level = lax.axis_index("blk")
    sub = lax.axis_index("sub")
    pair = lax.axis_index("pair")
    span = synthetic.shape[1]
    piece = synthetic.shape[0] // levels
    stations = station_weights.shape[0]

    def owned_by(steps):
        owner = (level + steps) % levels
        return jnp.concatenate(
            [
                lax.dynamic_slice_in_dim(synthetic, owner * piece, piece, 0),
                lax.dynamic_slice_in_dim(observed, owner * piece, piece, 0),
            ],
            axis=0,
        )

    order = sweep(levels)
    blocks = {0: owned_by(0)}
    for steps in order:
        blocks[steps] = shift(owned_by(steps), "blk", steps)
    arrivals = [0] + order
    firsts = jnp.stack([(level - steps) % levels * span for steps in arrivals]).astype(jnp.int32)
    basis = make_basis(firsts, span)
    member = sub * pairs + pair
    members = jnp.stack(
        [
            (sub - s) % subs * pairs + (pair - q) % pairs
            for s in range(subs)
            for q in range(pairs)
        ]
    )
    gains = station_weights.astype(jnp.float32).reshape(-1, piece)
    link = jnp.maximum(pair_mask, pair_mask.T).astype(jnp.float32)
    row_pieces = members * levels + level
    row_gain = gains[row_pieces].reshape(-1, 1)
    row_link = link[row_pieces]
    factor = 4.0 / math.sqrt(stations)
    coefs, col_gains = [], []
    for steps in arrivals:
        column_piece = member * levels + (level - steps) % levels
        active = lax.dynamic_slice_in_dim(row_link, column_piece, 1, 1)
        coefs.append(factor * row_gain * jnp.repeat(active, piece, axis=0))
        col_gains.append(lax.dynamic_slice_in_dim(gains, column_piece, 1, 0))
    last = order[-1]
    blocks[last], coefs, col_gains = lax.optimization_barrier((blocks[last], coefs, col_gains))
    total = None
    for place, steps in enumerate(arrivals):
        part = jnp.dot(
            blocks[steps],
            basis[place * span : (place + 1) * span],
            preferred_element_type=jnp.float32,
        )
        total = part if total is None else total + part
    spec = (total * (1.0 / math.sqrt(NT))).astype(jnp.bfloat16)
    own = jnp.concatenate([spec[:piece], spec[piece:]], axis=1)

    columns = {0: own}
    for steps in order:
        columns[steps] = shift(own, "blk", steps)
    blocks_of_rows = []
    for s in range(subs):
        here = own if s == 0 else shift(own, "sub", s)
        for q in range(pairs):
            blocks_of_rows.append(here if q == 0 else shift(here, "pair", q))
    rows = jnp.concatenate(blocks_of_rows, axis=0)
    widened = rows[:, : 2 * NF].astype(jnp.float32)
    row_rate = rate_of(widened[:, :NF], widened[:, NF:])
    row_power = jnp.sum(jnp.square(row_rate.astype(jnp.float32)), axis=1, keepdims=True)

    running = None
    for place, steps in enumerate(arrivals):
        running = pair_tile(
            running, rows, row_power, coefs[place], col_gains[place], columns[steps]
        )

    partial = running.reshape(subs, pairs, piece, 2 * NF)
    held = partial[:, 0]
    for q in range(1, pairs):
        sent = partial[:, q].astype(jnp.bfloat16)
        held = held + shift(sent, "pair", -q).astype(jnp.float32)
    adjoint = held[0]
    for s in range(1, subs):
        adjoint = adjoint + shift(held[s].astype(jnp.bfloat16), "sub", -s).astype(jnp.float32)
    adjoint = adjoint.astype(jnp.bfloat16)

    gathered = jnp.zeros((levels * piece, 2 * NF), jnp.bfloat16)
    for steps in arrivals:
        arrived = adjoint if steps == 0 else shift(adjoint, "blk", steps)
        gathered = lax.dynamic_update_slice_in_dim(
            gathered, arrived, (level - steps) % levels * piece, 0
        )
    return (
        lax.dot_general(
            gathered, basis[:span], CONTRACT_LAST, preferred_element_type=jnp.float32
        )
        * (1.0 / math.sqrt(NF))
    ).astype(jnp.bfloat16)


def power_of(spec):
    wide = spec.astype(jnp.float32)
    rate = rate_of(wide[:, :NF], wide[:, NF:])
    return rate, jnp.sum(jnp.square(rate.astype(jnp.float32)), axis=1, keepdims=True)


def couple_kernel(piece, row_count, col_count, before, out_count, *refs):
    row_refs = refs[:row_count]
    col_refs = refs[row_count : row_count + col_count]
    gain_ref, weight_ref = refs[-out_count - 2 : -out_count]
    sums = row_count // (gain_ref.shape[1] // piece)
    row_models, row_datas = [], []
    for at in range(0, row_count, sums):
        block = row_refs[at][...]
        if sums == 2:
            block = (
                block.astype(jnp.float32) + row_refs[at + 1][...].astype(jnp.float32)
            ).astype(jnp.bfloat16)
        row_models.append(block[:piece])
        row_datas.append(block[piece:])
    row_model = jnp.concatenate(row_models, axis=0)
    row_data = jnp.concatenate(row_datas, axis=0)
    row_power = power_of(row_model)[1]
    models, datas, powers = [], [], []
    for ref in col_refs:
        rate, power = power_of(ref[:piece])
        models.append(rate)
        powers.append(power)
        wide = ref[piece:].astype(jnp.float32)
        datas.append(rate_of(wide[:, :NF], wide[:, NF:]))
    col_model = jnp.concatenate(models, axis=0)
    col_data = jnp.concatenate(datas, axis=0)
    powers = jnp.concatenate(powers, axis=0)

    def diagonal(width):
        return lax.broadcasted_iota(jnp.int32, (width, width), 0) == lax.broadcasted_iota(
            jnp.int32, (width, width), 1
        )

    col_power = jnp.sum(
        jnp.where(diagonal(powers.shape[0]), powers, 0.0), axis=0, keepdims=True
    )
    height = gain_ref.shape[1]
    row_gain = jnp.sum(
        jnp.where(diagonal(height), gain_ref[...], 0.0), axis=1, keepdims=True
    )
    cross = lax.dot_general(
        row_model, col_model, CONTRACT_LAST, preferred_element_type=jnp.float32
    ) - lax.dot_general(row_data, col_data, CONTRACT_LAST, preferred_element_type=jnp.float32)
    normalizer = 0.5 * (row_power + col_power) + epsilon
    ratio = row_gain * cross / normalizer
    coupling = jnp.concatenate(
        [
            (weight_ref[at : at + 1, :] * ratio[at * piece : (at + 1) * piece]).astype(
                jnp.bfloat16
            )
            for at in range(height // piece)
        ],
        axis=0,
    )
    update = jnp.dot(coupling, col_model, preferred_element_type=jnp.float32)
    if before:
        update = update + refs[row_count + col_count][...]
    for place, out_ref in enumerate(refs[-out_count:]):
        rows = out_ref.shape[0]
        out_ref[...] = update[place * rows : (place + 1) * rows].astype(out_ref.dtype)


def couple(rows, cols, gains, weights, piece, outs, before=None, kind=jnp.bfloat16):
    args = [*rows, *cols] + ([] if before is None else [before]) + [gains, weights]
    height, width = gains.shape[1], weights.shape[1]
    return pl.pallas_call(
        functools.partial(
            couple_kernel, piece, len(rows), len(cols), before is not None, outs
        ),
        in_specs=[VMEM] * len(args),
        out_specs=[VMEM] * outs,
        out_shape=[jax.ShapeDtypeStruct((height // outs, 2 * NF), kind)] * outs,
        compiler_params=pltpu.CompilerParams(vmem_limit_bytes=16 << 20),
        cost_estimate=pl.CostEstimate(
            flops=12 * height * width * NF,
            bytes_accessed=8 * (height + width) * NF,
            transcendentals=0,
        ),
        name="couple",
    )(*args)


def to_time_kernel(count, own_side, *refs):
    basis_ref = refs[2 * count]
    out_ref, stage_ref, done_sem = refs[-3:]
    level = lax.axis_index("blk")
    is_inner = (level == 1) | (level == 2)
    upper = level >= 2
    block = jnp.where(upper, 1, 0) if own_side else jnp.where(upper, 0, 1)
    adjoint = jnp.concatenate(
        [
            jnp.where(is_inner, here_ref[...], there_ref[...])
            for here_ref, there_ref in zip(refs[:count], refs[count : 2 * count])
        ],
        axis=0,
    )
    half, span = stage_ref.shape
    start = pl.multiple_of(block * half, half)
    wide = span // 2
    copies = []
    for part in range(2):
        columns = slice(part * wide, (part + 1) * wide)
        traces = jnp.dot(
            adjoint, basis_ref[:, columns], preferred_element_type=jnp.float32
        )
        stage_ref[:, columns] = (traces * (1.0 / math.sqrt(NF))).astype(jnp.bfloat16)
        copies.append(
            pltpu.make_async_copy(
                stage_ref.at[:, columns],
                out_ref.at[pl.ds(start, half), columns],
                done_sem.at[part],
            )
        )
        copies[-1].start()
    for copy in copies:
        copy.wait()


def to_time(own_side, here, there, basis, rows, before):
    span = basis.shape[1]
    half = sum(block.shape[0] for block in here)
    args = [*here, *there, basis]
    specs = [VMEM] * len(args)
    aliases = {}
    if before is not None:
        aliases = {len(args): 0}
        specs.append(pl.BlockSpec(memory_space=pl.ANY))
        args.append(before)
    return pl.pallas_call(
        functools.partial(to_time_kernel, len(here), own_side),
        in_specs=specs,
        out_specs=pl.BlockSpec(memory_space=pl.ANY),
        out_shape=jax.ShapeDtypeStruct((rows, span), jnp.bfloat16),
        scratch_shapes=[
            pltpu.VMEM((half, span), jnp.bfloat16),
            pltpu.SemaphoreType.DMA((2,)),
        ],
        input_output_aliases=aliases,
        compiler_params=pltpu.CompilerParams(vmem_limit_bytes=12 << 20),
        cost_estimate=pl.CostEstimate(
            flops=4 * half * span * NF, bytes_accessed=4 * span * NF, transcendentals=0
        ),
        name="to_time",
    )(*args)


def two_bases_kernel(per_step, low_rows, *refs):
    lc_ref, ls_ref = refs[4:6]
    for high, out_ref in zip((refs[:2], refs[2:4]), refs[6:]):
        basis_kernel(per_step, low_rows, *high, lc_ref, ls_ref, out_ref)


def two_bases(first, second, span):
    low_rows = math.gcd(span, 64)
    tables = []
    for start in (first, second):
        tables += cos_sin(start + jnp.arange(0, span, low_rows, dtype=jnp.int32))
    tables += cos_sin(jnp.arange(low_rows, dtype=jnp.int32))
    per_step = math.gcd(span // low_rows, 4)
    block = pl.BlockSpec((per_step * low_rows, 2 * NF), lambda i: (i, 0))
    return pl.pallas_call(
        functools.partial(two_bases_kernel, per_step, low_rows),
        grid=(span // low_rows // per_step,),
        in_specs=[pl.BlockSpec(table.shape, lambda i: (0, 0)) for table in tables],
        out_specs=[block, block],
        out_shape=[jax.ShapeDtypeStruct((span, 2 * NF), jnp.bfloat16)] * 2,
        compiler_params=pltpu.CompilerParams(vmem_limit_bytes=12 << 20),
        cost_estimate=pl.CostEstimate(
            flops=16 * span * NF, bytes_accessed=8 * span * NF, transcendentals=0
        ),
        name="two_bases",
    )(*tables)


def turn_kernel(basis_ref, out_ref):
    out_ref[...] = basis_ref[...].T


def turned(basis):
    return pl.pallas_call(
        turn_kernel,
        in_specs=[VMEM],
        out_specs=VMEM,
        out_shape=jax.ShapeDtypeStruct(basis.shape[::-1], basis.dtype),
        compiler_params=pltpu.CompilerParams(vmem_limit_bytes=12 << 20),
        cost_estimate=pl.CostEstimate(
            flops=basis.size, bytes_accessed=4 * basis.size, transcendentals=0
        ),
        name="turned",
    )(basis)


def own_parts_kernel(count, *refs):
    basis_ref = refs[count]
    for block_ref, out_ref in zip(refs[:count], refs[count + 1 :]):
        out_ref[...] = jnp.dot(
            block_ref[...], basis_ref[...], preferred_element_type=jnp.float32
        )


def own_parts(blocks, basis):
    rows, span = blocks[0].shape
    return pl.pallas_call(
        functools.partial(own_parts_kernel, len(blocks)),
        in_specs=[VMEM] * (len(blocks) + 1),
        out_specs=[VMEM] * len(blocks),
        out_shape=[jax.ShapeDtypeStruct((rows, 2 * NF), jnp.float32)] * len(blocks),
        compiler_params=pltpu.CompilerParams(vmem_limit_bytes=12 << 20),
        cost_estimate=pl.CostEstimate(
            flops=4 * len(blocks) * rows * span * NF,
            bytes_accessed=4 * span * NF,
            transcendentals=0,
        ),
        name="own_parts",
    )(*blocks, basis)


def sum_kernel(part_ref, near_ref, basis_ref, *rest):
    total = part_ref[...] + jnp.dot(
        near_ref[...], basis_ref[...], preferred_element_type=jnp.float32
    )
    total = total * (1.0 / math.sqrt(NT))
    if len(rest) == 3:
        rest_ref, own_ref, sum_ref = rest
        own_ref[...] = (total + rest_ref[...].astype(jnp.float32)).astype(jnp.bfloat16)
    else:
        sum_ref = rest[0]
    sum_ref[...] = total.astype(jnp.bfloat16)


def spectra(part, near, basis, others=None):
    rows, span = near.shape
    args = [part, near, basis] + ([] if others is None else [others])
    outs = 1 if others is None else 2
    return pl.pallas_call(
        sum_kernel,
        in_specs=[VMEM] * len(args),
        out_specs=[VMEM] * outs,
        out_shape=[jax.ShapeDtypeStruct((rows, 2 * NF), jnp.bfloat16)] * outs,
        compiler_params=pltpu.CompilerParams(vmem_limit_bytes=12 << 20),
        cost_estimate=pl.CostEstimate(
            flops=4 * rows * span * NF, bytes_accessed=4 * span * NF, transcendentals=0
        ),
        name="spectra",
    )(*args)


def inner_body(synthetic, observed, station_weights, pair_mask):
    levels = lax.axis_size("blk")
    subs = lax.axis_size("sub")
    pairs = lax.axis_size("pair")
    level = lax.axis_index("blk")
    sub = lax.axis_index("sub")
    pair = lax.axis_index("pair")
    span = synthetic.shape[1]
    half = synthetic.shape[0] // 2
    per_half = levels // 2
    stations = station_weights.shape[0]
    piece = half // per_half
    side = level // 2
    inward, swapped, outward = [(0, 1), (3, 2)], [(1, 2), (2, 1)], [(1, 0), (2, 3)]

    def piece_of(which, at, sources):
        return jnp.concatenate(
            [
                lax.dynamic_slice_in_dim(source, which * half + at, piece, 0)
                for source in sources
            ],
            axis=0,
        )

    sources = (synthetic, observed)
    front = piece_of(1 - side, 0, sources)
    front, sources = lax.optimization_barrier((front, sources))
    passed = [front] + [piece_of(1 - side, at, sources) for at in range(piece, half, piece)]
    kept = [piece_of(side, at, sources) for at in range(0, half, piece)]
    near_passed, near_kept = [], []
    for blocks, arrived in ((passed, near_passed), (kept, near_kept)):
        for block in blocks:
            arrived.append(lax.ppermute(block, "blk", inward))

    member = sub * pairs + pair
    hops = [(s, q) for s in range(subs) for q in range(pairs)]
    starts = [
        ((sub - s) % subs * pairs + (pair - q) % pairs) * 2 * half + side * half + at
        for at in range(0, half, piece)
        for s, q in hops
    ]
    gains = station_weights.astype(jnp.float32)
    col_gains = jnp.concatenate(
        [lax.dynamic_slice_in_dim(gains, start, piece, 0) for start in starts]
    )[None, :]
    firsts = [member * 2 * half + which * half for which in (side, 1 - side)]
    own_gains, other_gains = [
        lax.dynamic_slice_in_dim(gains, start, half, 0)[None, :] for start in firsts
    ]
    link = jnp.maximum(pair_mask, pair_mask.T).astype(jnp.float32)
    link_rows = jnp.concatenate(
        [lax.dynamic_slice_in_dim(link, start // piece, per_half, 0) for start in firsts], axis=0
    )
    col_pieces = jnp.repeat(jnp.stack(starts) // piece, piece)
    chosen = jnp.arange(link.shape[0], dtype=jnp.int32)[:, None] == col_pieces[None, :]
    active = jnp.sum(jnp.where(chosen[None], link_rows[:, :, None], 0.0), axis=1)
    weights = 4.0 / math.sqrt(stations) * col_gains * active
    late = (subs - 1) * pairs
    early_width = (len(starts) - late) * piece
    own_early, own_late = weights[:per_half, :early_width], weights[:per_half, early_width:]
    here, own_gains, other_gains, own_early, own_late, other_weights = lax.optimization_barrier(
        (level, own_gains, other_gains, own_early, own_late, weights[per_half:])
    )

    here_basis, near_basis = two_bases(here * span, (here ^ 1) * span, span)
    passed_parts = own_parts(passed, here_basis)
    kept_parts = own_parts(kept, here_basis)
    to_pass, kept_rest = [], []
    for place in range(per_half):
        (summed,) = spectra(passed_parts[place], near_passed[place], near_basis)
        to_pass.append(summed)
        kept_rest.append(lax.ppermute(summed, "blk", swapped))
    turned_basis = turned(here_basis)
    near_kept[0], turned_basis = lax.optimization_barrier((near_kept[0], turned_basis))
    own, passed_rest, cols = [], [], {}
    for place in range(per_half):
        whole, summed = spectra(
            kept_parts[place], near_kept[place], near_basis, kept_rest[place]
        )
        own.append(whole)
        for s, q in hops:
            if q == 0:
                cols[s, q, place] = whole if s == 0 else shift(whole, "sub", s)
            else:
                cols[s, q, place] = shift(cols[s, 0, place], "pair", q)
        passed_rest.append(lax.ppermute(summed, "blk", swapped))
    cols = [cols[s, q, place] for place in range(per_half) for s, q in hops]
    (begun,) = couple(own, cols[:-late], own_gains, own_early, piece, 1, None, jnp.float32)
    own_part = couple(own, cols[-late:], own_gains, own_late, piece, per_half, begun)
    other = [block for both in zip(to_pass, passed_rest) for block in both]
    other_part = couple(other, cols, other_gains, other_weights, piece, per_half)

    def finish(sent, mine):
        sums, arrived = [], []
        for place in range(per_half):
            rest = lax.ppermute(sent[place], "blk", swapped)
            whole = mine[place].astype(jnp.float32) + rest.astype(jnp.float32)
            sums.append(whole.astype(jnp.bfloat16))
            arrived.append(lax.ppermute(sums[-1], "blk", outward))
        return sums, arrived

    first = finish(own_part, other_part)
    second = finish(other_part, own_part)
    rows = synthetic.shape[0]
    traces = to_time(False, *first, turned_basis, rows, None)
    return to_time(True, *second, turned_basis, rows, traces)


def shards(*args):
    body = inner_body if lax.axis_size("blk") == 4 else ring_body
    return body(*args)


def solution(mesh):
    placed = (
        P(("events", "sub", "pair"), "blk"),
        P(("events", "sub", "pair"), "blk"),
        P("events"),
        P("events", None),
    )
    return jax.shard_map(
        shards,
        mesh=mesh,
        in_specs=placed,
        out_specs=P(("events", "sub", "pair"), "blk"),
        check_vma=False,
    )
```
